32 devices in a mesh: dp: 4 (over y, x), shard: 8 (over z, core).
Axes of the slice: x: 2, y: 2, z: 4, core: 2. Of those that a mesh axis runs over, the one named last changes fastest.
Arguments:
- text_input: bfloat16 [4096, 768], P(('dp', 'shard')), may hold values from -6 to 6
- layout_input: bfloat16 [4096, 192], P(('dp', 'shard')), may hold values from -6 to 6
- text_cot: bfloat16 [4096, 768], P(('dp', 'shard')), may hold values from -6 to 6
- layout_cot: bfloat16 [4096, 192], P(('dp', 'shard')), may hold values from -6 to 6
- segment_ids: int32 [4096], P(('dp', 'shard')), may hold values from 0 to 63, as said below
- page_groups: int32 [64], P(('dp', 'shard')), may hold values from 0 to 7
- lang_table: bfloat16 [2, 6144], P(None, ('dp', 'shard')), may hold values from -3 to 3
- text_attn: bfloat16 [2, 768, 3072], P(None, None, ('dp', 'shard'))
- text_up: bfloat16 [2, 768, 3072], P(None, None, ('dp', 'shard')), may hold values from -0.21875 to 0.21875
- text_down: bfloat16 [2, 3072, 768], P(None, ('dp', 'shard')), may hold values from -0.109375 to 0.109375
- text_vector: bfloat16 [2, 9216], P(None, ('dp', 'shard'))
- layout_attn: bfloat16 [2, 192, 768], P(None, None, ('dp', 'shard'))
- layout_up: bfloat16 [2, 192, 768], P(None, None, ('dp', 'shard')), may hold values from -0.4375 to 0.4375
- layout_down: bfloat16 [2, 768, 192], P(None, ('dp', 'shard')), may hold values from -0.21875 to 0.21875
- layout_vector: bfloat16 [2, 2304], P(None, ('dp', 'shard'))
Outputs:
- text_out: float32 [4096, 768], P(('dp', 'shard'))
- layout_out: float32 [4096, 192], P(('dp', 'shard'))
- text_input_grad: float32 [4096, 768], P(('dp', 'shard'))
- layout_input_grad: float32 [4096, 192], P(('dp', 'shard'))
- text_attn_grad: float32 [2, 768, 3072], P(None, None, ('dp', 'shard'))
- text_up_grad: float32 [2, 768, 3072], P(None, None, ('dp', 'shard'))
- text_down_grad: float32 [2, 3072, 768], P(None, ('dp', 'shard'))
- text_vector_grad: float32 [2, 9216], P(None, ('dp', 'shard'))
- lang_table_grad: float32 [2, 6144], P(None, ('dp', 'shard'))
- layout_attn_grad: float32 [2, 192, 768], P(None, None, ('dp', 'shard'))
- layout_up_grad: float32 [2, 192, 768], P(None, None, ('dp', 'shard'))
- layout_down_grad: float32 [2, 768, 192], P(None, ('dp', 'shard'))
- layout_vector_grad: float32 [2, 2304], P(None, ('dp', 'shard'))
The draws below stay inside these ranges and needn't reach their ends.
Inputs may be any that keep to these rules, and one draw needn't show every extreme that they name: `segment_ids`: each aligned block of 128 tokens (the tokens of one device) holds one or two whole pages, numbered 2b and 2b + 1 in block b, page 2b first; no page crosses a block; the first block is a single page of 128 tokens and the last block holds two pages.
All inputs are finite; a program needn't handle non-finite values.
Results may differ from the reference program's by a relative error of at most 0.025.
The reference program's roundings to bfloat16 on the way count: a program that leaves them out, or rounds other values in their place, can miss the bound.
Values may be sent and summed in bfloat16 or wider, within the bound.
A program may use at most 256 MiB of HBM per device.

```python
import math
import jax
import jax.numpy as jnp
from jax import lax

D = 768
H = 12
FF = 3072
L = 192
FFL = 768
TOK_DEV = 128
LAYERS = 2
LANGS = 8
TOKENS = 4096
PAGES = 64


def attention_draw(key, stream_width):
    shape_all = (LAYERS, stream_width, 4 * stream_width)
    random_part = jnp.clip(jax.random.normal(key, shape_all, jnp.float32), -4.0, 4.0)
    column = jnp.arange(4 * stream_width, dtype=jnp.int32)
    factor = jnp.where(column < 3 * stream_width, jnp.float32(1.0), jnp.float32(8.0)) / math.sqrt(stream_width)
    return (random_part * factor[None, None, :]).astype(jnp.bfloat16)


def vector_draw(key, stream_width, hidden_width):
    length_all = 8 * stream_width + hidden_width
    shape_all = (LAYERS, length_all)
    offsets = 0.3 * jnp.clip(jax.random.normal(key, shape_all, jnp.float32), -4.0, 4.0)
    scales = jnp.exp(jax.random.uniform(jax.random.fold_in(key, 1), shape_all, jnp.float32, -0.69, 0.69))
    position = jnp.arange(length_all, dtype=jnp.int32)
    gain_slot = (position >= 4 * stream_width) & (position < 5 * stream_width) | (position >= 6 * stream_width) & (position < 7 * stream_width)
    return jnp.where(gain_slot[None, :], scales, offsets).astype(jnp.bfloat16)


def draw_text_attn(key, part):
    return attention_draw(jax.random.fold_in(key, 11), D)


def draw_layout_attn(key, part):
    return attention_draw(jax.random.fold_in(key, 12), L)


def draw_text_vector(key, part):
    return vector_draw(jax.random.fold_in(key, 21), D, FF)


def draw_layout_vector(key, part):
    return vector_draw(jax.random.fold_in(key, 22), L, FFL)


def draw_segment_ids(key, part):
    block_total = TOKENS // TOK_DEV
    cut_points = jax.random.randint(key, (block_total,), TOK_DEV // 4, 3 * TOK_DEV // 4 + 1, dtype=jnp.int32)
    whole_page = jax.random.randint(jax.random.fold_in(key, 1), (block_total,), 0, 4, dtype=jnp.int32) == 0
    block_index = jnp.arange(block_total, dtype=jnp.int32)
    whole_page = whole_page & (block_index != block_total - 1) | (block_index == 0)
    cut_points = jnp.where(whole_page, TOK_DEV, cut_points)
    position = jnp.arange(TOK_DEV, dtype=jnp.int32)
    second = (position[None, :] >= cut_points[:, None]).astype(jnp.int32)
    return (2 * block_index[:, None] + second).reshape(TOKENS)


def place_ends(result, key, low, top_value):
    place = [jax.random.randint(jax.random.fold_in(key, axis), (), 0, length) for axis, length in enumerate(result.shape)]
    widest = result.shape.index(max(result.shape))
    beside = place[:widest] + [(place[widest] + 1) % result.shape[widest]] + place[widest + 1:]
    return result.at[tuple(place)].set(low).at[tuple(beside)].set(top_value)


def level_of(own_key, extent, cuts, least, top_value):
    gain = 1.0
    for dim, parts in cuts:
        draws = jax.random.uniform(jax.random.fold_in(jax.random.fold_in(own_key, 6), dim), (parts,), jnp.float32, least / len(cuts), top_value / len(cuts))
        gain = gain * jnp.repeat(jnp.exp(draws), extent[dim] // parts).reshape((-1,) + (1,) * (len(extent) - 1 - dim))
    return gain


def scatter_about(key, extent, scale, limit, cuts=(), held_as=jnp.bfloat16):
    values = jax.random.normal(key, extent, jnp.float32) * scale
    if len(cuts) > 0:
        values = level_of(key, extent, cuts, -0.22, 0.18) * values
    return jnp.clip(values, min=-limit, max=limit).astype(held_as)


def setup_inputs(seed: int = 0) -> dict:
    keys = jax.random.split(jax.random.key(seed), 16)
    return {
        "text_input": scatter_about(keys[0], (TOKENS, D), 1.0, 6.0, ((0, 32),)),
        "layout_input": scatter_about(keys[1], (TOKENS, L), 1.0, 6.0, ((0, 32),)),
        "text_cot": scatter_about(keys[2], (TOKENS, D), 1.0, 6.0, ((0, 32),)),
        "layout_cot": scatter_about(keys[3], (TOKENS, L), 1.0, 6.0, ((0, 32),)),
        "segment_ids": draw_segment_ids(jax.random.fold_in(keys[15], 71), 0),
        "page_groups": place_ends(jax.random.randint(keys[5], (PAGES,), 0, LANGS), jax.random.fold_in(keys[5], 1), 0, LANGS - 1).astype(jnp.int32),
        "lang_table": scatter_about(keys[6], (LAYERS, LANGS * D), 0.5, 3.0, ((1, 32),)),
        "text_attn": draw_text_attn(jax.random.fold_in(keys[15], 71), 0),
        "text_up": scatter_about(keys[8], (LAYERS, D, FF), D ** -0.5, 0.21875, ((2, 32),)),
        "text_down": scatter_about(keys[9], (LAYERS, FF, D), FF ** -0.5, 0.109375, ((1, 32),)),
        "text_vector": draw_text_vector(jax.random.fold_in(keys[15], 71), 0),
        "layout_attn": draw_layout_attn(jax.random.fold_in(keys[15], 71), 0),
        "layout_up": scatter_about(keys[12], (LAYERS, L, FFL), L ** -0.5, 0.4375, ((2, 32),)),
        "layout_down": scatter_about(keys[13], (LAYERS, FFL, L), FFL ** -0.5, 0.21875, ((1, 32),)),
        "layout_vector": draw_layout_vector(jax.random.fold_in(keys[15], 71), 0),
    }


@jax.custom_vjp
def low(v):
    return lax.optimization_barrier(v.astype(jnp.bfloat16)).astype(jnp.float32)

@jax.custom_vjp
def low_back(v):
    return v

def low_keep(v):
    return (low(v), None)

def low_pass(kept, grad):
    return (grad,)

def back_keep(v):
    return (v, None)

def back_low(kept, grad):
    return (low(grad),)
low.defvjp(low_keep, low_pass)
low_back.defvjp(back_keep, back_low)
EPSILON = 1e-05
MASKED = -1e+30
HIGHEST_PRECISION = lax.Precision.HIGHEST

def product(left, right):
    return jnp.dot(left, right, precision=HIGHEST_PRECISION)

def norm_rows(residual, norm_gain, norm_shift):
    average = lax.optimization_barrier(jnp.mean(residual, axis=-1, keepdims=True))
    centred = residual - average
    variance = lax.optimization_barrier(jnp.mean(centred * centred, axis=-1, keepdims=True))
    return centred * lax.rsqrt(variance + EPSILON) * norm_gain + norm_shift

def unpack(vector, stream_width, hidden_width):
    pieces = [vector[member * stream_width:(member + 1) * stream_width] for member in range(8)]
    return pieces + [vector[8 * stream_width:8 * stream_width + hidden_width]]

def project(stream_low, attn_weight, pieces, block_count):
    stream_width = stream_low.shape[1]
    head_shape = (block_count, stream_low.shape[0] // block_count, H, stream_width // H)
    joined = product(stream_low, attn_weight[:, :3 * stream_width])
    query = low(low_back(joined[:, :stream_width] + pieces[0]))
    keyed = low(low_back(joined[:, stream_width:2 * stream_width]))
    valued = low(low_back(joined[:, 2 * stream_width:] + pieces[1]))
    return (query.reshape(head_shape), keyed.reshape(head_shape), valued.reshape(head_shape))

def attend(probs, valued):
    context = jnp.einsum('bhst,bthd->bshd', probs, valued, precision=HIGHEST_PRECISION)
    return low(low_back(context.reshape(-1, context.shape[2] * context.shape[3])))

def tail(stream_rows, context_rows, attn_weight, up_weight, down_weight, pieces):
    stream_width = stream_rows.shape[1]
    branch = low_back(product(context_rows, attn_weight[:, 3 * stream_width:]) + pieces[2])
    normed = norm_rows(stream_rows + branch, pieces[4], pieces[5])
    upper = low_back(product(low(normed), up_weight) + pieces[8])
    second = low_back(product(low(jax.nn.gelu(upper, approximate=False)), down_weight) + pieces[3])
    return norm_rows(normed + second, pieces[6], pieces[7])

def reference_layer(params, text_rows, layout_rows, onehot_rows, same_page, block_count):
    text_attn, text_up, text_down, text_vector, lang_layer, layout_attn, layout_up, layout_down, layout_vector = params
    text_rows = text_rows + product(onehot_rows, lang_layer.reshape(LANGS, D))
    text_pieces = unpack(text_vector, D, FF)
    layout_pieces = unpack(layout_vector, L, FFL)
    text_heads = project(low(text_rows), text_attn, text_pieces, block_count)
    layout_heads = project(low(layout_rows), layout_attn, layout_pieces, block_count)
    text_part = jnp.einsum('bshd,bthd->bhst', text_heads[0], text_heads[1], precision=HIGHEST_PRECISION)
    layout_part = jnp.einsum('bshd,bthd->bhst', layout_heads[0], layout_heads[1], precision=HIGHEST_PRECISION)
    scores = low_back(text_part * (1.0 / math.sqrt(D // H)) + layout_part * (1.0 / math.sqrt(L // H)))
    scores = jnp.where(same_page[:, None], scores, MASKED)
    probs = low(jax.nn.softmax(scores, axis=-1))
    text_context = attend(probs, text_heads[2])
    layout_context = attend(probs, layout_heads[2])
    text_next = tail(text_rows, text_context, text_attn, text_up, text_down, text_pieces)
    layout_next = tail(layout_rows, layout_context, layout_attn, layout_up, layout_down, layout_pieces)
    return (text_next, layout_next)

def reference(text_input, layout_input, text_cot, layout_cot, segment_ids, page_groups, lang_table, text_attn, text_up, text_down, text_vector, layout_attn, layout_up, layout_down, layout_vector):
    weights = tuple((member.astype(jnp.float32) for member in (text_attn, text_up, text_down, text_vector, lang_table, layout_attn, layout_up, layout_down, layout_vector)))
    block_total = TOKENS // TOK_DEV
    per_step = math.gcd(block_total, max(1, 4096 // TOK_DEV))
    step_count = block_total // per_step
    step_rows = per_step * TOK_DEV
    token_group = page_groups[segment_ids]
    onehot = (token_group[:, None] == jnp.arange(LANGS, dtype=jnp.int32)[None, :]).astype(jnp.float32)

    def forward(params, text_rows, layout_rows, onehot_rows, page_rows):
        page_blocks = page_rows.reshape(per_step, TOK_DEV)
        same_page = page_blocks[:, :, None] == page_blocks[:, None, :]
        for layer_index in range(LAYERS):
            layer_params = tuple((member[layer_index] for member in params))
            text_rows, layout_rows = reference_layer(layer_params, text_rows, layout_rows, onehot_rows, same_page, per_step)
        return (text_rows, layout_rows)

    def advance(totals, inputs):
        text_rows, layout_rows, text_grad_out, layout_grad_out, onehot_rows, page_rows = inputs

        def local_forward(params, text_start, layout_start):
            return forward(params, text_start, layout_start, onehot_rows, page_rows)
        outputs, pullback = jax.vjp(local_forward, weights, text_rows, layout_rows)
        grad_params, grad_text, grad_layout = pullback((text_grad_out, layout_grad_out))
        totals = jax.tree.map(jnp.add, totals, grad_params)
        return (totals, (outputs[0], outputs[1], grad_text, grad_layout))
    inputs = (text_input.astype(jnp.float32).reshape(step_count, step_rows, D), layout_input.astype(jnp.float32).reshape(step_count, step_rows, L), text_cot.astype(jnp.float32).reshape(step_count, step_rows, D), layout_cot.astype(jnp.float32).reshape(step_count, step_rows, L), onehot.reshape(step_count, step_rows, LANGS), segment_ids.reshape(step_count, step_rows))
    starting = jax.tree.map(jnp.zeros_like, weights)
    totals, stacked = lax.scan(advance, starting, inputs)
    return (stacked[0].reshape(TOKENS, D), stacked[1].reshape(TOKENS, L), stacked[2].reshape(TOKENS, D), stacked[3].reshape(TOKENS, L), totals[0], totals[1], totals[2], totals[3], totals[4], totals[5], totals[6], totals[7], totals[8])
```

```python
import functools
import math
from types import SimpleNamespace

import jax
import jax.numpy as jnp
from jax import lax
from jax.experimental import pallas as pl
from jax.experimental.pallas import tpu as pltpu
from jax.sharding import PartitionSpec as P

H = 12
LANGS = 8


EPSILON = 1e-05
MASKED = -1e30


def norm_rows(residual, norm_gain, norm_shift):
    average = jnp.mean(residual, axis=-1, keepdims=True)
    centred = residual - average
    variance = jnp.mean(centred * centred, axis=-1, keepdims=True)
    return centred * lax.rsqrt(variance + EPSILON) * norm_gain + norm_shift


def exact_gelu(values):
    return jax.nn.gelu(values, approximate=False)


def norm_back(residual, norm_gain, norm_shift, grad_rows):
    unused, pullback = jax.vjp(norm_rows, residual, norm_gain, norm_shift)
    return pullback(grad_rows)


def gelu_back(upper, grad_rows):
    unused, pullback = jax.vjp(exact_gelu, upper)
    return pullback(grad_rows)[0]


def column_sum(matrix):
    return jnp.sum(matrix.astype(jnp.float32), axis=0)


def unpack(vector, stream_width, hidden_width):
    values = vector.astype(jnp.float32)
    pieces = [values[member * stream_width : (member + 1) * stream_width] for member in range(8)]
    return pieces + [values[8 * stream_width : 8 * stream_width + hidden_width]]


def project(stream_low, attn_weight, pieces):
    stream_width = stream_low.shape[1]
    joined = jnp.dot(
        stream_low, attn_weight[:, : 3 * stream_width], preferred_element_type=jnp.float32
    )
    head_shape = (stream_low.shape[0], H, stream_width // H)
    query = (joined[:, :stream_width] + pieces[0]).astype(jnp.bfloat16).reshape(head_shape)
    keyed = joined[:, stream_width : 2 * stream_width].astype(jnp.bfloat16).reshape(head_shape)
    valued = (joined[:, 2 * stream_width :] + pieces[1]).astype(jnp.bfloat16).reshape(head_shape)
    return (query, keyed, valued)


def joint_scores(text_heads, layout_heads, same_page):
    text_part = jnp.einsum(
        "shd,thd->hst", text_heads[0], text_heads[1], preferred_element_type=jnp.float32
    )
    layout_part = jnp.einsum(
        "shd,thd->hst", layout_heads[0], layout_heads[1], preferred_element_type=jnp.float32
    )
    combined = text_part * (1.0 / math.sqrt(text_heads[0].shape[2])) + layout_part * (
        1.0 / math.sqrt(layout_heads[0].shape[2])
    )
    return jnp.where(same_page[None], combined, MASKED)


def attend(probs_low, valued):
    context = jnp.einsum("hst,thd->shd", probs_low, valued, preferred_element_type=jnp.float32)
    return context.reshape(context.shape[0], -1).astype(jnp.bfloat16)


def tail_forward(stream_rows, context_low, attn_weight, up_weight, down_weight, pieces):
    stream_width = stream_rows.shape[1]
    branch = (
        jnp.dot(context_low, attn_weight[:, 3 * stream_width :], preferred_element_type=jnp.float32)
        + pieces[2]
    )
    first_sum = stream_rows + branch
    normed = norm_rows(first_sum, pieces[4], pieces[5])
    normed_low = normed.astype(jnp.bfloat16)
    upper = jnp.dot(normed_low, up_weight, preferred_element_type=jnp.float32) + pieces[8]
    active_low = exact_gelu(upper).astype(jnp.bfloat16)
    second_sum = (
        normed + jnp.dot(active_low, down_weight, preferred_element_type=jnp.float32) + pieces[3]
    )
    result = norm_rows(second_sum, pieces[6], pieces[7])
    return (result, (first_sum, normed_low, upper, active_low, second_sum))


def layer_forward(text_rows, layout_rows, text_weights, layout_weights, same_page, onehot):
    group_table = text_weights[4].astype(jnp.float32).reshape(onehot.shape[1], -1)
    text_rows = text_rows + jnp.dot(onehot, group_table, precision=lax.Precision.HIGHEST)
    text_pieces = unpack(text_weights[3], text_rows.shape[1], text_weights[1].shape[1])
    layout_pieces = unpack(layout_weights[3], layout_rows.shape[1], layout_weights[1].shape[1])
    text_low = text_rows.astype(jnp.bfloat16)
    layout_low = layout_rows.astype(jnp.bfloat16)
    text_heads = project(text_low, text_weights[0], text_pieces)
    layout_heads = project(layout_low, layout_weights[0], layout_pieces)
    scores = joint_scores(text_heads, layout_heads, same_page)
    row_peak = jnp.max(scores, axis=-1, keepdims=True)
    log_total = row_peak + jnp.log(jnp.sum(jnp.exp(scores - row_peak), axis=-1, keepdims=True))
    probs_low = jnp.exp(scores - log_total).astype(jnp.bfloat16)
    text_context = attend(probs_low, text_heads[2])
    layout_context = attend(probs_low, layout_heads[2])
    text_next, text_stored = tail_forward(
        text_rows, text_context, text_weights[0], text_weights[1], text_weights[2], text_pieces
    )
    layout_next, layout_stored = tail_forward(
        layout_rows,
        layout_context,
        layout_weights[0],
        layout_weights[1],
        layout_weights[2],
        layout_pieces,
    )
    stored = (
        text_low,
        layout_low,
        text_heads,
        layout_heads,
        log_total,
        text_context,
        layout_context,
        text_stored,
        layout_stored,
    )
    return (text_next, layout_next, stored)


def tail_backward(grad_result, stored, context_low, attn_weight, up_weight, down_weight, pieces):
    first_sum, normed_low, upper, active_low, second_sum = stored
    stream_width = first_sum.shape[1]
    grad_second, grad_gain_two, grad_shift_two = norm_back(
        second_sum, pieces[6], pieces[7], grad_result
    )
    grad_down_low = grad_second.astype(jnp.bfloat16)
    grad_down_bias = column_sum(grad_down_low)
    grad_down = jnp.einsum(
        "sf,sd->fd", active_low, grad_down_low, preferred_element_type=jnp.float32
    )
    grad_active = jnp.einsum(
        "sd,fd->sf", grad_down_low, down_weight, preferred_element_type=jnp.float32
    )
    grad_upper_low = gelu_back(upper, grad_active).astype(jnp.bfloat16)
    grad_up_bias = column_sum(grad_upper_low)
    grad_up = jnp.einsum(
        "sd,sf->df", normed_low, grad_upper_low, preferred_element_type=jnp.float32
    )
    grad_normed = grad_second + jnp.einsum(
        "sf,df->sd", grad_upper_low, up_weight, preferred_element_type=jnp.float32
    )
    grad_first, grad_gain_one, grad_shift_one = norm_back(
        first_sum, pieces[4], pieces[5], grad_normed
    )
    grad_branch_low = grad_first.astype(jnp.bfloat16)
    grad_out_bias = column_sum(grad_branch_low)
    output_weight = attn_weight[:, 3 * stream_width :]
    grad_output_proj = jnp.einsum(
        "sd,se->de", context_low, grad_branch_low, preferred_element_type=jnp.float32
    )
    grad_context = jnp.einsum(
        "se,de->sd", grad_branch_low, output_weight, preferred_element_type=jnp.float32
    ).astype(jnp.bfloat16)
    matrices = (grad_output_proj, grad_up, grad_down)
    vectors = (
        grad_out_bias,
        grad_down_bias,
        grad_gain_one,
        grad_shift_one,
        grad_gain_two,
        grad_shift_two,
        grad_up_bias,
    )
    return (grad_first, grad_context, matrices, vectors)


def head_grads(head_set, grad_context_low, probs_low, grad_scores_low):
    inverse_root = 1.0 / math.sqrt(head_set[0].shape[2])
    grad_heads = grad_context_low.reshape(head_set[2].shape)
    grad_query = (
        jnp.einsum("hst,thd->shd", grad_scores_low, head_set[1], preferred_element_type=jnp.float32)
        * inverse_root
    )
    grad_key = (
        jnp.einsum("hst,shd->thd", grad_scores_low, head_set[0], preferred_element_type=jnp.float32)
        * inverse_root
    )
    grad_value = jnp.einsum(
        "hst,shd->thd", probs_low, grad_heads, preferred_element_type=jnp.float32
    )
    row_count = head_set[0].shape[0]
    joined = jnp.concatenate(
        [
            grad_query.reshape(row_count, -1),
            grad_key.reshape(row_count, -1),
            grad_value.reshape(row_count, -1),
        ],
        axis=1,
    )
    return joined.astype(jnp.bfloat16)


def attention_backward(
    text_heads, layout_heads, log_total, same_page, grad_text_context, grad_layout_context
):
    scores = joint_scores(text_heads, layout_heads, same_page)
    probs = jnp.exp(scores - log_total)
    probs_low = probs.astype(jnp.bfloat16)
    grad_text_heads = grad_text_context.reshape(text_heads[2].shape)
    grad_layout_heads = grad_layout_context.reshape(layout_heads[2].shape)
    grad_probs = jnp.einsum(
        "shd,thd->hst", grad_text_heads, text_heads[2], preferred_element_type=jnp.float32
    )
    grad_probs = grad_probs + jnp.einsum(
        "shd,thd->hst", grad_layout_heads, layout_heads[2], preferred_element_type=jnp.float32
    )
    inner = jnp.sum(grad_probs * probs, axis=-1, keepdims=True)
    grad_scores_low = (probs * (grad_probs - inner)).astype(jnp.bfloat16)
    text_joined = head_grads(text_heads, grad_text_context, probs_low, grad_scores_low)
    layout_joined = head_grads(layout_heads, grad_layout_context, probs_low, grad_scores_low)
    return (text_joined, layout_joined)


def head_backward(stream_low, grad_joined_low, attn_weight, grad_first, matrices, vectors):
    stream_width = stream_low.shape[1]
    grad_in_proj = jnp.einsum(
        "sd,se->de", stream_low, grad_joined_low, preferred_element_type=jnp.float32
    )
    grad_bias_query = column_sum(grad_joined_low[:, :stream_width])
    grad_bias_value = column_sum(grad_joined_low[:, 2 * stream_width :])
    grad_stream = grad_first + jnp.einsum(
        "se,de->sd",
        grad_joined_low,
        attn_weight[:, : 3 * stream_width],
        preferred_element_type=jnp.float32,
    )
    grad_attn = jnp.concatenate([grad_in_proj, matrices[0]], axis=1)
    grad_vector = jnp.concatenate([grad_bias_query, grad_bias_value] + list(vectors))
    return (grad_stream, (grad_attn, matrices[1], matrices[2], grad_vector))


def layer_backward(grad_text, grad_layout, stored, text_weights, layout_weights, same_page, onehot):
    (
        text_low,
        layout_low,
        text_heads,
        layout_heads,
        log_total,
        text_context,
        layout_context,
        text_stored,
        layout_stored,
    ) = stored
    text_pieces = unpack(text_weights[3], text_low.shape[1], text_weights[1].shape[1])
    layout_pieces = unpack(layout_weights[3], layout_low.shape[1], layout_weights[1].shape[1])
    text_first, grad_text_context, text_mats, text_vecs = tail_backward(
        grad_text,
        text_stored,
        text_context,
        text_weights[0],
        text_weights[1],
        text_weights[2],
        text_pieces,
    )
    layout_first, grad_layout_context, layout_mats, layout_vecs = tail_backward(
        grad_layout,
        layout_stored,
        layout_context,
        layout_weights[0],
        layout_weights[1],
        layout_weights[2],
        layout_pieces,
    )
    text_joined, layout_joined = attention_backward(
        text_heads, layout_heads, log_total, same_page, grad_text_context, grad_layout_context
    )
    grad_text_in, text_terms = head_backward(
        text_low, text_joined, text_weights[0], text_first, text_mats, text_vecs
    )
    grad_layout_in, layout_terms = head_backward(
        layout_low, layout_joined, layout_weights[0], layout_first, layout_mats, layout_vecs
    )
    grad_group = jnp.einsum(
        "sg,sd->gd", onehot, grad_text_in, precision=lax.Precision.HIGHEST
    ).reshape(-1)
    return (grad_text_in, grad_layout_in, text_terms + (grad_group,), layout_terms)


def fetch_layer(
    text_attn,
    text_up,
    text_down,
    text_vector,
    lang_table,
    layout_attn,
    layout_up,
    layout_down,
    layout_vector,
    layer_index,
):
    fetched = (
        lax.all_gather(text_attn[layer_index], AXES, axis=1, tiled=True),
        lax.all_gather(text_up[layer_index], AXES, axis=1, tiled=True),
        lax.all_gather(text_down[layer_index], AXES, axis=0, tiled=True),
        lax.all_gather(text_vector[layer_index], AXES, axis=0, tiled=True),
        lax.all_gather(lang_table[layer_index], AXES, axis=0, tiled=True),
        lax.all_gather(layout_attn[layer_index], AXES, axis=1, tiled=True),
        lax.all_gather(layout_up[layer_index], AXES, axis=1, tiled=True),
        lax.all_gather(layout_down[layer_index], AXES, axis=0, tiled=True),
        lax.all_gather(layout_vector[layer_index], AXES, axis=0, tiled=True),
    )
    return (fetched[:5], fetched[5:])


def fetch_layer_back(
    text_attn,
    text_up,
    text_down,
    text_vector,
    lang_table,
    layout_attn,
    layout_up,
    layout_down,
    layout_vector,
    layer_index,
):
    fetched = (
        lax.all_gather(text_attn[layer_index], AXES, axis=1, tiled=True),
        lax.all_gather(text_up[layer_index], AXES, axis=1, tiled=True),
        lax.all_gather(text_down[layer_index], AXES, axis=0, tiled=True),
        lax.all_gather(text_vector[layer_index], AXES, axis=0, tiled=True),
        lax.all_gather(lang_table[layer_index], AXES, axis=0, tiled=True),
        lax.all_gather(layout_attn[layer_index], AXES, axis=1, tiled=True),
        lax.all_gather(layout_up[layer_index], AXES, axis=1, tiled=True),
        lax.all_gather(layout_down[layer_index], AXES, axis=0, tiled=True),
        lax.all_gather(layout_vector[layer_index], AXES, axis=0, tiled=True),
    )
    return (fetched[:5], fetched[5:])


def generic_shards(
    text_input,
    layout_input,
    text_cot,
    layout_cot,
    segment_ids,
    page_groups,
    lang_table,
    text_attn,
    text_up,
    text_down,
    text_vector,
    layout_attn,
    layout_up,
    layout_down,
    layout_vector,
):
    layer_count = text_attn.shape[0]
    same_page = segment_ids[:, None] == segment_ids[None, :]
    page_slot = segment_ids % 2
    token_group = jnp.where(page_slot == 0, page_groups[0], page_groups[1])
    onehot = (token_group[:, None] == jnp.arange(LANGS, dtype=jnp.int32)[None, :]).astype(
        jnp.float32
    )
    text_rows = text_input.astype(jnp.float32)
    layout_rows = layout_input.astype(jnp.float32)
    saved_layers = []
    for layer_index in range(layer_count):
        text_fetched, layout_fetched = fetch_layer(
            text_attn,
            text_up,
            text_down,
            text_vector,
            lang_table,
            layout_attn,
            layout_up,
            layout_down,
            layout_vector,
            layer_index,
        )
        text_rows, layout_rows, stored = layer_forward(
            text_rows, layout_rows, text_fetched, layout_fetched, same_page, onehot
        )
        saved_layers.append(stored)
    grad_text = text_cot.astype(jnp.float32)
    grad_layout = layout_cot.astype(jnp.float32)
    owned_all = [None] * layer_count
    for layer_index in reversed(range(layer_count)):
        text_fetched, layout_fetched = fetch_layer_back(
            text_attn,
            text_up,
            text_down,
            text_vector,
            lang_table,
            layout_attn,
            layout_up,
            layout_down,
            layout_vector,
            layer_index,
        )
        grad_text, grad_layout, text_terms, layout_terms = layer_backward(
            grad_text,
            grad_layout,
            saved_layers[layer_index],
            text_fetched,
            layout_fetched,
            same_page,
            onehot,
        )
        joined_terms = tuple(text_terms) + tuple(layout_terms)
        owned_all[layer_index] = (
            lax.psum_scatter(joined_terms[0], AXES, scatter_dimension=1, tiled=True),
            lax.psum_scatter(joined_terms[1], AXES, scatter_dimension=1, tiled=True),
            lax.psum_scatter(joined_terms[2], AXES, scatter_dimension=0, tiled=True),
            lax.psum_scatter(joined_terms[3], AXES, scatter_dimension=0, tiled=True),
            lax.psum_scatter(joined_terms[4], AXES, scatter_dimension=0, tiled=True),
            lax.psum_scatter(joined_terms[5], AXES, scatter_dimension=1, tiled=True),
            lax.psum_scatter(joined_terms[6], AXES, scatter_dimension=1, tiled=True),
            lax.psum_scatter(joined_terms[7], AXES, scatter_dimension=0, tiled=True),
            lax.psum_scatter(joined_terms[8], AXES, scatter_dimension=0, tiled=True),
        )
    stacks = [jnp.stack([owned[member] for owned in owned_all]) for member in range(9)]
    return (
        text_rows,
        layout_rows,
        grad_text,
        grad_layout,
        stacks[0],
        stacks[1],
        stacks[2],
        stacks[3],
        stacks[4],
        stacks[5],
        stacks[6],
        stacks[7],
        stacks[8],
    )


MESH = pl.DeviceIdType.MESH
AXES = ("dp", "shard")
ANY = pl.BlockSpec(memory_space=pl.ANY)
IN_VMEM = pl.BlockSpec(memory_space=pltpu.VMEM)
PLANE = 4
SUBLANES = 8
VECTOR_ROWS = 32


def fits_blocks(mesh):
    return mesh.shape[AXES[0]] == PLANE and mesh.shape[AXES[1]] == 2 * PLANE


def place(depth):
    dp, shard = lax.axis_index(AXES[0]), lax.axis_index(AXES[1])
    core, level = lax.rem(shard, 2), shard // 2
    dx = dp + 1 - 2 * lax.rem(dp, 2)
    dy = lax.rem(dp + 2, PLANE)
    me = dp * (2 * depth) + shard
    at = SimpleNamespace(dp=dp, z=level, core=core, dx=dx, dy=dy, dd=PLANE - 1 - dp, me=me)

    def device(plane_index, shard_index):
        return dict(zip(AXES, (plane_index, shard_index)))

    devices = SimpleNamespace(
        x=device(dx, shard),
        y=device(dy, shard),
        up=device(dp, lax.rem(shard + 2, 2 * depth)),
        down=device(dp, lax.rem(shard + 2 * depth - 2, 2 * depth)),
        far=device(dp, lax.rem(shard + depth, 2 * depth)),
        pair=device(dp, 2 * (level + 1 - 2 * lax.rem(level, 2)) + core),
        core=device(dp, shard + 1 - 2 * core),
    )
    return at, devices


def signal(devices):
    barrier = pltpu.get_barrier_semaphore()
    partners = (devices.x, devices.y, devices.up, devices.down, devices.far, devices.core)
    for partner in partners:
        pl.semaphore_signal(barrier, inc=1, device_id=partner, device_id_type=MESH)


def greeted():
    pl.semaphore_wait(pltpu.get_barrier_semaphore(), 6)


def remote(source, target, send_sem, recv_sem, device):
    return pltpu.make_async_remote_copy(
        src_ref=source,
        dst_ref=target,
        send_sem=send_sem,
        recv_sem=recv_sem,
        device_id=device,
        device_id_type=MESH,
    )


class AllSum:
    STEPS = 5

    def __init__(self, devices, running, held, landed, send_sem, recv_sem):
        self.partners = (devices.core, devices.pair, devices.far, devices.x, devices.y)
        self.running, self.held, self.landed = running, held, landed
        self.send_sem, self.recv_sem = send_sem, recv_sem

    def copy(self, step):
        return remote(
            self.held.at[step],
            self.landed.at[step],
            self.send_sem.at[step],
            self.recv_sem.at[step],
            self.partners[step],
        )

    def send(self, step):
        self.held[step] = self.running[...].astype(self.held.dtype)
        self.copy(step).start()

    def advance(self, step):
        self.copy(step).wait_recv()
        self.running[...] += self.landed[step].astype(jnp.float32)
        if step + 1 < self.STEPS:
            self.send(step + 1)

    def close(self):
        for step in range(self.STEPS):
            self.copy(step).wait_send()

    @classmethod
    def scratch(cls, shape):
        return [
            pltpu.VMEM((cls.STEPS,) + shape, jnp.bfloat16),
            pltpu.VMEM((cls.STEPS,) + shape, jnp.bfloat16),
            pltpu.SemaphoreType.DMA((cls.STEPS,)),
            pltpu.SemaphoreType.DMA((cls.STEPS,)),
        ]


class Plan:
    LAG = dict(x=1.8, z=1.8, c=1.0, h=0.3)
    PATIENCE = 1.0

    def __init__(self):
        self.tasks = []

    def add(self, name, run, after=(), needs=(), sends=(), time=0.2, rank=0, patient=False):
        self.tasks.append((name, run, tuple(after), tuple(needs), tuple(sends), time, rank, patient))

    def order(self):
        now, free, landed, done = 0.0, {}, {}, set()
        waiting, result = list(self.tasks), []
        while waiting:
            best = None
            for place_in_list, task in enumerate(waiting):
                name, run, after, needs, sends, time, rank, patient = task
                if any(other not in done for other in after):
                    continue
                if any(event not in landed for event in needs):
                    continue
                start = max([now] + [landed[event] for event in needs])
                key = (start + (self.PATIENCE if patient else 0.0), rank, place_in_list)
                if best is None or key < best[0]:
                    best = (key, task, start)
            assert best is not None
            task, start = best[1:]
            waiting.remove(task)
            result.append(task)
            name, run, after, needs, sends, time, rank, patient = task
            now = start + time
            done.add(name)
            for link, amount, event in sends:
                free[link] = max(now, free.get(link, 0.0)) + amount
                landed[event] = free[link] + self.LAG[link[0]]
        return result

    def run(self):
        for task in self.order():
            task[1]()


UNIT_ROWS_PER_US = 96 / 3.26


def add_rows(target, term):
    total = target[...].astype(jnp.float32) + term[...].astype(jnp.float32)
    target[...] = total.astype(target.dtype)


def add_units(target, *terms):
    def body(index, carry):
        total = target[index].astype(jnp.float32)
        for term in terms:
            total = total + term[index].astype(jnp.float32)
        target[index] = total.astype(target.dtype)
        return carry

    lax.fori_loop(0, target.shape[0], body, 0)


LANE = 128
PAD = 256
PIECE_ROWS = 12
TABLE_ROW = 12
SMALL_ROW = 20
SMALL_HIDDEN_ROW = 28


def dot_nt(left, right):
    return lax.dot_general(
        left, right, (((1,), (1,)), ((), ())), preferred_element_type=jnp.float32
    )


def dot_nn(left, right):
    return jnp.dot(left, right, preferred_element_type=jnp.float32)


def lane_of(shape):
    return lax.broadcasted_iota(jnp.int32, shape, len(shape) - 1)


def unit_rows(ref, dp):
    block = ref[dp]
    return block.reshape(-1, block.shape[-1])


def standard(residual, width):
    padded = residual.shape[1] != width
    average = jnp.sum(residual, axis=1, keepdims=True) * (1.0 / width)
    centred = residual - average
    if padded:
        centred = jnp.where(lane_of(residual.shape) < width, centred, 0.0)
    variance = jnp.sum(centred * centred, axis=1, keepdims=True) * (1.0 / width)
    scale = lax.rsqrt(variance + EPSILON)
    return centred * scale, scale


def gelu_parts(upper):
    cdf = 0.5 * (1.0 + lax.erf(upper * math.sqrt(0.5)))
    density = jnp.exp(upper * upper * -0.5) * (1.0 / math.sqrt(2.0 * math.pi))
    return upper * cdf, cdf + upper * density


def natural_rows(span, step):
    row = lax.broadcasted_iota(jnp.int32, (PAD, PAD), 0)
    column = lax.broadcasted_iota(jnp.int32, (PAD, PAD), 1)
    unit = jnp.zeros((PAD, PAD), jnp.int32)
    for n in range(1, PAD // step):
        unit = unit + jnp.where(row >= n * span, 1, 0)
    source = unit * step + row - unit * span
    return jnp.where((source == column) & (row < (PAD // step) * span), 1.0, 0.0)


def saved_shapes(layers, tokens, width, narrow_hidden):
    low, full = jnp.bfloat16, jnp.float32
    hidden = 4 * width
    return dict(
        low=((layers, 3, tokens, width), low),
        low_small=((layers, 3, tokens, PAD), low),
        heads=((layers, 3, tokens, width), low),
        heads_small=((layers, 3, tokens, PAD), low),
        probs=((layers, H, tokens, tokens), full),
        norm=((layers, 2, tokens, width), full),
        norm_small=((layers, 2, tokens, PAD), full),
        scales=((layers, 4, tokens, LANE), full),
        slope=((layers, tokens, hidden), full),
        slope_small=((layers, tokens, narrow_hidden), full),
        turned=((layers, hidden, tokens), low),
        turned_small=((layers, narrow_hidden, tokens), low),
        small_attn=((layers, 4, PAD, PAD), low),
        small_ff=((layers, 2, narrow_hidden, PAD), low),
    )


SAVED = tuple(saved_shapes(1, 1, 1, 1))


def forward_steps(layer, m, narrow, span):
    tokens, width = m.x.shape
    low = jnp.bfloat16
    vec = lambda row, count=1: m.vectors[pl.ds(layer * VECTOR_ROWS + row, count), :]
    small_vec = lambda row: vec(SMALL_ROW + row)[:, :PAD]

    def embed():
        rows = m.x[...]
        for group in range(LANGS):
            rows = rows + m.onehot[:, group : group + 1] * vec(TABLE_ROW + group)
        m.x[...] = rows
        m.low[layer, 0] = rows.astype(low)
        m.low_small[layer, 0] = m.y[...].astype(low)

    def project_text():
        def body(part, carry):
            joined = dot_nt(m.low[layer, 0], unit_rows(m.attn_w, part))
            bias = jnp.where(part == 0, vec(0), jnp.where(part == 2, vec(1), 0.0))
            m.heads[layer, part] = (joined + bias).astype(low)
            return carry

        lax.fori_loop(0, 3, body, 0)

    def prepare_small():
        permute = natural_rows(span, m.small_raw.shape[3] // m.small_raw_layers).astype(low)
        step = m.small_raw.shape[3] // m.small_raw_layers

        def body(block, carry):
            for member in range(3):
                raw = m.small_raw[
                    block, :, :, pl.ds(layer * step, step), pl.ds(member * PAD, PAD)
                ].reshape(PAD, PAD)
                rows = dot_nn(permute, raw).astype(low)
                if member == 0:
                    m.small_attn[layer, block] = rows
                else:
                    start = pl.multiple_of(block * narrow, 64)
                    m.small_ff[layer, member - 1, pl.ds(start, narrow), :] = rows[:narrow]
            return carry

        lax.fori_loop(0, PLANE, body, 0)

    def project_small():
        for part in range(3):
            joined = dot_nt(m.low_small[layer, 0], m.small_attn[layer, part])
            if part == 0:
                joined = joined + small_vec(0)
            if part == 2:
                joined = joined + small_vec(1)
            m.heads_small[layer, part] = joined.astype(low)
        m.mixed[...] = jnp.zeros_like(m.mixed)

    def attend_pairs(first, count):
        def body(pair, carry):
            lanes = pl.ds(pl.multiple_of(pair * LANE, LANE), LANE)
            query, keyed, valued = (m.heads[layer, n, :, lanes] for n in range(3))
            small_query, small_keyed, small_valued = (m.heads_small[layer, n] for n in range(3))
            lane, small_lane = lane_of((1, LANE)), lane_of((1, PAD))
            same = m.same[...] > 0.0
            contexts = []
            for side in range(2):
                head = 2 * pair + side
                chosen = (lane >= 64 * side) & (lane < 64 * side + 64)
                small_chosen = (small_lane >= 16 * head) & (small_lane < 16 * head + 16)
                mask = jnp.where(chosen, 0.125, 0.0).astype(low)
                small_mask = jnp.where(small_chosen, 0.25, 0.0).astype(low)
                scores = dot_nt(query * mask, keyed) + dot_nt(small_query * small_mask, small_keyed)
                scores = jnp.where(same, scores, MASKED)
                peak = jnp.max(scores, axis=1, keepdims=True)
                powers = jnp.exp(scores - peak)
                probs = powers * (1.0 / jnp.sum(powers, axis=1, keepdims=True))
                m.probs[layer, head] = probs
                probs_low = probs.astype(low)
                contexts.append(dot_nn(probs_low, valued))
                m.mixed[...] += jnp.where(small_chosen, dot_nn(probs_low, small_valued), 0.0)
            m.low[layer, 1, :, lanes] = jnp.where(lane < 64, contexts[0], contexts[1]).astype(low)
            return carry

        lax.fori_loop(first, first + count, body, 0)

    def first_norm():
        m.low_small[layer, 1] = m.mixed[...].astype(low)
        residual = m.x[...] + dot_nt(m.low[layer, 1], unit_rows(m.attn_w, 3)) + vec(2)
        normed, scale = standard(residual, width)
        m.norm[layer, 0] = normed
        m.scales[layer, 0] = jnp.broadcast_to(scale, (tokens, LANE))
        result = normed * vec(4) + vec(5)
        m.normed[...] = result
        m.low[layer, 2] = result.astype(low)

    def first_norm_small():
        branch = dot_nt(m.low_small[layer, 1], m.small_attn[layer, 3]) + small_vec(2)
        normed, scale = standard(m.y[...] + branch, narrow)
        m.norm_small[layer, 0] = normed
        m.scales[layer, 1] = jnp.broadcast_to(scale, (tokens, LANE))
        result = normed * small_vec(4) + small_vec(5)
        m.normed_small[...] = result
        m.low_small[layer, 2] = result.astype(low)

    def activate(column, upper_ref, source, active, slope, turned):
        here = pl.ds(column, LANE)
        value, rate = gelu_parts(upper_ref[:, source])
        slope[layer, :, here] = rate
        value_low = value.astype(low)
        active[:, here] = value_low
        turned[layer, here, :] = value.T.astype(low)

    def up_small():
        m.upper[...] = dot_nt(m.low_small[layer, 2], m.small_ff[layer, 0]) + vec(SMALL_HIDDEN_ROW)

        def body(tile, carry):
            column = pl.multiple_of(tile * LANE, LANE)
            activate(
                column, m.upper, pl.ds(column, LANE), m.active_small, m.slope_small, m.turned_small
            )
            return carry

        lax.fori_loop(0, m.active_small.shape[1] // LANE, body, 0)

    def down_small():
        second = dot_nn(m.active_small[...], m.small_ff[layer, 1]) + small_vec(3)
        normed, scale = standard(m.normed_small[...] + second, narrow)
        m.norm_small[layer, 1] = normed
        m.scales[layer, 3] = jnp.broadcast_to(scale, (tokens, LANE))
        m.y[...] = normed * small_vec(6) + small_vec(7)

    def up_text(first, count):
        def body(block, carry):
            m.upper[...] = dot_nt(m.low[layer, 2], unit_rows(m.up_w, block)) + vec(8 + block)

            def tile_body(tile, inner):
                column = pl.multiple_of(tile * LANE, LANE)
                activate(
                    pl.multiple_of(block * width + column, LANE),
                    m.upper,
                    pl.ds(column, LANE),
                    m.active,
                    m.slope,
                    m.turned,
                )
                return inner

            return lax.fori_loop(0, width // LANE, tile_body, carry)

        lax.fori_loop(first, first + count, body, 0)

    def down_text(first, count):
        def body(block, carry):
            columns = pl.ds(pl.multiple_of(block * width, LANE), width)
            m.second[...] += dot_nn(m.active[:, columns], unit_rows(m.down_w, block))
            return carry

        if first == 0:
            m.second[...] = m.normed[...] + vec(3)
        lax.fori_loop(first, first + count, body, 0)

    def second_norm():
        normed, scale = standard(m.second[...], width)
        m.norm[layer, 1] = normed
        m.scales[layer, 2] = jnp.broadcast_to(scale, (tokens, LANE))
        m.x[...] = normed * vec(6) + vec(7)

    third = H // 6
    after_attn = [(embed, 0.8), (project_text, 1.5)]
    after_small = [(prepare_small, 1.0), (project_small, 0.5)]
    for first in range(0, H // 2, third):
        after_small.append((functools.partial(attend_pairs, first, third), 2.5))
    after_small += [(first_norm, 1.5), (first_norm_small, 0.7), (up_small, 1.5), (down_small, 0.7)]
    after_up = [(functools.partial(up_text, first, 2), 2.5) for first in (0, 2)]
    after_down = [(functools.partial(down_text, first, 2), 1.0) for first in (0, 2)]
    after_down.append((second_norm, 1.0))
    return after_attn, after_small, after_up, after_down


def forward_shapes(layers, depth, tokens, width, narrow, step):
    low, full = jnp.bfloat16, jnp.float32
    span = 4 * width // (PLANE * depth * 2)
    whole = (PLANE, depth, 2, span, width)
    return dict(
        attn_w=(whole, low),
        up_w=(whole, low),
        down_w=(whole, low),
        small_raw=((PLANE, depth, 2, layers * step, width), low),
        own_small=((layers * step, width), low),
        own_small_full=((layers * step, width), full),
        same=((tokens, tokens), full),
        x=((tokens, width), full),
        y=((tokens, PAD), full),
        mixed=((tokens, PAD), full),
        normed=((tokens, width), full),
        normed_small=((tokens, PAD), full),
        upper=((tokens, width), full),
        active=((tokens, 4 * width), low),
        active_small=((tokens, 4 * narrow), low),
        second=((tokens, width), full),
        spread=((3 * SUBLANES, width), full),
    )


FORWARD_SCRATCH = tuple(forward_shapes(1, 1, 1, 1, 1, 1))


def flat_rows(width, narrow):
    rows = [(n, 0, n * width, width) for n in range(PIECE_ROWS)]
    rows += [(TABLE_ROW + n, 1, n * width, width) for n in range(LANGS)]
    rows += [(SMALL_ROW + n, 2, n * narrow, narrow) for n in range(8)]
    return rows + [(SMALL_HIDDEN_ROW, 2, 8 * narrow, 4 * narrow)]


def forward_kernel(depth, layers, narrow, span, *refs):
    refs = list(refs)

    def take(number):
        taken = refs[:number]
        del refs[:number]
        return taken

    count = 3 * layers + 1
    fill = count - 2
    text_attn, text_up, text_down, layout_attn, layout_up, layout_down = take(6)
    pieces = take(3)
    text_in, layout_in, page_row, groups = take(4)
    outs = take(count)
    vector_out, onehot_out, text_out, layout_out = take(4)
    kept = take(len(SAVED))
    own_sem, zs, zr, ps, pr, us, ur, cs, cr, load_sem, keep_sem = take(11)
    all_sum = take(4)
    m = SimpleNamespace()
    for name in SAVED + FORWARD_SCRATCH:
        setattr(m, name, refs.pop(0))
    m.vectors, m.onehot, m.small_raw_layers = vector_out, onehot_out, layers
    at, devices = place(depth)
    dp, z, core, dx, dy, dd = at.dp, at.z, at.core, at.dx, at.dy, at.dd
    half = depth // 2
    low, full = jnp.bfloat16, jnp.float32
    tokens, width = m.x.shape
    step = m.own_small.shape[0] // layers
    vectors = AllSum(devices, vector_out, *all_sum)

    sources = [text_attn.at[0], m.own_small]
    for layer in range(layers):
        if layer > 0:
            sources.append(text_attn.at[layer])
        sources += [text_up.at[layer], text_down.at[layer]]

    def own(k):
        return pltpu.make_async_copy(sources[k], outs[k].at[dp, z, core], own_sem.at[k])

    def line(k, rising, hop, side=0):
        level = z - hop if rising else z + hop
        owner = (dp, dx, dy, dd)[side]
        target = outs[k].at[owner, level, core]
        row = k if side == 0 else count - 1 + side
        return remote(
            sources[k] if hop == 0 and side == 0 else target,
            target,
            zs.at[row, int(rising), hop],
            zr.at[row, level],
            devices.up if rising else devices.down,
        )

    def exists(rising, hop):
        return (z - hop >= 0) if rising else (z + hop < depth)

    def goes_on(rising, hop):
        return exists(rising, hop) & ((z < depth - 1) if rising else (z > 0))

    def unit(rising, hop, to_x):
        level = z - hop if rising else z + hop
        target = outs[0].at[dp, level, core]
        return remote(
            sources[0] if hop == 0 else target,
            target,
            us.at[int(to_x), level],
            ur.at[int(to_x), level],
            devices.x if to_x else devices.y,
        )

    def unit_landed(to_x, level):
        target = outs[0].at[dx if to_x else dy, level, core]
        return remote(
            target, target, us.at[int(to_x), level], ur.at[int(to_x), level], devices.x
        )

    def line_start(k, hop, side=0):
        for rising in (True, False):

            @pl.when(goes_on(rising, hop))
            def start():
                line(k, rising, hop, side).start()

    def line_wait(k, hop, side=0, then=None):
        for rising in (True, False):

            @pl.when(exists(rising, hop))
            def wait():
                line(k, rising, hop, side).wait_recv()
                if then is not None:
                    then(rising, hop)

    def unit_start(rising, hop):
        unit(rising, hop, True).start()
        unit(rising, hop, False).start()

    def plane(k, index, sending=True):
        if k == fill:
            rows = span // 2
            lower, upper = pl.ds(0, rows), pl.ds(rows, rows)
            if sending:
                blocks = ((dp, None), (dp, None), (dx, lower), (dy, upper))
            else:
                blocks = ((dx, None), (dy, None), (dd, lower), (dd, upper))
            owner, rows = blocks[index]
            block = outs[k].at[owner, z, core]
            block = block if rows is None else block.at[rows]
            source = sources[k] if sending and index < 2 else block
        else:
            lower, upper, every = pl.ds(0, half), pl.ds(half, half), pl.ds(0, depth)
            if sending:
                blocks = ((dp, every), (dp, every), (dx, lower), (dy, upper))
            else:
                blocks = ((dx, every), (dy, every), (dd, lower), (dd, upper))
            owner, levels = blocks[index]
            block = outs[k].at[owner, levels, core]
            source = block
        device = (devices.x, devices.y, devices.y, devices.x)[index]
        return remote(source, block, ps.at[k, index], pr.at[k, index], device)

    def across(k, index, side):
        lower, upper, every = pl.ds(0, half), pl.ds(half, half), pl.ds(0, depth)
        if k == fill:
            blocks = ((dp, every), (dx, every), (dy, every), (dd, every))
        else:
            blocks = ((dp, every), (dx, every), (dy, every), (dd, lower), (dd, upper))
        owner, levels = blocks[index]
        block = outs[k].at[owner, levels, side]
        return remote(block, block, cs.at[k, index], cr.at[k, index], devices.core)

    def landed_across(k):
        return range(4 if k == fill else 5)

    held = [m.attn_w, m.small_raw, m.up_w, m.down_w] + [m.attn_w, m.up_w, m.down_w] * (layers - 1)

    def load(k):
        return pltpu.make_async_copy(outs[k], held[k], load_sem.at[k])

    def keep(index, layer):
        source = getattr(m, SAVED[index])
        return pltpu.make_async_copy(
            source.at[layer], kept[index].at[layer], keep_sem.at[index, layer]
        )

    def keep_layer(layer):
        for index in range(len(SAVED)):
            keep(index, layer).start()

    stages = []
    for layer in range(layers):
        steps = forward_steps(layer, m, narrow, layout_down.shape[1])
        if layer == 0:
            stages += [steps[0], steps[1], steps[2], steps[3]]
        else:
            stages += [steps[0] + steps[1], steps[2], steps[3]]
        stages[-1].append((functools.partial(keep_layer, layer), 0.3))

    def make_small():
        m.own_small_full[...] = jnp.zeros_like(m.own_small_full)
        units = layout_down.shape[1]
        for layer in range(layers):
            rows = pl.ds(layer * step, units)
            m.own_small_full[rows, 0:narrow] = layout_attn[layer].astype(full)
            m.own_small_full[rows, PAD : PAD + narrow] = layout_up[layer].astype(full)
            m.own_small_full[rows, 2 * PAD : 2 * PAD + narrow] = layout_down[layer].astype(full)
        m.own_small[...] = m.own_small_full[...].astype(low)

    def spread_vectors():
        m.spread[...] = jnp.zeros_like(m.spread)
        for n, piece in enumerate(pieces):
            m.spread[pl.ds(SUBLANES * n, layers), 0 : piece.shape[1]] = piece[...].astype(full)
        start = vector_out
        start[...] = jnp.zeros_like(start)
        lane = lane_of((SUBLANES, width))
        for row, n, base, lanes in flat_rows(width, narrow):
            length = pieces[n].shape[1]
            shift = lax.rem(at.me * length - base + 16 * width, width)
            rolled = pltpu.roll(m.spread[pl.ds(SUBLANES * n, SUBLANES), :], shift, 1)
            index = lane + (base - at.me * length)
            inside = (index >= 0) & (index < length) & (lane < lanes)
            rolled = jnp.where(inside, rolled, 0.0)
            for layer in range(layers):
                start[pl.ds(layer * VECTOR_ROWS + row, 1), :] = rolled[layer : layer + 1]
        vectors.send(0)

    def make_masks():
        pages = jnp.broadcast_to(page_row[...].astype(full), (tokens, tokens))
        turned = pages.T
        m.same[...] = jnp.where(pages == turned, 1.0, 0.0)
        group = jnp.where(
            turned == (2 * at.me).astype(full),
            jnp.broadcast_to(groups[:, 0:1], (tokens, tokens)),
            jnp.broadcast_to(groups[:, 1:2], (tokens, tokens)),
        )
        m.onehot[...] = jnp.where(group == lane_of((tokens, tokens)), 1.0, 0.0)

    def take_in():
        m.x[...] = text_in[...].astype(full)
        m.y[...] = jnp.zeros_like(m.y)
        m.y[:, 0:narrow] = layout_in[...].astype(full).T

    def land(k):
        for index in landed_across(k):
            across(k, index, 1 - core).wait_recv()
        load(k).start()

    signal(devices)
    make_small()
    greeted()
    for k in (0, fill, 1):
        own(k).start()
    line_start(0, 0)
    unit_start(True, 0)
    plane(fill, 0).start()
    plane(fill, 1).start()
    for k in range(2, count):
        if k != fill:
            own(k).start()

    plan = Plan()
    chain = [k for k in range(count) if k != fill]
    size = [sources[k].shape[0] / UNIT_ROWS_PER_US for k in range(count)]

    def begin_line(k, side):
        if side == 0:
            own(k).wait()
        if k > 0:
            line_start(k, 0, side)

    def next_line(k, hop, side):
        line_wait(k, hop, side, unit_start if k == 0 else None)
        if hop < depth - 1:
            line_start(k, hop, side)

    def add_line(k, side, after, needs, rank):
        sends = [("z", size[k], ("z", 1, k, side))]
        if k == 0:
            sends.append(("x", size[k], ("u", 0)))
        plan.add(("z", 0, k, side), functools.partial(begin_line, k, side), after, needs, sends, 0.3, rank)
        for hop in range(1, depth):
            sends = []
            if hop < depth - 1:
                sends.append(("z", size[k], ("z", hop + 1, k, side)))
            if k == 0:
                sends.append(("x", size[k], ("u", hop)))
            plan.add(
                ("z", hop, k, side),
                functools.partial(next_line, k, hop, side),
                [("z", hop - 1, k, side)],
                [("z", hop, k, side)],
                sends,
                0.3,
                rank,
            )

    def plane_first(k):
        if k > 0:
            plane(k, 0).start()
            plane(k, 1).start()
        across(k, 0, core).start()

    def plane_second(k):
        for index in (0, 1):
            if k == 0:
                for level in range(depth):
                    unit_landed(index == 0, level).wait_recv()
            else:
                plane(k, index, False).wait_recv()
            plane(k, index + 2).start()
            if k != fill:
                across(k, index + 1, core).start()

    def plane_third(k):
        for index in (2, 3):
            plane(k, index, False).wait_recv()
            if k != fill:
                across(k, index + 1, core).start()

    def cross_fill(side):
        across(fill, side, core).start()

    last = {}
    lines = [(k, 0) for k in chain]
    for side in range(4):
        lines.insert((4, 6, 7, 9)[side], (fill, side))
    for n, (k, side) in enumerate(lines):
        after = [("z", 1) + lines[n - 1]] if n else []
        if k == fill:
            after.append(("p", 2 if side < 3 else 3, fill))
        add_line(k, side, after, [], 10 * n)
    for n, k in enumerate(chain):
        arrive = ("x", k) if k else ("u", depth - 1)
        sends = [("c", 0.4 * size[k], ("c", 0, k))]
        if k:
            sends.append(("x", 4 * size[k], arrive))
        plan.add(("p", 1, k), functools.partial(plane_first, k), [("z", depth - 1, k, 0)], [], sends, 0.2, 10 * n + 1)
        sends = [("x", 2 * size[k], ("d", k)), ("c", 0.8 * size[k], ("c", 1, k))]
        plan.add(("p", 2, k), functools.partial(plane_second, k), [("p", 1, k)], [arrive], sends, 0.2, 10 * n + 2)
        sends = [("c", 0.4 * size[k], ("c", 2, k))]
        plan.add(("p", 3, k), functools.partial(plane_third, k), [("p", 2, k)], [("d", k)], sends, 0.2, 10 * n + 3)
    plan.add(0, lambda: None, sends=[("x", size[fill], ("f", 1))], time=0.0, rank=-1)
    plan.add(
        ("p", 2, fill),
        functools.partial(plane_second, fill),
        [0],
        [("f", 1)],
        [("x", size[fill] / 2, ("f", 2))],
        0.2,
        5,
    )
    plan.add(("p", 3, fill), functools.partial(plane_third, fill), [("p", 2, fill)], [("f", 2)], rank=6)
    for side in range(4):
        plan.add(
            ("a", side),
            functools.partial(cross_fill, side),
            [("z", depth - 1, fill, side)],
            [],
            [("c", 0.4 * size[fill], ("a", side))],
            0.1,
            25 + 10 * side,
        )
    previous = None
    vector_steps = [spread_vectors]
    vector_steps += [functools.partial(vectors.advance, n) for n in range(AllSum.STEPS)]
    for n, step_of in enumerate(vector_steps):
        link, amount = (("c", 0.3), ("z", 2.2), ("z", 6.0), ("x", 2.2), ("x", 2.2), ("h", 0.0))[n]
        sends = [(link, amount, ("v", n))]
        needs = [("v", n - 1)] if n else []
        plan.add(("v", n), step_of, [("v", n - 1)] if n else [], needs, sends, 0.3 if n else 3.0, 2)
    plan.add("i", take_in, [("v", 0)], time=0.7, rank=3)
    plan.add("m", make_masks, ["i"], time=1.0, rank=3)
    previous = [("v", AllSum.STEPS), "m"]
    for k in range(count):
        landed = [("a", side) for side in range(4)] if k == fill else [("c", n, k) for n in range(3)]
        follow = [("a", side) for side in range(4)] if k == fill else [("p", 3, k)]
        if k > 3:
            follow.append(last[k - 3])
        plan.add(("l", k), functools.partial(land, k), follow, landed, [("h", 2.4, ("h", k))], 0.2, 10 * k)
        for n, (closure, time) in enumerate(stages[k]):
            run = closure
            if n == 0:
                run = functools.partial(lambda k, closure: (load(k).wait(), closure()), k, closure)
            plan.add(("s", k, n), run, previous + [("l", k)], [("h", k)], (), time, 1000 + k, True)
            previous = [("s", k, n)]
        last[k] = previous[0]
    plan.run()
    text_out[...] = m.x[...]
    layout_out[...] = m.y[:, 0:narrow].T
    vectors.close()
    for index in range(len(SAVED)):
        for layer in range(layers):
            keep(index, layer).wait()
    for level in range(depth):
        for to_x in (True, False):
            unit_landed(to_x, level).wait_send()
    for k in range(count):
        for index in landed_across(k):
            across(k, index, core).wait_send()
        for index in range(4):
            if k > 0 or index > 1:
                plane(k, index).wait_send()
        for rising in (True, False):
            for hop in range(depth):

                @pl.when(goes_on(rising, hop))
                def drain():
                    for side in range(4 if k == fill else 1):
                        line(k, rising, hop, side).wait_send()


def run_forward(depth, narrow, step, weights, pieces, text_in, layout_in, page_row, groups):
    dma = pltpu.SemaphoreType.DMA
    tokens, width = text_in.shape
    layers, span, unused = weights[0].shape
    count = 3 * layers + 1
    full = jnp.float32
    saved = saved_shapes(layers, tokens, width, 4 * narrow)
    scratch = forward_shapes(layers, depth, tokens, width, narrow, step)
    rows = [span, layers * step] + [span] * (count - 2)
    vector_shape = (layers * VECTOR_ROWS, width)
    results = pl.pallas_call(
        functools.partial(forward_kernel, depth, layers, narrow, span),
        out_shape=[
            jax.ShapeDtypeStruct((PLANE, depth, 2, row, width), weights[0].dtype) for row in rows
        ]
        + [
            jax.ShapeDtypeStruct(vector_shape, full),
            jax.ShapeDtypeStruct((tokens, LANE), full),
            jax.ShapeDtypeStruct((tokens, width), full),
            jax.ShapeDtypeStruct((narrow, tokens), full),
        ]
        + [jax.ShapeDtypeStruct(*saved[name]) for name in SAVED],
        in_specs=[IN_VMEM] * 13,
        out_specs=[ANY] * count + [IN_VMEM] * 4 + [ANY] * len(SAVED),
        scratch_shapes=[
            dma((count,)),
            dma((count + 3, 2, depth)),
            dma((count + 3, depth)),
            dma((count, 4)),
            dma((count, 4)),
            dma((2, depth)),
            dma((2, depth)),
            dma((count, 5)),
            dma((count, 5)),
            dma((count,)),
            dma((len(SAVED), layers)),
        ]
        + AllSum.scratch(vector_shape)
        + [pltpu.VMEM(*saved[name]) for name in SAVED]
        + [pltpu.VMEM(*scratch[name]) for name in FORWARD_SCRATCH],
        compiler_params=pltpu.CompilerParams(
            collective_id=0, has_side_effects=True, vmem_limit_bytes=66000000
        ),
        name="forward_blocks",
    )(*weights, *pieces, text_in, layout_in, page_row, groups)
    return results[:count], results[count : count + 4], results[count + 4 :]


TEXT_MEMBERS = 3
LINKS = 10


def back_shapes(layers, depth, tokens, width, narrow_hidden):
    low, full = jnp.bfloat16, jnp.float32
    span = 4 * width // (PLANE * depth * 2)
    unit = (PLANE, depth, span, LANE)
    whole = (PLANE, depth, 2, span, LANE)
    return dict(
        weights=((2, PLANE, depth, 2, span, width), low),
        gx=((tokens, width), full),
        gy=((tokens, PAD), full),
        down_low=((tokens, width), low),
        down_low_small=((tokens, PAD), low),
        branch_low=((tokens, width), low),
        branch_low_small=((tokens, PAD), low),
        wide=((tokens, width), full),
        upper_low=((tokens, 4 * width), low),
        upper_low_small=((tokens, narrow_hidden), low),
        context=((tokens, width), low),
        context_small=((tokens, PAD), low),
        joined=((3, tokens, width), low),
        mixed=((3, tokens, PAD), full),
        rows_up=(whole, low),
        rows_attn=(whole, low),
        rows_small=((2, narrow_hidden, tokens), low),
        in_land=((layers, 4, tokens, width), low),
        in_land_small=((layers, 4, tokens, PAD), low),
        rows_land=((layers, 3) + unit, low),
        rows_land_small=((layers, 3, narrow_hidden, tokens), low),
        sums=((layers * VECTOR_ROWS, width), full),
    )


BACK_SCRATCH = tuple(back_shapes(1, 1, 1, 1, 1))


def standard_back(grad, normed, scale, gain, width):
    pushed = grad * gain
    average = jnp.sum(pushed, axis=1, keepdims=True) * (1.0 / width)
    along = jnp.sum(pushed * normed, axis=1, keepdims=True) * (1.0 / width)
    result = scale * (pushed - average - normed * along)
    if grad.shape[1] != width:
        result = jnp.where(lane_of(grad.shape) < width, result, 0.0)
    return result, total(grad * normed), total(grad)


def total(rows):
    return jnp.sum(rows.astype(jnp.float32), axis=0, keepdims=True)


def padded_rows_of_core(span, step, core):
    units = PAD // step // 2
    shape = (units * step, units * 2 * span)
    row = lax.broadcasted_iota(jnp.int32, shape, 0)
    column = lax.broadcasted_iota(jnp.int32, shape, 1)
    unit = jnp.zeros(shape, jnp.int32)
    for n in range(1, units):
        unit = unit + jnp.where(row >= n * step, 1, 0)
    inside = row - unit * step
    source = (2 * unit + core) * span + inside
    return jnp.where((source == column) & (inside < span), 1.0, 0.0)


def backward_kernel(depth, layers, narrow, span, step, *refs):
    refs = list(refs)

    def take(number):
        taken = refs[:number]
        del refs[:number]
        return taken

    text_count = TEXT_MEMBERS * layers
    count = (TEXT_MEMBERS + 1) * layers
    gathered = take(text_count)
    kept = take(len(SAVED))
    vec_ref, text_cot, layout_cot, onehot = take(4)
    outs = take(count)
    vector_out, text_out, layout_out = take(3)
    m = SimpleNamespace()
    for name in SAVED + BACK_SCRATCH:
        setattr(m, name, refs.pop(0))
    mine_text, mine_small = take(2)
    landed_diag, landed_plane, landed_line = take(count), take(count), take(count)
    weight_sem, keep_sem, xs, xr, ps, pr, zs, zr = take(8)
    all_sum = take(4)
    at, devices = place(depth)
    dp, z, core, dx, dy, dd = at.dp, at.z, at.core, at.dx, at.dy, at.dd
    fill = 1
    owners = (dp, dx, dy, dd)
    half = depth // 2
    low = jnp.bfloat16
    tokens, width = m.gx.shape
    hidden_small = m.upper_low_small.shape[1]
    signal(devices)
    greeted()
    vectors = AllSum(devices, vector_out, *all_sum)

    slots, reuse = {}, {}
    for k in range(count):
        if k % 4 != 3:
            spare = [n for n in range(mine_text.shape[0]) if n not in slots.values()]
            if spare:
                slots[k] = spare[0]
            else:
                reuse[k] = min(n for n in slots if n != fill and n not in reuse.values())
                slots[k] = slots[reuse[k]]

    def mine(k):
        if k % 4 == 3:
            return mine_small.at[k // 4]
        return mine_text.at[slots[k]]

    order = []
    for layer in reversed(range(layers)):
        order += [3 * layer + 2, 3 * layer + 1, 3 * layer]

    def weight_load(index):
        return pltpu.make_async_copy(
            gathered[order[index]], m.weights.at[index % 2], weight_sem.at[index]
        )

    def saved_load(name, layer):
        index = SAVED.index(name)
        return pltpu.make_async_copy(
            kept[index].at[layer], getattr(m, name), keep_sem.at[index, layer]
        )

    def cross(layer, link):
        moves = (
            (m.low, m.in_land.at[layer, pl.ds(0, 3)]),
            (m.turned.at[:, :, 1 - core], m.rows_land.at[layer, 0]),
            (m.down_low, m.in_land.at[layer, 3]),
            (m.rows_up.at[:, :, 1 - core], m.rows_land.at[layer, 1]),
            (m.rows_attn.at[:, :, 1 - core], m.rows_land.at[layer, 2]),
            (m.low_small, m.in_land_small.at[layer, pl.ds(0, 3)]),
            (m.turned_small, m.rows_land_small.at[layer, 0]),
            (m.down_low_small, m.in_land_small.at[layer, 3]),
            (m.rows_small.at[0], m.rows_land_small.at[layer, 1]),
            (m.rows_small.at[1], m.rows_land_small.at[layer, 2]),
        )
        source, target = moves[link]
        return remote(
            source, target, xs.at[layer, link], xr.at[layer, link], devices.core
        )

    def plane(k, index):
        if k == fill:
            size = landed_diag[k].shape[1]
            lower, upper = pl.ds(0, size), pl.ds(size, size)
            own = lambda owner, rows: mine(k).at[owner, z, rows]
        else:
            lower, upper = pl.ds(0, half), pl.ds(half, half)
            own = lambda owner, levels: mine(k).at[owner, levels]
        diag, direct = landed_diag[k], landed_plane[k]
        moves = (
            (dd, lower, diag.at[0], devices.y),
            (dd, upper, diag.at[1], devices.x),
            (dx, upper, direct.at[0, upper], devices.x),
            (dy, lower, direct.at[1, lower], devices.y),
            (dx, lower, direct.at[0, lower], devices.x),
            (dy, upper, direct.at[1, upper], devices.y),
        )
        owner, part, target, device = moves[index]
        return remote(own(owner, part), target, ps.at[k, index], pr.at[k, index], device)

    def line(k, rising, level, slot, side=0):
        row = k if side == 0 else count - 1 + side
        return remote(
            mine(k).at[owners[side], level],
            landed_line[k].at[slot, side],
            zs.at[row, int(rising), level],
            zr.at[row, int(rising), level],
            devices.up if rising else devices.down,
        )

    def second_sums(k):
        if k == fill:
            size = landed_diag[k].shape[1]
            lower, upper = pl.ds(0, size), pl.ds(size, size)
            one, other = mine(k).at[dx, z, lower], mine(k).at[dy, z, upper]
            add = add_rows
        else:
            one = mine(k).at[dx, pl.ds(0, half)]
            other = mine(k).at[dy, pl.ds(half, half)]
            add = add_units
        plane(k, 0).wait_recv()
        add(one, landed_diag[k].at[0])
        plane(k, 4).start()
        plane(k, 1).wait_recv()
        add(other, landed_diag[k].at[1])
        plane(k, 5).start()

    def third_sums(k):
        for index in (2, 3, 4, 5):
            plane(k, index).wait_recv()
        if k == fill:
            result = mine(k)[dp, z].astype(jnp.float32)
            for side in range(2):
                result = result + landed_plane[k][side].astype(jnp.float32)
            outs[k][...] = result
        else:
            add_units(mine(k).at[dp], landed_plane[k].at[0], landed_plane[k].at[1])
            line_step(k, 0)

    def passed(rising, hop):
        return range(hop + 1, depth) if rising else range(depth - 1 - hop)

    def line_step(k, hop, side=0):
        for rising in (True, False):

            @pl.when(z == (hop if rising else depth - 1 - hop))
            def move():
                for level in passed(rising, hop):
                    if hop > 0:
                        line(k, rising, level, level, side).wait_recv()
                        add_rows(mine(k).at[owners[side], level], landed_line[k].at[level, side])
                    last = rising and level == hop + 1
                    line(k, rising, level, depth if last else level, side).start()

    def last_sums(k, side=0):
        if k != fill:
            outs[k][...] = mine(k)[dp, z].astype(jnp.float32)
        for rising in (True, False):

            @pl.when((z > 0) if rising else (z < depth - 1))
            def add():
                slot = depth if rising else z
                line(k, rising, z, slot, side).wait_recv()
                if k == fill:
                    add_rows(mine(k).at[owners[side], z], landed_line[k].at[slot, side])
                else:
                    outs[k][...] += landed_line[k][slot, side].astype(jnp.float32)

    def fill_plane():
        for index in range(4):
            plane(fill, index).start()

    def drain(k):
        for index in range(6):
            plane(k, index).wait_send()
        for hop in range(depth - 1):
            for rising in (True, False):

                @pl.when(z == (hop if rising else depth - 1 - hop))
                def wait():
                    for level in passed(rising, hop):
                        for side in range(PLANE if k == fill else 1):
                            line(k, rising, level, level, side).wait_send()

    plan = Plan()
    size = [outs[k].shape[0] / UNIT_ROWS_PER_US for k in range(count)]

    def add_scatter(k, rank):
        one = size[k]

        def step(hop, side):
            if hop < depth - 1:
                line_step(k, hop, side)
            else:
                last_sums(k, side)

        for side in range(PLANE if k == fill else 1):
            for hop in range(0 if k == fill else 1, depth):
                sends = []
                if hop < depth - 1:
                    sends.append((("z", hop), (depth - 1 - hop) * one, ("z", hop + 1, k, side)))
                after = [("z", hop - 1, k, side)] if hop else [("o", k)]
                if k != fill and hop == 1:
                    after = [("s", 3, k)]
                if k == fill and hop == 0 and side:
                    after.append(("z", 1, k, side - 1))
                needs = [("z", hop, k, side)] if hop else []
                plan.add(
                    ("z", hop, k, side), functools.partial(step, hop, side), after, needs, sends, 0.3, rank
                )
        first = ("o", k)
        share = 2 * one
        if k == fill:
            first, share = ("f", 0), one / 2
            sends = [("x", share, ("d", k)), ("x", share, ("e", k))]
            ends = [("z", depth - 1, k, side) for side in range(PLANE)]
            plan.add(first, fill_plane, ends, [], sends, 0.2, rank)
        plan.add(
            ("s", 2, k), functools.partial(second_sums, k), [first], [("d", k)], [("x", share, ("g", k))], 0.5, rank
        )
        sends = [(("z", 0), (depth - 1) * one, ("z", 1, k, 0))] if k != fill else []
        plan.add(
            ("s", 3, k), functools.partial(third_sums, k), [("s", 2, k)], [("e", k), ("g", k)], sends, 1.0, rank
        )

    def own_sends(k):
        if k == fill:
            return []
        return [("x", 2 * size[k], ("d", k)), ("x", 2 * size[k], ("e", k))]

    previous = []

    def then(name, run, time, needs=(), sends=(), after=()):
        plan.add(name, run, previous + list(after), needs, sends, time, 1000, True)
        previous[:] = [name]

    def done(k):
        return [("s", 3, k), ("z", depth - 1, k, 0)]

    def own_sums(k, rows, rows_land, ins, ins_land):
        if k in reuse:
            drain(reuse[k])

        def block(owner):
            left = jnp.concatenate(
                [
                    rows[owner, :, core].reshape(-1, tokens),
                    rows_land[owner].reshape(-1, tokens),
                ],
                axis=1,
            )
            right = jnp.concatenate([ins(owner), ins_land(owner)], axis=0)
            result = dot_nn(left, right)
            mine(k)[owner] = result.astype(low).reshape(depth, -1, width)

        block(dd)
        if k == fill:
            for owner in (dx, dy, dp):
                block(owner)
            return
        plane(k, 0).start()
        plane(k, 1).start()
        block(dx)
        plane(k, 2).start()
        block(dy)
        plane(k, 3).start()
        block(dp)

    m.gx[...] = text_cot[...].astype(jnp.float32)
    m.gy[...] = jnp.zeros_like(m.gy)
    m.gy[:, 0:narrow] = layout_cot[...].astype(jnp.float32).T
    first_names = ("norm", "scales", "turned", "norm_small", "turned_small", "slope", "low")
    names = first_names + tuple(name for name in SAVED if name not in first_names)
    weight_load(0).start()
    for name in names:
        saved_load(name, layers - 1).start()
    weight_load(1).start()

    def add_layer(turn, layer):
        k = 4 * turn
        vec = lambda row, n=1: vec_ref[pl.ds(layer * VECTOR_ROWS + row, n), :]
        small_vec = lambda row: vec(SMALL_ROW + row)[:, :PAD]
        slot = lambda member: m.weights.at[(3 * turn + member) % 2]

        def put(row, value):
            m.sums[pl.ds(layer * VECTOR_ROWS + row, 1), :] = value

        def put_small(row, value):
            m.sums[pl.ds(layer * VECTOR_ROWS + SMALL_ROW + row, 1), :PAD] = value


        def tail():
            m.sums[pl.ds(layer * VECTOR_ROWS + SMALL_ROW, VECTOR_ROWS - SMALL_ROW), :] = jnp.zeros(
                (VECTOR_ROWS - SMALL_ROW, width), jnp.float32
            )
            for name in ("norm", "scales", "turned"):
                saved_load(name, layer).wait()
            cross(layer, 1).start()
            grad, gain_sum, shift_sum = standard_back(
                m.gx[...], m.norm[1], m.scales[2][:, :1], vec(6), width
            )
            put(6, gain_sum)
            put(7, shift_sum)
            m.gx[...] = grad
            m.down_low[...] = grad.astype(low)
            cross(layer, 2).start()
            put(3, total(m.down_low[...]))

        def tail_small():
            for name in ("norm_small", "turned_small"):
                saved_load(name, layer).wait()
            cross(layer, 6).start()
            grad, gain_sum, shift_sum = standard_back(
                m.gy[...], m.norm_small[1], m.scales[3][:, :1], small_vec(6), narrow
            )
            put_small(6, gain_sum)
            put_small(7, shift_sum)
            m.gy[...] = grad
            m.down_low_small[...] = grad.astype(low)
            cross(layer, 7).start()
            put_small(3, total(m.down_low_small[...]))

        def own_down():
            cross(layer, 1).wait_recv()
            cross(layer, 2).wait_recv()
            own_sums(
                k,
                m.turned,
                m.rows_land.at[layer, 0],
                lambda owner: m.down_low[...],
                lambda owner: m.in_land[layer, 3],
            )

        cut = 3 * LANE

        def hidden(block, carry):
            m.wide[...] = dot_nt(m.down_low[...], unit_rows(slot(0), block))
            for side in range(width // cut):
                inside = pl.ds(side * cut, cut)
                columns = pl.ds(pl.multiple_of(block * width + side * cut, LANE), cut)
                rows = m.slope[:, columns] * m.wide[:, inside]
                rows_low = rows.astype(low)
                m.upper_low[:, columns] = rows_low
                m.sums[pl.ds(layer * VECTOR_ROWS + 8 + block, 1), inside] = total(rows_low)
                levels = depth * cut // width
                m.rows_up[block, pl.ds(side * levels, levels)] = (
                    rows.T.astype(low).reshape(levels, 2, -1, tokens)
                )
            return carry


        def hidden_blocks(first, number):
            if first == 0:
                for name in names[5:]:
                    saved_load(name, layer).wait()
                cross(layer, 0).start()
                cross(layer, 5).start()
                weight_load(3 * turn).wait()
            lax.fori_loop(first, first + number, hidden, 0)
            if first + number == PLANE:
                cross(layer, 3).start()
                if 3 * turn + 2 < 3 * layers:
                    weight_load(3 * turn + 2).start()

        def hide_small():
            m.wide[...] = dot_nt(m.down_low_small[...], m.small_ff[1])

            for side in range(hidden_small // cut):
                columns = pl.ds(side * cut, cut)
                rows = m.slope_small[:, columns] * m.wide[:, columns]
                rows_low = rows.astype(low)
                m.upper_low_small[:, columns] = rows_low
                m.rows_small[0, columns, :] = rows.T.astype(low)
                m.sums[
                    pl.ds(layer * VECTOR_ROWS + SMALL_HIDDEN_ROW, 1), columns
                ] = total(rows_low)
            cross(layer, 8).start()

        def own_up():
            cross(layer, 0).wait_recv()
            cross(layer, 3).wait_recv()
            own_sums(
                k + 1,
                m.rows_up,
                m.rows_land.at[layer, 1],
                lambda owner: m.low[2],
                lambda owner: m.in_land[layer, 2],
            )

        def lower_text():
            weight_load(3 * turn + 1).wait()

            def lower(block, carry):
                columns = pl.ds(pl.multiple_of(block * width, LANE), width)
                m.gx[...] += dot_nn(m.upper_low[:, columns], unit_rows(slot(1), block))
                return carry

            lax.fori_loop(0, PLANE, lower, 0)
            if 3 * turn + 3 < 3 * layers:
                weight_load(3 * turn + 3).start()
            grad, gain_sum, shift_sum = standard_back(
                m.gx[...], m.norm[0], m.scales[0][:, :1], vec(4), width
            )
            put(4, gain_sum)
            put(5, shift_sum)
            m.gx[...] = grad
            m.branch_low[...] = grad.astype(low)
            put(2, total(m.branch_low[...]))
            for side in range(width // cut):
                levels = depth * cut // width
                tile = m.gx[:, side * cut : (side + 1) * cut]
                m.rows_attn[3, pl.ds(side * levels, levels)] = (
                    tile.T.astype(low).reshape(levels, 2, -1, tokens)
                )

        def lower_small():
            grad = m.gy[...] + dot_nn(m.upper_low_small[...], m.small_ff[0])
            grad, gain_sum, shift_sum = standard_back(
                grad, m.norm_small[0], m.scales[1][:, :1], small_vec(4), narrow
            )
            put_small(4, gain_sum)
            put_small(5, shift_sum)
            m.gy[...] = grad
            m.branch_low_small[...] = grad.astype(low)
            put_small(2, total(m.branch_low_small[...]))
            m.rows_small[1, pl.ds(3 * narrow, narrow), :] = grad.T[:narrow].astype(low)

        def contexts():
            weight_load(3 * turn + 2).wait()
            m.context[...] = dot_nn(m.branch_low[...], unit_rows(slot(2), 3)).astype(low)
            m.context_small[...] = dot_nn(m.branch_low_small[...], m.small_attn[3]).astype(low)
            m.mixed[...] = jnp.zeros_like(m.mixed)

        def pair_back(pair, carry):
            lanes = pl.ds(pl.multiple_of(pair * LANE, LANE), LANE)
            query, keyed, valued = (m.heads[n, :, lanes] for n in range(3))
            small_query, small_keyed, small_valued = (m.heads_small[n] for n in range(3))
            context, context_small = m.context[:, lanes], m.context_small[...]
            lane, small_lane = lane_of((1, LANE)), lane_of((1, PAD))
            results = []
            for side in range(2):
                head = 2 * pair + side
                chosen = (lane >= 64 * side) & (lane < 64 * side + 64)
                small_chosen = (small_lane >= 16 * head) & (small_lane < 16 * head + 16)
                mask = jnp.where(chosen, 1.0, 0.0).astype(low)
                small_mask = jnp.where(small_chosen, 1.0, 0.0).astype(low)
                probs = m.probs[head]
                grad_probs = dot_nt(context * mask, valued) + dot_nt(
                    context_small * small_mask, small_valued
                )
                inner = jnp.sum(grad_probs * probs, axis=1, keepdims=True)
                scores = probs * (grad_probs - inner)
                scores_low = scores.astype(low)
                scores_turned = scores.T.astype(low)
                probs_turned = probs.T.astype(low)
                results.append(
                    (
                        dot_nn(scores_low, keyed) * 0.125,
                        dot_nn(scores_turned, query) * 0.125,
                        dot_nn(probs_turned, context),
                    )
                )
                small = (
                    dot_nn(scores_low, small_keyed) * 0.25,
                    dot_nn(scores_turned, small_query) * 0.25,
                    dot_nn(probs_turned, context_small),
                )
                for n in range(3):
                    m.mixed[n] += jnp.where(small_chosen, small[n], 0.0)
            for n in range(3):
                m.joined[n, :, lanes] = jnp.where(lane < 64, results[0][n], results[1][n]).astype(
                    low
                )
            return carry


        def pairs(first, number):
            lax.fori_loop(first, first + number, pair_back, 0)

        def turn_rows():
            for part in range(3):
                for side in range(width // cut):
                    levels = depth * cut // width
                    tile = m.joined[part, :, side * cut : (side + 1) * cut].astype(jnp.float32)
                    m.rows_attn[part, pl.ds(side * levels, levels)] = (
                        tile.T.astype(low).reshape(levels, 2, -1, tokens)
                    )
                tile = m.mixed[part].astype(low).astype(jnp.float32)
                m.rows_small[1, pl.ds(part * narrow, narrow), :] = tile.T[:narrow].astype(low)
            cross(layer, 4).start()
            cross(layer, 9).start()
            put(0, total(m.joined[0]))
            put(1, total(m.joined[2]))
            put_small(0, total(m.mixed[0].astype(low)))
            put_small(1, total(m.mixed[2].astype(low)))

        def entering(part, carry):
            m.gx[...] += dot_nn(m.joined[part], unit_rows(slot(2), part))
            return carry


        def attn_sums():
            cross(layer, 4).wait_recv()
            own_sums(
                k + 2,
                m.rows_attn,
                m.rows_land.at[layer, 2],
                lambda owner: m.low[jnp.where(owner == PLANE - 1, 1, 0)],
                lambda owner: m.in_land[layer, jnp.where(owner == PLANE - 1, 1, 0)],
            )


        def enter():
            lax.fori_loop(0, 3, entering, 0)
            if 3 * turn + 4 < 3 * layers:
                weight_load(3 * turn + 4).start()
            grad = m.gy[...]
            for part in range(3):
                grad = grad + dot_nn(m.mixed[part].astype(low), m.small_attn[part])
            m.gy[...] = grad
            for group in range(LANGS):
                put(TABLE_ROW + group, total(onehot[:, group : group + 1] * m.gx[...]))
            if layer == 0:
                text_out[...] = m.gx[...]
                layout_out[...] = m.gy[:, 0:narrow].T
                vector_out[...] = m.sums[...]
                vectors.send(0)

        def small_sums():
            for link in (5, 6, 7, 8, 9):
                cross(layer, link).wait_recv()
            arrange = padded_rows_of_core(span, step, core).astype(low)
            small_rows = (m.rows_small.at[1], m.rows_small.at[0], m.turned_small)
            small_land = (2, 1, 0)
            for member in range(3):
                for block in range(PLANE):
                    rows = pl.ds(block * narrow, narrow)
                    source = (1 if block == PLANE - 1 else 0, 2, 3)[member]
                    own_in = m.down_low_small[...] if member == 2 else m.low_small[source]
                    left = jnp.concatenate(
                        [
                            small_rows[member][rows, :],
                            m.rows_land_small[layer, small_land[member], rows, :],
                        ],
                        axis=1,
                    )
                    right = jnp.concatenate([own_in, m.in_land_small[layer, source]], axis=0)
                    placed = dot_nn(arrange, dot_nn(left, right).astype(low)).astype(low)
                    mine(k + 3)[block, :, :, pl.ds(member * PAD, PAD)] = placed.reshape(
                        depth, step, PAD
                    )
            if layer > 0:
                for link in range(LINKS):
                    cross(layer, link).wait_send()
                for name in names:
                    saved_load(name, layer - 1).start()
            for index in range(4):
                plane(k + 3, index).start()

        own = lambda n: ("o", k + n)
        crossed = lambda link: ("c", layer, link)
        free = lambda n: done(reuse[k + n]) if k + n in reuse else []
        then(("t", 0, turn), tail, 3.0, sends=[("c", 1.0, crossed(1)), ("c", 0.5, crossed(2))])
        then(("t", 1, turn), tail_small, 0.8, sends=[("c", 0.8, crossed(6))])
        then(own(0), own_down, 2.5, [crossed(1), crossed(2)], own_sends(k), free(0))
        add_scatter(k, 4 * k)
        then(
            ("h", 0, turn), functools.partial(hidden_blocks, 0, 2), 3.0, sends=[("c", 1.5, crossed(0))]
        )
        then(
            ("h", 1, turn), functools.partial(hidden_blocks, 2, 2), 2.5, sends=[("c", 1.0, crossed(3))]
        )
        then(("h", 2, turn), hide_small, 0.8, sends=[("c", 0.5, crossed(8))])
        then(own(1), own_up, 2.5, [crossed(0), crossed(3)], own_sends(k + 1), free(1))
        add_scatter(k + 1, 4 * k + 4)
        then(("n", 0, turn), lower_text, 3.0)
        then(("n", 1, turn), lower_small, 0.8)
        then(("n", 2, turn), contexts, 0.8)
        then(("p", 0, turn), functools.partial(pairs, 0, H // 4), 4.0)
        then(("p", 1, turn), functools.partial(pairs, H // 4, H // 4), 4.0)
        then(("r", turn), turn_rows, 2.0, sends=[("c", 1.0, crossed(4)), ("c", 0.5, crossed(9))])
        then(own(2), attn_sums, 2.5, [crossed(4)], own_sends(k + 2), free(2))
        add_scatter(k + 2, 4 * k + 8)
        then(("e", turn), enter, 2.0, sends=[("c", 0.3, ("v", 0))] if layer == 0 else [])
        then(own(3), small_sums, 2.0, [crossed(9)], own_sends(k + 3))
        add_scatter(k + 3, 4 * k + 12)

    for turn, layer in enumerate(reversed(range(layers))):
        add_layer(turn, layer)
    for n in range(AllSum.STEPS):
        sends = [((("z", 0), 2.2), (("z", 0), 4.4), ("x", 2.2), ("x", 2.2), ("c", 0.0))[n] + (("v", n + 1),)]
        after = [("v", n - 1)] if n else [("e", layers - 1)]
        plan.add(("v", n), functools.partial(vectors.advance, n), after, [("v", n)], sends, 0.2, -1)
    plan.run()
    vectors.close()
    for link in range(LINKS):
        cross(0, link).wait_send()
    drained = list(reuse.values())
    for k in range(count):
        if k not in drained:
            drain(k)


def run_backward(depth, layers, narrow, span, step, gathered, saved, vectors, text_cot, layout_cot, onehot):
    dma = pltpu.SemaphoreType.DMA
    tokens, width = text_cot.shape
    low, full = jnp.bfloat16, jnp.float32
    shapes = back_shapes(layers, depth, tokens, width, 4 * narrow)
    unit = gathered[0].shape[3:]
    small_unit = (step, width)
    units = [small_unit if k % 4 == 3 else unit for k in range(4 * layers)]
    count = len(units)
    whole = (layers, PLANE, depth, 2, -1, tokens)
    kept = [
        array.reshape(whole) if array.ndim == 3 and array.shape[1] == 4 * width else array
        for array in saved
    ]
    scratch = [pltpu.VMEM(array.shape[1:], array.dtype) for array in kept]
    scratch += [pltpu.VMEM(*shapes[name]) for name in BACK_SCRATCH]
    scratch += [
        pltpu.VMEM((4, PLANE, depth) + unit, low),
        pltpu.VMEM((layers, PLANE, depth) + small_unit, low),
    ]
    fill = 1
    landing = [((2, depth // 2) + one, (2, depth) + one, (depth + 1, 1) + one) for one in units]
    landing[fill] = (
        (2, unit[0] // 2, width),
        (2,) + unit,
        (depth + 1, PLANE) + unit,
    )
    for n in range(3):
        scratch += [pltpu.VMEM(shapes_of[n], low) for shapes_of in landing]
    scratch += [
        dma((len(gathered),)),
        dma((len(SAVED), layers)),
        dma((layers, LINKS)),
        dma((layers, LINKS)),
        dma((count, 6)),
        dma((count, 6)),
        dma((count + 3, 2, depth)),
        dma((count + 3, 2, depth)),
    ]
    scratch += AllSum.scratch(vectors.shape)
    results = pl.pallas_call(
        functools.partial(backward_kernel, depth, layers, narrow, span, step),
        out_shape=[jax.ShapeDtypeStruct(one, full) for one in units]
        + [
            jax.ShapeDtypeStruct(vectors.shape, full),
            jax.ShapeDtypeStruct((tokens, width), full),
            jax.ShapeDtypeStruct((narrow, tokens), full),
        ],
        in_specs=[ANY] * (len(gathered) + len(kept)) + [IN_VMEM] * 4,
        out_specs=[IN_VMEM] * (count + 3),
        scratch_shapes=scratch,
        compiler_params=pltpu.CompilerParams(
            collective_id=1, has_side_effects=True, vmem_limit_bytes=67000000
        ),
        name="backward_blocks",
    )(*gathered, *kept, vectors, text_cot, layout_cot, onehot)
    return results


def finish_kernel(depth, layers, narrow, span, small_span, *refs):
    count = 4 * layers
    summed, totals, ins = refs[:count], refs[count], refs[count + 1 : count + 5]
    outs = refs[count + 5 :]
    width = ins[0].shape[1]
    at, unused = place(depth)
    for n in range(4):
        outs[n][...] = ins[n][...]
    attn, up, down = outs[4:7]
    pieces = outs[7:9] + outs[12:13]
    small_attn, small_up, small_down = outs[9:12]
    for layer in range(layers):
        parts = summed[4 * (layers - 1 - layer) :]
        down[layer] = parts[0][...]
        up[layer] = parts[1][...]
        attn[layer] = parts[2][...]
        small = parts[3]
        small_attn[layer] = small[0:small_span, 0:narrow]
        small_up[layer] = small[0:small_span, PAD : PAD + narrow]
        small_down[layer] = small[0:small_span, 2 * PAD : 2 * PAD + narrow]
    lane = lane_of((layers, width))
    found = [jnp.zeros((layers, width), jnp.float32) for piece in pieces]
    for row, n, base, lanes in flat_rows(width, narrow):
        first = at.me * pieces[n].shape[1] - base
        rows = jnp.concatenate(
            [totals[pl.ds(layer * VECTOR_ROWS + row, 1), :] for layer in range(layers)], axis=0
        )
        rolled = pltpu.roll(rows, lax.rem(16 * width - first, width), 1)
        index = lane + first
        found[n] = found[n] + jnp.where((index >= 0) & (index < lanes), rolled, 0.0)
    for n, piece in enumerate(pieces):
        piece[...] = found[n][:, : piece.shape[1]]


def run_finish(depth, layers, narrow, span, small_span, lengths, results, text_out, layout_out):
    count = 4 * layers
    summed, (totals, text_grad, layout_grad) = results[:count], results[count:]
    tokens, width = text_out.shape
    shapes = [
        (tokens, width),
        (narrow, tokens),
        (tokens, width),
        (narrow, tokens),
        (layers, span, width),
        (layers, span, width),
        (layers, span, width),
        (layers, lengths[0]),
        (layers, lengths[1]),
        (layers, small_span, narrow),
        (layers, small_span, narrow),
        (layers, small_span, narrow),
        (layers, lengths[2]),
    ]
    return pl.pallas_call(
        functools.partial(finish_kernel, depth, layers, narrow, span, small_span),
        out_shape=[jax.ShapeDtypeStruct(shape, jnp.float32) for shape in shapes],
        in_specs=[IN_VMEM] * (count + 5),
        out_specs=[IN_VMEM] * len(shapes),
        name="finish",
    )(*summed, totals, text_out, layout_out, text_grad, layout_grad)


def block_shards(
    depth,
    text_input,
    layout_input,
    text_cot,
    layout_cot,
    segment_ids,
    page_groups,
    lang_table,
    text_attn,
    text_up,
    text_down,
    text_vector,
    layout_attn,
    layout_up,
    layout_down,
    layout_vector,
):
    layers, unused, span = text_attn.shape
    narrow, small_span = layout_input.shape[1], layout_down.shape[1]
    step = PAD * PLANE // (PLANE * depth * 2)

    def turned(array):
        return jnp.swapaxes(array, -1, -2)

    weights = (
        turned(text_attn),
        turned(text_up),
        text_down,
        turned(layout_attn),
        turned(layout_up),
        layout_down,
    )
    pieces = (text_vector, lang_table, layout_vector)
    gathered, (vectors, onehot, text_out, layout_out), saved = run_forward(
        depth,
        narrow,
        step,
        weights,
        pieces,
        text_input,
        turned(layout_input),
        segment_ids.reshape(1, -1),
        page_groups.reshape(1, -1),
    )
    text_gathered = [part for n, part in enumerate(gathered) if n != 1]
    results = run_backward(
        depth,
        layers,
        narrow,
        small_span,
        step,
        text_gathered,
        saved,
        vectors,
        text_cot,
        turned(layout_cot),
        onehot,
    )
    lengths = [piece.shape[1] for piece in pieces]
    outs = run_finish(
        depth, layers, narrow, span, small_span, lengths, results, text_out, layout_out
    )
    return tuple(turned(out) if n in (1, 3, 4, 5, 9, 10) else out for n, out in enumerate(outs))


def solution(mesh):
    in_specs = (
        P(AXES, None),
        P(AXES, None),
        P(AXES, None),
        P(AXES, None),
        P(AXES),
        P(AXES),
        P(None, AXES),
        P(None, None, AXES),
        P(None, None, AXES),
        P(None, AXES, None),
        P(None, AXES),
        P(None, None, AXES),
        P(None, None, AXES),
        P(None, AXES, None),
        P(None, AXES),
    )
    out_specs = (
        P(AXES, None),
        P(AXES, None),
        P(AXES, None),
        P(AXES, None),
        P(None, None, AXES),
        P(None, None, AXES),
        P(None, AXES, None),
        P(None, AXES),
        P(None, AXES),
        P(None, None, AXES),
        P(None, None, AXES),
        P(None, AXES, None),
        P(None, AXES),
    )
    plan = functools.partial(block_shards, mesh.shape[AXES[1]] // 2) if fits_blocks(mesh) else generic_shards
    return jax.shard_map(plan, mesh=mesh, in_specs=in_specs, out_specs=out_specs, check_vma=False)
```

```python
import functools
import math
from types import SimpleNamespace

import jax
import jax.numpy as jnp
from jax import lax
from jax.experimental import pallas as pl
from jax.experimental.pallas import tpu as pltpu
from jax.sharding import PartitionSpec as P

H = 12
LANGS = 8


EPSILON = 1e-05
MASKED = -1e30


def norm_rows(residual, norm_gain, norm_shift):
    average = jnp.mean(residual, axis=-1, keepdims=True)
    centred = residual - average
    variance = jnp.mean(centred * centred, axis=-1, keepdims=True)
    return centred * lax.rsqrt(variance + EPSILON) * norm_gain + norm_shift


def exact_gelu(values):
    return jax.nn.gelu(values, approximate=False)


def norm_back(residual, norm_gain, norm_shift, grad_rows):
    unused, pullback = jax.vjp(norm_rows, residual, norm_gain, norm_shift)
    return pullback(grad_rows)


def gelu_back(upper, grad_rows):
    unused, pullback = jax.vjp(exact_gelu, upper)
    return pullback(grad_rows)[0]


def column_sum(matrix):
    return jnp.sum(matrix.astype(jnp.float32), axis=0)


def unpack(vector, stream_width, hidden_width):
    values = vector.astype(jnp.float32)
    pieces = [values[member * stream_width : (member + 1) * stream_width] for member in range(8)]
    return pieces + [values[8 * stream_width : 8 * stream_width + hidden_width]]


def project(stream_low, attn_weight, pieces):
    stream_width = stream_low.shape[1]
    joined = jnp.dot(
        stream_low, attn_weight[:, : 3 * stream_width], preferred_element_type=jnp.float32
    )
    head_shape = (stream_low.shape[0], H, stream_width // H)
    query = (joined[:, :stream_width] + pieces[0]).astype(jnp.bfloat16).reshape(head_shape)
    keyed = joined[:, stream_width : 2 * stream_width].astype(jnp.bfloat16).reshape(head_shape)
    valued = (joined[:, 2 * stream_width :] + pieces[1]).astype(jnp.bfloat16).reshape(head_shape)
    return (query, keyed, valued)


def joint_scores(text_heads, layout_heads, same_page):
    text_part = jnp.einsum(
        "shd,thd->hst", text_heads[0], text_heads[1], preferred_element_type=jnp.float32
    )
    layout_part = jnp.einsum(
        "shd,thd->hst", layout_heads[0], layout_heads[1], preferred_element_type=jnp.float32
    )
    combined = text_part * (1.0 / math.sqrt(text_heads[0].shape[2])) + layout_part * (
        1.0 / math.sqrt(layout_heads[0].shape[2])
    )
    return jnp.where(same_page[None], combined, MASKED)


def attend(probs_low, valued):
    context = jnp.einsum("hst,thd->shd", probs_low, valued, preferred_element_type=jnp.float32)
    return context.reshape(context.shape[0], -1).astype(jnp.bfloat16)


def tail_forward(stream_rows, context_low, attn_weight, up_weight, down_weight, pieces):
    stream_width = stream_rows.shape[1]
    branch = (
        jnp.dot(context_low, attn_weight[:, 3 * stream_width :], preferred_element_type=jnp.float32)
        + pieces[2]
    )
    first_sum = stream_rows + branch
    normed = norm_rows(first_sum, pieces[4], pieces[5])
    normed_low = normed.astype(jnp.bfloat16)
    upper = jnp.dot(normed_low, up_weight, preferred_element_type=jnp.float32) + pieces[8]
    active_low = exact_gelu(upper).astype(jnp.bfloat16)
    second_sum = (
        normed + jnp.dot(active_low, down_weight, preferred_element_type=jnp.float32) + pieces[3]
    )
    result = norm_rows(second_sum, pieces[6], pieces[7])
    return (result, (first_sum, normed_low, upper, active_low, second_sum))


def layer_forward(text_rows, layout_rows, text_weights, layout_weights, same_page, onehot):
    group_table = text_weights[4].astype(jnp.float32).reshape(onehot.shape[1], -1)
    text_rows = text_rows + jnp.dot(onehot, group_table, precision=lax.Precision.HIGHEST)
    text_pieces = unpack(text_weights[3], text_rows.shape[1], text_weights[1].shape[1])
    layout_pieces = unpack(layout_weights[3], layout_rows.shape[1], layout_weights[1].shape[1])
    text_low = text_rows.astype(jnp.bfloat16)
    layout_low = layout_rows.astype(jnp.bfloat16)
    text_heads = project(text_low, text_weights[0], text_pieces)
    layout_heads = project(layout_low, layout_weights[0], layout_pieces)
    scores = joint_scores(text_heads, layout_heads, same_page)
    row_peak = jnp.max(scores, axis=-1, keepdims=True)
    log_total = row_peak + jnp.log(jnp.sum(jnp.exp(scores - row_peak), axis=-1, keepdims=True))
    probs_low = jnp.exp(scores - log_total).astype(jnp.bfloat16)
    text_context = attend(probs_low, text_heads[2])
    layout_context = attend(probs_low, layout_heads[2])
    text_next, text_stored = tail_forward(
        text_rows, text_context, text_weights[0], text_weights[1], text_weights[2], text_pieces
    )
    layout_next, layout_stored = tail_forward(
        layout_rows,
        layout_context,
        layout_weights[0],
        layout_weights[1],
        layout_weights[2],
        layout_pieces,
    )
    stored = (
        text_low,
        layout_low,
        text_heads,
        layout_heads,
        log_total,
        text_context,
        layout_context,
        text_stored,
        layout_stored,
    )
    return (text_next, layout_next, stored)


def tail_backward(grad_result, stored, context_low, attn_weight, up_weight, down_weight, pieces):
    first_sum, normed_low, upper, active_low, second_sum = stored
    stream_width = first_sum.shape[1]
    grad_second, grad_gain_two, grad_shift_two = norm_back(
        second_sum, pieces[6], pieces[7], grad_result
    )
    grad_down_low = grad_second.astype(jnp.bfloat16)
    grad_down_bias = column_sum(grad_down_low)
    grad_down = jnp.einsum(
        "sf,sd->fd", active_low, grad_down_low, preferred_element_type=jnp.float32
    )
    grad_active = jnp.einsum(
        "sd,fd->sf", grad_down_low, down_weight, preferred_element_type=jnp.float32
    )
    grad_upper_low = gelu_back(upper, grad_active).astype(jnp.bfloat16)
    grad_up_bias = column_sum(grad_upper_low)
    grad_up = jnp.einsum(
        "sd,sf->df", normed_low, grad_upper_low, preferred_element_type=jnp.float32
    )
    grad_normed = grad_second + jnp.einsum(
        "sf,df->sd", grad_upper_low, up_weight, preferred_element_type=jnp.float32
    )
    grad_first, grad_gain_one, grad_shift_one = norm_back(
        first_sum, pieces[4], pieces[5], grad_normed
    )
    grad_branch_low = grad_first.astype(jnp.bfloat16)
    grad_out_bias = column_sum(grad_branch_low)
    output_weight = attn_weight[:, 3 * stream_width :]
    grad_output_proj = jnp.einsum(
        "sd,se->de", context_low, grad_branch_low, preferred_element_type=jnp.float32
    )
    grad_context = jnp.einsum(
        "se,de->sd", grad_branch_low, output_weight, preferred_element_type=jnp.float32
    ).astype(jnp.bfloat16)
    matrices = (grad_output_proj, grad_up, grad_down)
    vectors = (
        grad_out_bias,
        grad_down_bias,
        grad_gain_one,
        grad_shift_one,
        grad_gain_two,
        grad_shift_two,
        grad_up_bias,
    )
    return (grad_first, grad_context, matrices, vectors)


def head_grads(head_set, grad_context_low, probs_low, grad_scores_low):
    inverse_root = 1.0 / math.sqrt(head_set[0].shape[2])
    grad_heads = grad_context_low.reshape(head_set[2].shape)
    grad_query = (
        jnp.einsum("hst,thd->shd", grad_scores_low, head_set[1], preferred_element_type=jnp.float32)
        * inverse_root
    )
    grad_key = (
        jnp.einsum("hst,shd->thd", grad_scores_low, head_set[0], preferred_element_type=jnp.float32)
        * inverse_root
    )
    grad_value = jnp.einsum(
        "hst,shd->thd", probs_low, grad_heads, preferred_element_type=jnp.float32
    )
    row_count = head_set[0].shape[0]
    joined = jnp.concatenate(
        [
            grad_query.reshape(row_count, -1),
            grad_key.reshape(row_count, -1),
            grad_value.reshape(row_count, -1),
        ],
        axis=1,
    )
    return joined.astype(jnp.bfloat16)


def attention_backward(
    text_heads, layout_heads, log_total, same_page, grad_text_context, grad_layout_context
):
    scores = joint_scores(text_heads, layout_heads, same_page)
    probs = jnp.exp(scores - log_total)
    probs_low = probs.astype(jnp.bfloat16)
    grad_text_heads = grad_text_context.reshape(text_heads[2].shape)
    grad_layout_heads = grad_layout_context.reshape(layout_heads[2].shape)
    grad_probs = jnp.einsum(
        "shd,thd->hst", grad_text_heads, text_heads[2], preferred_element_type=jnp.float32
    )
    grad_probs = grad_probs + jnp.einsum(
        "shd,thd->hst", grad_layout_heads, layout_heads[2], preferred_element_type=jnp.float32
    )
    inner = jnp.sum(grad_probs * probs, axis=-1, keepdims=True)
    grad_scores_low = (probs * (grad_probs - inner)).astype(jnp.bfloat16)
    text_joined = head_grads(text_heads, grad_text_context, probs_low, grad_scores_low)
    layout_joined = head_grads(layout_heads, grad_layout_context, probs_low, grad_scores_low)
    return (text_joined, layout_joined)


def head_backward(stream_low, grad_joined_low, attn_weight, grad_first, matrices, vectors):
    stream_width = stream_low.shape[1]
    grad_in_proj = jnp.einsum(
        "sd,se->de", stream_low, grad_joined_low, preferred_element_type=jnp.float32
    )
    grad_bias_query = column_sum(grad_joined_low[:, :stream_width])
    grad_bias_value = column_sum(grad_joined_low[:, 2 * stream_width :])
    grad_stream = grad_first + jnp.einsum(
        "se,de->sd",
        grad_joined_low,
        attn_weight[:, : 3 * stream_width],
        preferred_element_type=jnp.float32,
    )
    grad_attn = jnp.concatenate([grad_in_proj, matrices[0]], axis=1)
    grad_vector = jnp.concatenate([grad_bias_query, grad_bias_value] + list(vectors))
    return (grad_stream, (grad_attn, matrices[1], matrices[2], grad_vector))


def layer_backward(grad_text, grad_layout, stored, text_weights, layout_weights, same_page, onehot):
    (
        text_low,
        layout_low,
        text_heads,
        layout_heads,
        log_total,
        text_context,
        layout_context,
        text_stored,
        layout_stored,
    ) = stored
    text_pieces = unpack(text_weights[3], text_low.shape[1], text_weights[1].shape[1])
    layout_pieces = unpack(layout_weights[3], layout_low.shape[1], layout_weights[1].shape[1])
    text_first, grad_text_context, text_mats, text_vecs = tail_backward(
        grad_text,
        text_stored,
        text_context,
        text_weights[0],
        text_weights[1],
        text_weights[2],
        text_pieces,
    )
    layout_first, grad_layout_context, layout_mats, layout_vecs = tail_backward(
        grad_layout,
        layout_stored,
        layout_context,
        layout_weights[0],
        layout_weights[1],
        layout_weights[2],
        layout_pieces,
    )
    text_joined, layout_joined = attention_backward(
        text_heads, layout_heads, log_total, same_page, grad_text_context, grad_layout_context
    )
    grad_text_in, text_terms = head_backward(
        text_low, text_joined, text_weights[0], text_first, text_mats, text_vecs
    )
    grad_layout_in, layout_terms = head_backward(
        layout_low, layout_joined, layout_weights[0], layout_first, layout_mats, layout_vecs
    )
    grad_group = jnp.einsum(
        "sg,sd->gd", onehot, grad_text_in, precision=lax.Precision.HIGHEST
    ).reshape(-1)
    return (grad_text_in, grad_layout_in, text_terms + (grad_group,), layout_terms)


def fetch_layer(
    text_attn,
    text_up,
    text_down,
    text_vector,
    lang_table,
    layout_attn,
    layout_up,
    layout_down,
    layout_vector,
    layer_index,
):
    fetched = (
        lax.all_gather(text_attn[layer_index], AXES, axis=1, tiled=True),
        lax.all_gather(text_up[layer_index], AXES, axis=1, tiled=True),
        lax.all_gather(text_down[layer_index], AXES, axis=0, tiled=True),
        lax.all_gather(text_vector[layer_index], AXES, axis=0, tiled=True),
        lax.all_gather(lang_table[layer_index], AXES, axis=0, tiled=True),
        lax.all_gather(layout_attn[layer_index], AXES, axis=1, tiled=True),
        lax.all_gather(layout_up[layer_index], AXES, axis=1, tiled=True),
        lax.all_gather(layout_down[layer_index], AXES, axis=0, tiled=True),
        lax.all_gather(layout_vector[layer_index], AXES, axis=0, tiled=True),
    )
    return (fetched[:5], fetched[5:])


def fetch_layer_back(
    text_attn,
    text_up,
    text_down,
    text_vector,
    lang_table,
    layout_attn,
    layout_up,
    layout_down,
    layout_vector,
    layer_index,
):
    fetched = (
        lax.all_gather(text_attn[layer_index], AXES, axis=1, tiled=True),
        lax.all_gather(text_up[layer_index], AXES, axis=1, tiled=True),
        lax.all_gather(text_down[layer_index], AXES, axis=0, tiled=True),
        lax.all_gather(text_vector[layer_index], AXES, axis=0, tiled=True),
        lax.all_gather(lang_table[layer_index], AXES, axis=0, tiled=True),
        lax.all_gather(layout_attn[layer_index], AXES, axis=1, tiled=True),
        lax.all_gather(layout_up[layer_index], AXES, axis=1, tiled=True),
        lax.all_gather(layout_down[layer_index], AXES, axis=0, tiled=True),
        lax.all_gather(layout_vector[layer_index], AXES, axis=0, tiled=True),
    )
    return (fetched[:5], fetched[5:])


def generic_shards(
    text_input,
    layout_input,
    text_cot,
    layout_cot,
    segment_ids,
    page_groups,
    lang_table,
    text_attn,
    text_up,
    text_down,
    text_vector,
    layout_attn,
    layout_up,
    layout_down,
    layout_vector,
):
    layer_count = text_attn.shape[0]
    same_page = segment_ids[:, None] == segment_ids[None, :]
    page_slot = segment_ids % 2
    token_group = jnp.where(page_slot == 0, page_groups[0], page_groups[1])
    onehot = (token_group[:, None] == jnp.arange(LANGS, dtype=jnp.int32)[None, :]).astype(
        jnp.float32
    )
    text_rows = text_input.astype(jnp.float32)
    layout_rows = layout_input.astype(jnp.float32)
    saved_layers = []
    for layer_index in range(layer_count):
        text_fetched, layout_fetched = fetch_layer(
            text_attn,
            text_up,
            text_down,
            text_vector,
            lang_table,
            layout_attn,
            layout_up,
            layout_down,
            layout_vector,
            layer_index,
        )
        text_rows, layout_rows, stored = layer_forward(
            text_rows, layout_rows, text_fetched, layout_fetched, same_page, onehot
        )
        saved_layers.append(stored)
    grad_text = text_cot.astype(jnp.float32)
    grad_layout = layout_cot.astype(jnp.float32)
    owned_all = [None] * layer_count
    for layer_index in reversed(range(layer_count)):
        text_fetched, layout_fetched = fetch_layer_back(
            text_attn,
            text_up,
            text_down,
            text_vector,
            lang_table,
            layout_attn,
            layout_up,
            layout_down,
            layout_vector,
            layer_index,
        )
        grad_text, grad_layout, text_terms, layout_terms = layer_backward(
            grad_text,
            grad_layout,
            saved_layers[layer_index],
            text_fetched,
            layout_fetched,
            same_page,
            onehot,
        )
        joined_terms = tuple(text_terms) + tuple(layout_terms)
        owned_all[layer_index] = (
            lax.psum_scatter(joined_terms[0], AXES, scatter_dimension=1, tiled=True),
            lax.psum_scatter(joined_terms[1], AXES, scatter_dimension=1, tiled=True),
            lax.psum_scatter(joined_terms[2], AXES, scatter_dimension=0, tiled=True),
            lax.psum_scatter(joined_terms[3], AXES, scatter_dimension=0, tiled=True),
            lax.psum_scatter(joined_terms[4], AXES, scatter_dimension=0, tiled=True),
            lax.psum_scatter(joined_terms[5], AXES, scatter_dimension=1, tiled=True),
            lax.psum_scatter(joined_terms[6], AXES, scatter_dimension=1, tiled=True),
            lax.psum_scatter(joined_terms[7], AXES, scatter_dimension=0, tiled=True),
            lax.psum_scatter(joined_terms[8], AXES, scatter_dimension=0, tiled=True),
        )
    stacks = [jnp.stack([owned[member] for owned in owned_all]) for member in range(9)]
    return (
        text_rows,
        layout_rows,
        grad_text,
        grad_layout,
        stacks[0],
        stacks[1],
        stacks[2],
        stacks[3],
        stacks[4],
        stacks[5],
        stacks[6],
        stacks[7],
        stacks[8],
    )


MESH = pl.DeviceIdType.MESH
AXES = ("dp", "shard")
ANY = pl.BlockSpec(memory_space=pl.ANY)
IN_VMEM = pl.BlockSpec(memory_space=pltpu.VMEM)
PLANE = 4
SUBLANES = 8
VECTOR_ROWS = 32


def fits_blocks(mesh):
    return mesh.shape[AXES[0]] == PLANE and mesh.shape[AXES[1]] == 2 * PLANE


def place(depth):
    dp, shard = lax.axis_index(AXES[0]), lax.axis_index(AXES[1])
    core, level = lax.rem(shard, 2), shard // 2
    dx = dp + 1 - 2 * lax.rem(dp, 2)
    dy = lax.rem(dp + 2, PLANE)
    me = dp * (2 * depth) + shard
    at = SimpleNamespace(dp=dp, z=level, core=core, dx=dx, dy=dy, dd=PLANE - 1 - dp, me=me)

    def device(plane_index, shard_index):
        return dict(zip(AXES, (plane_index, shard_index)))

    devices = SimpleNamespace(
        x=device(dx, shard),
        y=device(dy, shard),
        up=device(dp, lax.rem(shard + 2, 2 * depth)),
        down=device(dp, lax.rem(shard + 2 * depth - 2, 2 * depth)),
        far=device(dp, lax.rem(shard + depth, 2 * depth)),
        pair=device(dp, 2 * (level + 1 - 2 * lax.rem(level, 2)) + core),
        core=device(dp, shard + 1 - 2 * core),
    )
    return at, devices


def signal(devices):
    barrier = pltpu.get_barrier_semaphore()
    partners = (devices.x, devices.y, devices.up, devices.down, devices.far, devices.core)
    for partner in partners:
        pl.semaphore_signal(barrier, inc=1, device_id=partner, device_id_type=MESH)


def greeted():
    pl.semaphore_wait(pltpu.get_barrier_semaphore(), 6)


def remote(source, target, send_sem, recv_sem, device):
    return pltpu.make_async_remote_copy(
        src_ref=source,
        dst_ref=target,
        send_sem=send_sem,
        recv_sem=recv_sem,
        device_id=device,
        device_id_type=MESH,
    )


class AllSum:
    STEPS = 5

    def __init__(self, devices, running, held, landed, send_sem, recv_sem):
        self.partners = (devices.core, devices.pair, devices.far, devices.x, devices.y)
        self.running, self.held, self.landed = running, held, landed
        self.send_sem, self.recv_sem = send_sem, recv_sem

    def copy(self, step):
        return remote(
            self.held.at[step],
            self.landed.at[step],
            self.send_sem.at[step],
            self.recv_sem.at[step],
            self.partners[step],
        )

    def send(self, step):
        self.held[step] = self.running[...].astype(self.held.dtype)
        self.copy(step).start()

    def advance(self, step):
        self.copy(step).wait_recv()
        self.running[...] += self.landed[step].astype(jnp.float32)
        if step + 1 < self.STEPS:
            self.send(step + 1)

    def close(self):
        for step in range(self.STEPS):
            self.copy(step).wait_send()

    @classmethod
    def scratch(cls, shape):
        return [
            pltpu.VMEM((cls.STEPS,) + shape, jnp.bfloat16),
            pltpu.VMEM((cls.STEPS,) + shape, jnp.bfloat16),
            pltpu.SemaphoreType.DMA((cls.STEPS,)),
            pltpu.SemaphoreType.DMA((cls.STEPS,)),
        ]


class Plan:
    LAG = dict(x=1.8, z=1.8, c=1.0, h=0.3)
    PATIENCE = 1.0

    def __init__(self):
        self.tasks = []

    def add(self, name, run, after=(), needs=(), sends=(), time=0.2, rank=0, patient=False):
        self.tasks.append((name, run, tuple(after), tuple(needs), tuple(sends), time, rank, patient))

    def order(self):
        now, free, landed, done = 0.0, {}, {}, set()
        waiting, result = list(self.tasks), []
        while waiting:
            best = None
            for place_in_list, task in enumerate(waiting):
                name, run, after, needs, sends, time, rank, patient = task
                if any(other not in done for other in after):
                    continue
                if any(event not in landed for event in needs):
                    continue
                start = max([now] + [landed[event] for event in needs])
                key = (start + (self.PATIENCE if patient else 0.0), rank, place_in_list)
                if best is None or key < best[0]:
                    best = (key, task, start)
            assert best is not None
            task, start = best[1:]
            waiting.remove(task)
            result.append(task)
            name, run, after, needs, sends, time, rank, patient = task
            now = start + time
            done.add(name)
            for link, amount, event in sends:
                free[link] = max(now, free.get(link, 0.0)) + amount
                landed[event] = free[link] + self.LAG[link[0]]
        return result

    def run(self):
        for task in self.order():
            task[1]()


UNIT_ROWS_PER_US = 96 / 3.26


def add_rows(target, term):
    total = target[...].astype(jnp.float32) + term[...].astype(jnp.float32)
    target[...] = total.astype(target.dtype)


def add_units(target, *terms):
    def body(index, carry):
        total = target[index].astype(jnp.float32)
        for term in terms:
            total = total + term[index].astype(jnp.float32)
        target[index] = total.astype(target.dtype)
        return carry

    lax.fori_loop(0, target.shape[0], body, 0)


LANE = 128
PAD = 256
PIECE_ROWS = 12
TABLE_ROW = 12
SMALL_ROW = 20
SMALL_HIDDEN_ROW = 28


def dot_nt(left, right):
    return lax.dot_general(
        left, right, (((1,), (1,)), ((), ())), preferred_element_type=jnp.float32
    )


def dot_nn(left, right):
    return jnp.dot(left, right, preferred_element_type=jnp.float32)


def lane_of(shape):
    return lax.broadcasted_iota(jnp.int32, shape, len(shape) - 1)


def unit_rows(ref, dp):
    block = ref[dp]
    return block.reshape(-1, block.shape[-1])


def standard(residual, width):
    padded = residual.shape[1] != width
    average = jnp.sum(residual, axis=1, keepdims=True) * (1.0 / width)
    centred = residual - average
    if padded:
        centred = jnp.where(lane_of(residual.shape) < width, centred, 0.0)
    variance = jnp.sum(centred * centred, axis=1, keepdims=True) * (1.0 / width)
    scale = lax.rsqrt(variance + EPSILON)
    return centred * scale, scale


def gelu_parts(upper):
    cdf = 0.5 * (1.0 + lax.erf(upper * math.sqrt(0.5)))
    density = jnp.exp(upper * upper * -0.5) * (1.0 / math.sqrt(2.0 * math.pi))
    return upper * cdf, cdf + upper * density


def natural_rows(span, step):
    row = lax.broadcasted_iota(jnp.int32, (PAD, PAD), 0)
    column = lax.broadcasted_iota(jnp.int32, (PAD, PAD), 1)
    unit = jnp.zeros((PAD, PAD), jnp.int32)
    for n in range(1, PAD // step):
        unit = unit + jnp.where(row >= n * span, 1, 0)
    source = unit * step + row - unit * span
    return jnp.where((source == column) & (row < (PAD // step) * span), 1.0, 0.0)


def saved_shapes(layers, tokens, width, narrow_hidden):
    low, full = jnp.bfloat16, jnp.float32
    hidden = 4 * width
    return dict(
        low=((layers, 3, tokens, width), low),
        low_small=((layers, 3, tokens, PAD), low),
        heads=((layers, 3, tokens, width), low),
        heads_small=((layers, 3, tokens, PAD), low),
        probs=((layers, H, tokens, tokens), full),
        norm=((layers, 2, tokens, width), full),
        norm_small=((layers, 2, tokens, PAD), full),
        scales=((layers, 4, tokens, LANE), full),
        slope=((layers, tokens, hidden), full),
        slope_small=((layers, tokens, narrow_hidden), full),
        turned=((layers, hidden, tokens), low),
        turned_small=((layers, narrow_hidden, tokens), low),
        small_attn=((layers, 4, PAD, PAD), low),
        small_ff=((layers, 2, narrow_hidden, PAD), low),
    )


SAVED = tuple(saved_shapes(1, 1, 1, 1))


def forward_steps(layer, m, narrow, span):
    tokens, width = m.x.shape
    low = jnp.bfloat16
    vec = lambda row, count=1: m.vectors[pl.ds(layer * VECTOR_ROWS + row, count), :]
    small_vec = lambda row: vec(SMALL_ROW + row)[:, :PAD]

    def embed():
        rows = m.x[...]
        for group in range(LANGS):
            rows = rows + m.onehot[:, group : group + 1] * vec(TABLE_ROW + group)
        m.x[...] = rows
        m.low[layer, 0] = rows.astype(low)
        m.low_small[layer, 0] = m.y[...].astype(low)

    def project_text():
        def body(part, carry):
            joined = dot_nt(m.low[layer, 0], unit_rows(m.attn_w, part))
            bias = jnp.where(part == 0, vec(0), jnp.where(part == 2, vec(1), 0.0))
            m.heads[layer, part] = (joined + bias).astype(low)
            return carry

        lax.fori_loop(0, 3, body, 0)

    def prepare_small():
        permute = natural_rows(span, m.small_raw.shape[3] // m.small_raw_layers).astype(low)
        step = m.small_raw.shape[3] // m.small_raw_layers

        def body(block, carry):
            for member in range(3):
                raw = m.small_raw[
                    block, :, :, pl.ds(layer * step, step), pl.ds(member * PAD, PAD)
                ].reshape(PAD, PAD)
                rows = dot_nn(permute, raw).astype(low)
                if member == 0:
                    m.small_attn[layer, block] = rows
                else:
                    start = pl.multiple_of(block * narrow, 64)
                    m.small_ff[layer, member - 1, pl.ds(start, narrow), :] = rows[:narrow]
            return carry

        lax.fori_loop(0, PLANE, body, 0)

    def project_small():
        for part in range(3):
            joined = dot_nt(m.low_small[layer, 0], m.small_attn[layer, part])
            if part == 0:
                joined = joined + small_vec(0)
            if part == 2:
                joined = joined + small_vec(1)
            m.heads_small[layer, part] = joined.astype(low)
        m.mixed[...] = jnp.zeros_like(m.mixed)

    def attend_pairs(first, count):
        def body(pair, carry):
            lanes = pl.ds(pl.multiple_of(pair * LANE, LANE), LANE)
            query, keyed, valued = (m.heads[layer, n, :, lanes] for n in range(3))
            small_query, small_keyed, small_valued = (m.heads_small[layer, n] for n in range(3))
            lane, small_lane = lane_of((1, LANE)), lane_of((1, PAD))
            same = m.same[...] > 0.0
            contexts = []
            for side in range(2):
                head = 2 * pair + side
                chosen = (lane >= 64 * side) & (lane < 64 * side + 64)
                small_chosen = (small_lane >= 16 * head) & (small_lane < 16 * head + 16)
                mask = jnp.where(chosen, 0.125, 0.0).astype(low)
                small_mask = jnp.where(small_chosen, 0.25, 0.0).astype(low)
                scores = dot_nt(query * mask, keyed) + dot_nt(small_query * small_mask, small_keyed)
                scores = jnp.where(same, scores, MASKED)
                peak = jnp.max(scores, axis=1, keepdims=True)
                powers = jnp.exp(scores - peak)
                probs = powers * (1.0 / jnp.sum(powers, axis=1, keepdims=True))
                m.probs[layer, head] = probs
                probs_low = probs.astype(low)
                contexts.append(dot_nn(probs_low, valued))
                m.mixed[...] += jnp.where(small_chosen, dot_nn(probs_low, small_valued), 0.0)
            m.low[layer, 1, :, lanes] = jnp.where(lane < 64, contexts[0], contexts[1]).astype(low)
            return carry

        lax.fori_loop(first, first + count, body, 0)

    def first_norm():
        m.low_small[layer, 1] = m.mixed[...].astype(low)
        residual = m.x[...] + dot_nt(m.low[layer, 1], unit_rows(m.attn_w, 3)) + vec(2)
        normed, scale = standard(residual, width)
        m.norm[layer, 0] = normed
        m.scales[layer, 0] = jnp.broadcast_to(scale, (tokens, LANE))
        result = normed * vec(4) + vec(5)
        m.normed[...] = result
        m.low[layer, 2] = result.astype(low)

    def first_norm_small():
        branch = dot_nt(m.low_small[layer, 1], m.small_attn[layer, 3]) + small_vec(2)
        normed, scale = standard(m.y[...] + branch, narrow)
        m.norm_small[layer, 0] = normed
        m.scales[layer, 1] = jnp.broadcast_to(scale, (tokens, LANE))
        result = normed * small_vec(4) + small_vec(5)
        m.normed_small[...] = result
        m.low_small[layer, 2] = result.astype(low)

    def activate(column, upper_ref, source, active, slope, turned):
        here = pl.ds(column, LANE)
        value, rate = gelu_parts(upper_ref[:, source])
        slope[layer, :, here] = rate
        value_low = value.astype(low)
        active[:, here] = value_low
        turned[layer, here, :] = value.T.astype(low)

    def up_small():
        m.upper[...] = dot_nt(m.low_small[layer, 2], m.small_ff[layer, 0]) + vec(SMALL_HIDDEN_ROW)

        def body(tile, carry):
            column = pl.multiple_of(tile * LANE, LANE)
            activate(
                column, m.upper, pl.ds(column, LANE), m.active_small, m.slope_small, m.turned_small
            )
            return carry

        lax.fori_loop(0, m.active_small.shape[1] // LANE, body, 0)

    def down_small():
        second = dot_nn(m.active_small[...], m.small_ff[layer, 1]) + small_vec(3)
        normed, scale = standard(m.normed_small[...] + second, narrow)
        m.norm_small[layer, 1] = normed
        m.scales[layer, 3] = jnp.broadcast_to(scale, (tokens, LANE))
        m.y[...] = normed * small_vec(6) + small_vec(7)

    def up_text(first, count):
        def body(block, carry):
            m.upper[...] = dot_nt(m.low[layer, 2], unit_rows(m.up_w, block)) + vec(8 + block)

            def tile_body(tile, inner):
                column = pl.multiple_of(tile * LANE, LANE)
                activate(
                    pl.multiple_of(block * width + column, LANE),
                    m.upper,
                    pl.ds(column, LANE),
                    m.active,
                    m.slope,
                    m.turned,
                )
                return inner

            return lax.fori_loop(0, width // LANE, tile_body, carry)

        lax.fori_loop(first, first + count, body, 0)

    def down_text(first, count):
        def body(block, carry):
            columns = pl.ds(pl.multiple_of(block * width, LANE), width)
            m.second[...] += dot_nn(m.active[:, columns], unit_rows(m.down_w, block))
            return carry

        if first == 0:
            m.second[...] = m.normed[...] + vec(3)
        lax.fori_loop(first, first + count, body, 0)

    def second_norm():
        normed, scale = standard(m.second[...], width)
        m.norm[layer, 1] = normed
        m.scales[layer, 2] = jnp.broadcast_to(scale, (tokens, LANE))
        m.x[...] = normed * vec(6) + vec(7)

    part = H // 4
    after_attn = [(embed, 0.4), (project_text, 1.6)]
    after_small = [(prepare_small, 0.8), (project_small, 0.3)]
    for first in range(0, H // 2, part):
        after_small.append((functools.partial(attend_pairs, first, part), 2.5))
    after_small += [(first_norm, 0.8), (first_norm_small, 0.4), (up_small, 1.0), (down_small, 0.4)]
    after_up = [(functools.partial(up_text, first, 2), 2.4) for first in (0, 2)]
    after_down = [(functools.partial(down_text, first, 2), 0.7) for first in (0, 2)]
    after_down.append((second_norm, 0.3))
    return after_attn, after_small, after_up, after_down


def forward_shapes(layers, depth, tokens, width, narrow, step):
    low, full = jnp.bfloat16, jnp.float32
    span = 4 * width // (PLANE * depth * 2)
    whole = (PLANE, depth, 2, span, width)
    return dict(
        attn_w=(whole, low),
        up_w=(whole, low),
        down_w=(whole, low),
        small_raw=((PLANE, depth, 2, layers * step, width), low),
        own_small=((layers * step, width), low),
        own_small_full=((layers * step, width), full),
        same=((tokens, tokens), full),
        x=((tokens, width), full),
        y=((tokens, PAD), full),
        mixed=((tokens, PAD), full),
        normed=((tokens, width), full),
        normed_small=((tokens, PAD), full),
        upper=((tokens, width), full),
        active=((tokens, 4 * width), low),
        active_small=((tokens, 4 * narrow), low),
        second=((tokens, width), full),
        spread=((3 * SUBLANES, width), full),
    )


FORWARD_SCRATCH = tuple(forward_shapes(1, 1, 1, 1, 1, 1))


def flat_rows(width, narrow):
    rows = [(n, 0, n * width, width) for n in range(PIECE_ROWS)]
    rows += [(TABLE_ROW + n, 1, n * width, width) for n in range(LANGS)]
    rows += [(SMALL_ROW + n, 2, n * narrow, narrow) for n in range(8)]
    return rows + [(SMALL_HIDDEN_ROW, 2, 8 * narrow, 4 * narrow)]


def forward_kernel(depth, layers, narrow, span, *refs):
    refs = list(refs)

    def take(number):
        taken = refs[:number]
        del refs[:number]
        return taken

    count = 3 * layers + 1
    fill = count - 2
    text_attn, text_up, text_down, layout_attn, layout_up, layout_down = take(6)
    pieces = take(3)
    text_in, layout_in, page_row, groups = take(4)
    outs = take(count)
    vector_out, onehot_out, text_out, layout_out = take(4)
    kept = take(len(SAVED))
    own_sem, zs, zr, ps, pr, us, ur, cs, cr, load_sem, keep_sem = take(11)
    all_sum = take(4)
    m = SimpleNamespace()
    for name in SAVED + FORWARD_SCRATCH:
        setattr(m, name, refs.pop(0))
    m.vectors, m.onehot, m.small_raw_layers = vector_out, onehot_out, layers
    at, devices = place(depth)
    dp, z, core, dx, dy, dd = at.dp, at.z, at.core, at.dx, at.dy, at.dd
    half = depth // 2
    low, full = jnp.bfloat16, jnp.float32
    tokens, width = m.x.shape
    step = m.own_small.shape[0] // layers
    vectors = AllSum(devices, vector_out, *all_sum)

    sources = [text_attn.at[0], m.own_small]
    for layer in range(layers):
        if layer > 0:
            sources.append(text_attn.at[layer])
        sources += [text_up.at[layer], text_down.at[layer]]

    def own(k):
        return pltpu.make_async_copy(sources[k], outs[k].at[dp, z, core], own_sem.at[k])

    def line(k, rising, hop, side=0):
        level = z - hop if rising else z + hop
        owner = (dp, dx, dy, dd)[side]
        target = outs[k].at[owner, level, core]
        row = k if side == 0 else count - 1 + side
        return remote(
            sources[k] if hop == 0 and side == 0 else target,
            target,
            zs.at[row, int(rising), hop],
            zr.at[row, level],
            devices.up if rising else devices.down,
        )

    def exists(rising, hop):
        return (z - hop >= 0) if rising else (z + hop < depth)

    def goes_on(rising, hop):
        return exists(rising, hop) & ((z < depth - 1) if rising else (z > 0))

    def unit(rising, hop, to_x):
        level = z - hop if rising else z + hop
        target = outs[0].at[dp, level, core]
        return remote(
            sources[0] if hop == 0 else target,
            target,
            us.at[int(to_x), level],
            ur.at[int(to_x), level],
            devices.x if to_x else devices.y,
        )

    def unit_landed(to_x, level):
        target = outs[0].at[dx if to_x else dy, level, core]
        return remote(
            target, target, us.at[int(to_x), level], ur.at[int(to_x), level], devices.x
        )

    def line_start(k, hop, side=0):
        for rising in (True, False):

            @pl.when(goes_on(rising, hop))
            def start():
                line(k, rising, hop, side).start()

    def line_wait(k, hop, side=0, then=None):
        for rising in (True, False):

            @pl.when(exists(rising, hop))
            def wait():
                line(k, rising, hop, side).wait_recv()
                if then is not None:
                    then(rising, hop)

    def unit_start(rising, hop):
        unit(rising, hop, True).start()
        unit(rising, hop, False).start()

    def plane(k, index, sending=True):
        if k == fill:
            rows = span // 2
            lower, upper = pl.ds(0, rows), pl.ds(rows, rows)
            if sending:
                blocks = ((dp, None), (dp, None), (dx, lower), (dy, upper))
            else:
                blocks = ((dx, None), (dy, None), (dd, lower), (dd, upper))
            owner, rows = blocks[index]
            block = outs[k].at[owner, z, core]
            block = block if rows is None else block.at[rows]
            source = sources[k] if sending and index < 2 else block
        else:
            lower, upper, every = pl.ds(0, half), pl.ds(half, half), pl.ds(0, depth)
            if sending:
                blocks = ((dp, every), (dp, every), (dx, lower), (dy, upper))
            else:
                blocks = ((dx, every), (dy, every), (dd, lower), (dd, upper))
            owner, levels = blocks[index]
            block = outs[k].at[owner, levels, core]
            source = block
        device = (devices.x, devices.y, devices.y, devices.x)[index]
        return remote(source, block, ps.at[k, index], pr.at[k, index], device)

    def across(k, index, side):
        lower, upper, every = pl.ds(0, half), pl.ds(half, half), pl.ds(0, depth)
        if k == fill:
            blocks = ((dp, every), (dx, every), (dy, every), (dd, every))
        else:
            blocks = ((dp, every), (dx, every), (dy, every), (dd, lower), (dd, upper))
        owner, levels = blocks[index]
        block = outs[k].at[owner, levels, side]
        return remote(block, block, cs.at[k, index], cr.at[k, index], devices.core)

    def landed_across(k):
        return range(4 if k == fill else 5)

    held = [m.attn_w, m.small_raw, m.up_w, m.down_w] + [m.attn_w, m.up_w, m.down_w] * (layers - 1)

    def load(k, side):
        owner = (dp, dx, dy, dd)[side]
        return pltpu.make_async_copy(
            outs[k].at[owner], held[k].at[owner], load_sem.at[k, side]
        )

    def loaded(k):
        for side in range(PLANE):
            load(k, side).wait()

    def keep(index, layer):
        source = getattr(m, SAVED[index])
        return pltpu.make_async_copy(
            source.at[layer], kept[index].at[layer], keep_sem.at[index, layer]
        )

    def keep_some(layer, names):
        for name in names:
            keep(SAVED.index(name), layer).start()

    def then_keep(step, layer, names):
        def run():
            step[0]()
            keep_some(layer, names)

        return (run, step[1])

    stages = []
    for layer in range(layers):
        steps = forward_steps(layer, m, narrow, layout_down.shape[1])
        if layer == 0:
            stages += [steps[0], steps[1], steps[2], steps[3]]
        else:
            stages += [steps[0] + steps[1], steps[2], steps[3]]
        stages[-2][-1] = then_keep(stages[-2][-1], layer, SAVED[:5] + SAVED[8:])
        stages[-1][-1] = then_keep(stages[-1][-1], layer, SAVED[5:8])

    def make_small():
        m.own_small_full[...] = jnp.zeros_like(m.own_small_full)
        units = layout_down.shape[1]
        for layer in range(layers):
            rows = pl.ds(layer * step, units)
            m.own_small_full[rows, 0:narrow] = layout_attn[layer].astype(full)
            m.own_small_full[rows, PAD : PAD + narrow] = layout_up[layer].astype(full)
            m.own_small_full[rows, 2 * PAD : 2 * PAD + narrow] = layout_down[layer].astype(full)
        m.own_small[...] = m.own_small_full[...].astype(low)

    def spread_vectors():
        m.spread[...] = jnp.zeros_like(m.spread)
        for n, piece in enumerate(pieces):
            m.spread[pl.ds(SUBLANES * n, layers), 0 : piece.shape[1]] = piece[...].astype(full)
        start = vector_out
        start[...] = jnp.zeros_like(start)
        lane = lane_of((SUBLANES, width))
        for row, n, base, lanes in flat_rows(width, narrow):
            length = pieces[n].shape[1]
            shift = lax.rem(at.me * length - base + 16 * width, width)
            rolled = pltpu.roll(m.spread[pl.ds(SUBLANES * n, SUBLANES), :], shift, 1)
            index = lane + (base - at.me * length)
            inside = (index >= 0) & (index < length) & (lane < lanes)
            rolled = jnp.where(inside, rolled, 0.0)
            for layer in range(layers):
                start[pl.ds(layer * VECTOR_ROWS + row, 1), :] = rolled[layer : layer + 1]
        vectors.send(0)

    def make_masks():
        pages = jnp.broadcast_to(page_row[...].astype(full), (tokens, tokens))
        turned = pages.T
        m.same[...] = jnp.where(pages == turned, 1.0, 0.0)
        group = jnp.where(
            turned == (2 * at.me).astype(full),
            jnp.broadcast_to(groups[:, 0:1], (tokens, tokens)),
            jnp.broadcast_to(groups[:, 1:2], (tokens, tokens)),
        )
        m.onehot[...] = jnp.where(group == lane_of((tokens, tokens)), 1.0, 0.0)

    def take_in():
        m.x[...] = text_in[...].astype(full)
        m.y[...] = jnp.zeros_like(m.y)
        m.y[:, 0:narrow] = layout_in[...].astype(full).T

    def land(k, sides):
        for side in sides:
            across(k, side, 1 - core).wait_recv()
            if side == 3 and k != fill:
                across(k, 4, 1 - core).wait_recv()
            load(k, side).start()

    signal(devices)
    make_small()
    greeted()
    for k in (0, fill, 1):
        own(k).start()
    line_start(0, 0)
    unit_start(True, 0)
    plane(fill, 0).start()
    plane(fill, 1).start()
    for k in range(2, count):
        if k != fill:
            own(k).start()

    plan = Plan()
    chain = [k for k in range(count) if k != fill]
    size = [sources[k].shape[0] / UNIT_ROWS_PER_US for k in range(count)]

    def begin_line(k, side):
        if side == 0:
            own(k).wait()
        if k > 0:
            line_start(k, 0, side)

    def next_line(k, hop, side):
        line_wait(k, hop, side, unit_start if k == 0 else None)
        if hop < depth - 1:
            line_start(k, hop, side)

    def add_line(k, side, after, needs, rank):
        sends = [("z", size[k], ("z", 1, k, side))]
        if k == 0:
            sends += [("x", size[k], ("u", 0)), ("x", size[fill], ("f", 1))]
        plan.add(("z", 0, k, side), functools.partial(begin_line, k, side), after, needs, sends, 0.3, rank)
        for hop in range(1, depth):
            sends = []
            if hop < depth - 1:
                sends.append(("z", size[k], ("z", hop + 1, k, side)))
            if k == 0:
                sends.append(("x", size[k], ("u", hop)))
            plan.add(
                ("z", hop, k, side),
                functools.partial(next_line, k, hop, side),
                [("z", hop - 1, k, side)],
                [("z", hop, k, side)],
                sends,
                0.3,
                rank,
            )

    def plane_first(k):
        if k > 0:
            plane(k, 0).start()
            plane(k, 1).start()
        across(k, 0, core).start()

    def plane_second(k):
        for index in (0, 1):
            if k == 0:
                for level in range(depth):
                    unit_landed(index == 0, level).wait_recv()
            else:
                plane(k, index, False).wait_recv()
            plane(k, index + 2).start()
            if k != fill:
                across(k, index + 1, core).start()

    def plane_third(k):
        for index in (2, 3):
            plane(k, index, False).wait_recv()
            if k != fill:
                across(k, index + 1, core).start()

    def cross_fill(side):
        across(fill, side, core).start()

    last = {}
    lines = [(k, 0) for k in chain]
    for side in range(4):
        lines.insert((4, 6, 7, 9)[side], (fill, side))
    for n, (k, side) in enumerate(lines):
        after = [("z", 1 if n > 1 else 2) + lines[n - 1]] if n else []
        if k == fill:
            after.append(("p", 2 if side < 3 else 3, fill))
        add_line(k, side, after, [], 10 * n)
    for n, k in enumerate(chain):
        arrive = ("x", k) if k else ("u", depth - 1)
        sends = [("c", 0.4 * size[k], ("c", 0, k))]
        if k:
            sends.append(("x", 4 * size[k], arrive))
        plan.add(("p", 1, k), functools.partial(plane_first, k), [("z", depth - 1, k, 0)], [], sends, 0.2, 10 * n + 1)
        sends = [("x", 2 * size[k], ("d", k)), ("c", 0.8 * size[k], ("c", 1, k))]
        plan.add(("p", 2, k), functools.partial(plane_second, k), [("p", 1, k)], [arrive], sends, 0.2, 10 * n + 2)
        sends = [("c", 0.4 * size[k], ("c", 2, k))]
        plan.add(("p", 3, k), functools.partial(plane_third, k), [("p", 2, k)], [("d", k)], sends, 0.2, 10 * n + 3)
    plan.add(
        ("p", 2, fill),
        functools.partial(plane_second, fill),
        [("z", 1, 0, 0)],
        [("f", 1)],
        [("x", size[fill] / 2, ("f", 2))],
        0.2,
        5,
    )
    plan.add(("p", 3, fill), functools.partial(plane_third, fill), [("p", 2, fill)], [("f", 2)], rank=6)
    for side in range(4):
        plan.add(
            ("a", side),
            functools.partial(cross_fill, side),
            [("z", depth - 1, fill, side)],
            [],
            [("c", 0.4 * size[fill], ("a", side))],
            0.1,
            25 + 10 * side,
        )
    previous = None
    vector_steps = [spread_vectors]
    vector_steps += [functools.partial(vectors.advance, n) for n in range(AllSum.STEPS)]
    for n, step_of in enumerate(vector_steps):
        link, amount = (("c", 0.3), ("z", 2.2), ("z", 6.0), ("x", 2.2), ("x", 2.2), ("h", 0.0))[n]
        sends = [(link, amount, ("v", n))]
        needs = [("v", n - 1)] if n else []
        after = [("v", n - 1)] if n else []
        if n == 1:
            after.append(("z", 2, 0, 0))
        plan.add(("v", n), step_of, after, needs, sends, 0.1 if n else 0.5, 2)
    plan.add("i", take_in, [("v", 0)], time=0.1, rank=3)
    plan.add("m", make_masks, ["i"], time=0.1, rank=3)
    previous = [("v", AllSum.STEPS), "m"]
    for k in range(count):
        vacant = [last[k - 3]] if k > 3 else []
        if k == fill:
            landed = [("a", side) for side in range(4)]
            plan.add(("l", k), functools.partial(land, k, range(4)), landed + vacant, landed, [("h", 2.4, ("h", k))], 0.2, 10 * k)
        else:
            landed = [("c", 0, k), ("c", 1, k)]
            plan.add(("k", k), functools.partial(land, k, range(3)), [("p", 2, k)] + vacant, landed, [("h", 2.0, ("k", k))], 0.2, 10 * k)
            plan.add(("l", k), functools.partial(land, k, (3,)), [("p", 3, k), ("k", k)], [("c", 2, k)], [("h", 0.7, ("h", k))], 0.2, 10 * k)
        for n, (closure, time) in enumerate(stages[k]):
            run = closure
            if n == 0:
                run = functools.partial(lambda k, closure: (loaded(k), closure()), k, closure)
            plan.add(("s", k, n), run, previous + [("l", k)], [("h", k)], (), time, 1000 + k, True)
            previous = [("s", k, n)]
        last[k] = previous[0]
    plan.run()
    text_out[...] = m.x[...]
    layout_out[...] = m.y[:, 0:narrow].T
    vectors.close()
    for index in range(len(SAVED)):
        for layer in range(layers):
            keep(index, layer).wait()
    for level in range(depth):
        for to_x in (True, False):
            unit_landed(to_x, level).wait_send()
    for k in range(count):
        for index in landed_across(k):
            across(k, index, core).wait_send()
        for index in range(4):
            if k > 0 or index > 1:
                plane(k, index).wait_send()
        for rising in (True, False):
            for hop in range(depth):

                @pl.when(goes_on(rising, hop))
                def drain():
                    for side in range(4 if k == fill else 1):
                        line(k, rising, hop, side).wait_send()


def run_forward(depth, narrow, step, weights, pieces, text_in, layout_in, page_row, groups):
    dma = pltpu.SemaphoreType.DMA
    tokens, width = text_in.shape
    layers, span, unused = weights[0].shape
    count = 3 * layers + 1
    full = jnp.float32
    saved = saved_shapes(layers, tokens, width, 4 * narrow)
    scratch = forward_shapes(layers, depth, tokens, width, narrow, step)
    rows = [span, layers * step] + [span] * (count - 2)
    vector_shape = (layers * VECTOR_ROWS, width)
    results = pl.pallas_call(
        functools.partial(forward_kernel, depth, layers, narrow, span),
        out_shape=[
            jax.ShapeDtypeStruct((PLANE, depth, 2, row, width), weights[0].dtype) for row in rows
        ]
        + [
            jax.ShapeDtypeStruct(vector_shape, full),
            jax.ShapeDtypeStruct((tokens, LANE), full),
            jax.ShapeDtypeStruct((tokens, width), full),
            jax.ShapeDtypeStruct((narrow, tokens), full),
        ]
        + [jax.ShapeDtypeStruct(*saved[name]) for name in SAVED],
        in_specs=[IN_VMEM] * 13,
        out_specs=[ANY] * count + [IN_VMEM] * 4 + [ANY] * len(SAVED),
        scratch_shapes=[
            dma((count,)),
            dma((count + 3, 2, depth)),
            dma((count + 3, depth)),
            dma((count, 4)),
            dma((count, 4)),
            dma((2, depth)),
            dma((2, depth)),
            dma((count, 5)),
            dma((count, 5)),
            dma((count, PLANE)),
            dma((len(SAVED), layers)),
        ]
        + AllSum.scratch(vector_shape)
        + [pltpu.VMEM(*saved[name]) for name in SAVED]
        + [pltpu.VMEM(*scratch[name]) for name in FORWARD_SCRATCH],
        compiler_params=pltpu.CompilerParams(
            collective_id=0, has_side_effects=True, vmem_limit_bytes=66000000
        ),
        name="forward_blocks",
    )(*weights, *pieces, text_in, layout_in, page_row, groups)
    return results[:count], results[count : count + 4], results[count + 4 :]


TEXT_MEMBERS = 3
LINKS = 10


def back_shapes(layers, depth, tokens, width, narrow_hidden):
    low, full = jnp.bfloat16, jnp.float32
    span = 4 * width // (PLANE * depth * 2)
    unit = (PLANE, depth, span, LANE)
    whole = (PLANE, depth, 2, span, LANE)
    return dict(
        weights=((2, PLANE, depth, 2, span, width), low),
        gx=((tokens, width), full),
        gy=((tokens, PAD), full),
        down_low=((tokens, width), low),
        down_low_small=((tokens, PAD), low),
        branch_low=((tokens, width), low),
        branch_low_small=((tokens, PAD), low),
        wide=((tokens, width), full),
        upper_low=((tokens, 4 * width), low),
        upper_low_small=((tokens, narrow_hidden), low),
        context=((tokens, width), low),
        context_small=((tokens, PAD), low),
        joined=((3, tokens, width), low),
        mixed=((3, tokens, PAD), full),
        rows_up=(whole, low),
        rows_attn=(whole, low),
        rows_small=((2, narrow_hidden, tokens), low),
        in_land=((layers, 4, tokens, width), low),
        in_land_small=((layers, 4, tokens, PAD), low),
        rows_land=((layers, 3) + unit, low),
        rows_land_small=((layers, 3, narrow_hidden, tokens), low),
        sums=((layers * VECTOR_ROWS, width), full),
    )


BACK_SCRATCH = tuple(back_shapes(1, 1, 1, 1, 1))


def standard_back(grad, normed, scale, gain, width):
    pushed = grad * gain
    average = jnp.sum(pushed, axis=1, keepdims=True) * (1.0 / width)
    along = jnp.sum(pushed * normed, axis=1, keepdims=True) * (1.0 / width)
    result = scale * (pushed - average - normed * along)
    if grad.shape[1] != width:
        result = jnp.where(lane_of(grad.shape) < width, result, 0.0)
    return result, total(grad * normed), total(grad)


def total(rows):
    return jnp.sum(rows.astype(jnp.float32), axis=0, keepdims=True)


def padded_rows_of_core(span, step, core):
    units = PAD // step // 2
    shape = (units * step, units * 2 * span)
    row = lax.broadcasted_iota(jnp.int32, shape, 0)
    column = lax.broadcasted_iota(jnp.int32, shape, 1)
    unit = jnp.zeros(shape, jnp.int32)
    for n in range(1, units):
        unit = unit + jnp.where(row >= n * step, 1, 0)
    inside = row - unit * step
    source = (2 * unit + core) * span + inside
    return jnp.where((source == column) & (inside < span), 1.0, 0.0)


def backward_kernel(depth, layers, narrow, span, step, *refs):
    refs = list(refs)

    def take(number):
        taken = refs[:number]
        del refs[:number]
        return taken

    text_count = TEXT_MEMBERS * layers
    count = (TEXT_MEMBERS + 1) * layers
    gathered = take(text_count)
    kept = take(len(SAVED))
    vec_ref, text_cot, layout_cot, onehot = take(4)
    finals = take(count)
    vector_out, text_out, layout_out = take(3)
    m = SimpleNamespace()
    for name in SAVED + BACK_SCRATCH:
        setattr(m, name, refs.pop(0))
    mine_text, mine_small = take(2)
    landed_diag, landed_plane, landed_line = take(count), take(count), take(count)
    outs = take(count)
    weight_sem, keep_sem, out_sem, xs, xr, ps, pr, zs, zr = take(9)
    all_sum = take(4)
    at, devices = place(depth)
    dp, z, core, dx, dy, dd = at.dp, at.z, at.core, at.dx, at.dy, at.dd
    fill = 1
    owners = (dp, dx, dy, dd)
    half = depth // 2
    low = jnp.bfloat16
    tokens, width = m.gx.shape
    hidden_small = m.upper_low_small.shape[1]
    signal(devices)
    greeted()
    vectors = AllSum(devices, vector_out, *all_sum)

    slots, reuse = {}, {}
    for k in range(count):
        if k % 4 != 3:
            spare = [n for n in range(mine_text.shape[0]) if n not in slots.values()]
            if spare:
                slots[k] = spare[0]
            else:
                reuse[k] = min(n for n in slots if n != fill and n not in reuse.values())
                slots[k] = slots[reuse[k]]

    def mine(k):
        if k % 4 == 3:
            return mine_small.at[k // 4]
        return mine_text.at[slots[k]]

    order = []
    for layer in reversed(range(layers)):
        order += [3 * layer + 2, 3 * layer + 1, 3 * layer]

    def weight_load(index):
        return pltpu.make_async_copy(
            gathered[order[index]], m.weights.at[index % 2], weight_sem.at[index]
        )

    def saved_load(name, layer):
        index = SAVED.index(name)
        return pltpu.make_async_copy(
            kept[index].at[layer], getattr(m, name), keep_sem.at[index, layer]
        )

    def cross(layer, link):
        moves = (
            (m.low, m.in_land.at[layer, pl.ds(0, 3)]),
            (m.turned.at[:, :, 1 - core], m.rows_land.at[layer, 0]),
            (m.down_low, m.in_land.at[layer, 3]),
            (m.rows_up.at[:, :, 1 - core], m.rows_land.at[layer, 1]),
            (m.rows_attn.at[:, :, 1 - core], m.rows_land.at[layer, 2]),
            (m.low_small, m.in_land_small.at[layer, pl.ds(0, 3)]),
            (m.turned_small, m.rows_land_small.at[layer, 0]),
            (m.down_low_small, m.in_land_small.at[layer, 3]),
            (m.rows_small.at[0], m.rows_land_small.at[layer, 1]),
            (m.rows_small.at[1], m.rows_land_small.at[layer, 2]),
        )
        source, target = moves[link]
        return remote(
            source, target, xs.at[layer, link], xr.at[layer, link], devices.core
        )

    def plane(k, index):
        if k == fill:
            size = landed_diag[k].shape[1]
            lower, upper = pl.ds(0, size), pl.ds(size, size)
            own = lambda owner, rows: mine(k).at[owner, z, rows]
        else:
            lower, upper = pl.ds(0, half), pl.ds(half, half)
            own = lambda owner, levels: mine(k).at[owner, levels]
        diag, direct = landed_diag[k], landed_plane[k]
        moves = (
            (dd, lower, diag.at[0], devices.y),
            (dd, upper, diag.at[1], devices.x),
            (dx, upper, direct.at[0, upper], devices.x),
            (dy, lower, direct.at[1, lower], devices.y),
            (dx, lower, direct.at[0, lower], devices.x),
            (dy, upper, direct.at[1, upper], devices.y),
        )
        owner, part, target, device = moves[index]
        return remote(own(owner, part), target, ps.at[k, index], pr.at[k, index], device)

    def line(k, rising, level, slot, side=0):
        row = k if side == 0 else count - 1 + side
        return remote(
            mine(k).at[owners[side], level],
            landed_line[k].at[slot, side],
            zs.at[row, int(rising), level],
            zr.at[row, int(rising), level],
            devices.up if rising else devices.down,
        )

    def second_sums(k):
        if k == fill:
            size = landed_diag[k].shape[1]
            lower, upper = pl.ds(0, size), pl.ds(size, size)
            one, other = mine(k).at[dx, z, lower], mine(k).at[dy, z, upper]
            add = add_rows
        else:
            one = mine(k).at[dx, pl.ds(0, half)]
            other = mine(k).at[dy, pl.ds(half, half)]
            add = add_units
        plane(k, 0).wait_recv()
        add(one, landed_diag[k].at[0])
        plane(k, 4).start()
        plane(k, 1).wait_recv()
        add(other, landed_diag[k].at[1])
        plane(k, 5).start()

    def third_sums(k):
        for index in (2, 3, 4, 5):
            plane(k, index).wait_recv()
        if k == fill:
            result = mine(k)[dp, z].astype(jnp.float32)
            for side in range(2):
                result = result + landed_plane[k][side].astype(jnp.float32)
            outs[k][...] = result
            put_out(k).start()
        else:
            add_units(mine(k).at[dp], landed_plane[k].at[0], landed_plane[k].at[1])
            line_step(k, 0)

    def passed(rising, hop):
        return range(hop + 1, depth) if rising else range(depth - 1 - hop)

    def line_step(k, hop, side=0):
        for rising in (True, False):

            @pl.when(z == (hop if rising else depth - 1 - hop))
            def move():
                for level in passed(rising, hop):
                    if hop > 0:
                        line(k, rising, level, level, side).wait_recv()
                        add_rows(mine(k).at[owners[side], level], landed_line[k].at[level, side])
                    last = rising and level == hop + 1
                    line(k, rising, level, depth if last else level, side).start()

    def last_sums(k, side=0):
        if k != fill:
            outs[k][...] = mine(k)[dp, z].astype(jnp.float32)
        for rising in (True, False):

            @pl.when((z > 0) if rising else (z < depth - 1))
            def add():
                slot = depth if rising else z
                line(k, rising, z, slot, side).wait_recv()
                if k == fill:
                    add_rows(mine(k).at[owners[side], z], landed_line[k].at[slot, side])
                else:
                    outs[k][...] += landed_line[k][slot, side].astype(jnp.float32)

        if k != fill:
            put_out(k).start()

    def put_out(k):
        return pltpu.make_async_copy(outs[k], finals[k], out_sem.at[k])

    def fill_plane():
        for index in range(4):
            plane(fill, index).start()

    def drain(k):
        for index in range(6):
            plane(k, index).wait_send()
        for hop in range(depth - 1):
            for rising in (True, False):

                @pl.when(z == (hop if rising else depth - 1 - hop))
                def wait():
                    for level in passed(rising, hop):
                        for side in range(PLANE if k == fill else 1):
                            line(k, rising, level, level, side).wait_send()

    plan = Plan()
    size = [outs[k].shape[0] / UNIT_ROWS_PER_US for k in range(count)]

    def add_scatter(k, rank):
        one = size[k]

        def step(hop, side):
            if hop < depth - 1:
                line_step(k, hop, side)
            else:
                last_sums(k, side)

        for side in range(PLANE if k == fill else 1):
            for hop in range(0 if k == fill else 1, depth):
                sends = []
                if hop < depth - 1:
                    sends.append((("z", hop), (depth - 1 - hop) * one, ("z", hop + 1, k, side)))
                after = [("z", hop - 1, k, side)] if hop else [("o", k)]
                if k != fill and hop == 1:
                    after = [("s", 3, k)]
                if k == fill and hop == 0 and side:
                    after.append(("z", 1, k, side - 1))
                needs = [("z", hop, k, side)] if hop else []
                plan.add(
                    ("z", hop, k, side), functools.partial(step, hop, side), after, needs, sends, 0.3, rank
                )
        first = ("o", k)
        share = 2 * one
        if k == fill:
            first, share = ("f", 0), one / 2
            sends = [("x", share, ("d", k)), ("x", share, ("e", k))]
            ends = [("z", depth - 1, k, side) for side in range(PLANE)]
            plan.add(first, fill_plane, ends, [], sends, 0.2, rank)
        plan.add(
            ("s", 2, k), functools.partial(second_sums, k), [first], [("d", k)], [("x", share, ("g", k))], 0.5, rank
        )
        sends = [(("z", 0), (depth - 1) * one, ("z", 1, k, 0))] if k != fill else []
        plan.add(
            ("s", 3, k), functools.partial(third_sums, k), [("s", 2, k)], [("e", k), ("g", k)], sends, 1.0, rank
        )

    def own_sends(k):
        if k == fill:
            return []
        return [("x", 2 * size[k], ("d", k)), ("x", 2 * size[k], ("e", k))]

    previous = []

    def then(name, run, time, needs=(), sends=(), after=()):
        plan.add(name, run, previous + list(after), needs, sends, time, 1000, True)
        previous[:] = [name]

    def done(k):
        return [("s", 3, k), ("z", depth - 1, k, 0)]

    def own_sums(k, rows, rows_land, ins, ins_land):
        if k in reuse:
            drain(reuse[k])

        def block(turn, carry):
            owner = jnp.where(turn == 0, dd, jnp.where(turn == 1, dx, jnp.where(turn == 2, dy, dp)))
            left = jnp.concatenate(
                [
                    rows[owner, :, core].reshape(-1, tokens),
                    rows_land[owner].reshape(-1, tokens),
                ],
                axis=1,
            )
            right = jnp.concatenate([ins(owner), ins_land(owner)], axis=0)
            result = dot_nn(left, right)
            mine(k)[owner] = result.astype(low).reshape(depth, -1, width)
            if k != fill:
                for index, when in enumerate((0, 0, 1, 2)):

                    @pl.when(turn == when)
                    def send():
                        plane(k, index).start()

            return carry

        lax.fori_loop(0, PLANE, block, 0)

    m.gx[...] = text_cot[...].astype(jnp.float32)
    m.gy[...] = jnp.zeros_like(m.gy)
    m.gy[:, 0:narrow] = layout_cot[...].astype(jnp.float32).T
    first_names = ("norm", "scales", "turned", "norm_small", "turned_small", "slope", "low")
    names = first_names + tuple(name for name in SAVED if name not in first_names)
    weight_load(0).start()
    for name in names:
        saved_load(name, layers - 1).start()
    weight_load(1).start()

    def add_layer(turn, layer):
        k = 4 * turn
        vec = lambda row, n=1: vec_ref[pl.ds(layer * VECTOR_ROWS + row, n), :]
        small_vec = lambda row: vec(SMALL_ROW + row)[:, :PAD]
        slot = lambda member: m.weights.at[(3 * turn + member) % 2]

        def put(row, value):
            m.sums[pl.ds(layer * VECTOR_ROWS + row, 1), :] = value

        def put_small(row, value):
            m.sums[pl.ds(layer * VECTOR_ROWS + SMALL_ROW + row, 1), :PAD] = value


        def tail():
            m.sums[pl.ds(layer * VECTOR_ROWS + SMALL_ROW, VECTOR_ROWS - SMALL_ROW), :] = jnp.zeros(
                (VECTOR_ROWS - SMALL_ROW, width), jnp.float32
            )
            for name in ("norm", "scales", "turned"):
                saved_load(name, layer).wait()
            cross(layer, 1).start()
            grad, gain_sum, shift_sum = standard_back(
                m.gx[...], m.norm[1], m.scales[2][:, :1], vec(6), width
            )
            put(6, gain_sum)
            put(7, shift_sum)
            m.gx[...] = grad
            m.down_low[...] = grad.astype(low)
            cross(layer, 2).start()
            put(3, total(m.down_low[...]))

        def tail_small():
            for name in ("norm_small", "turned_small"):
                saved_load(name, layer).wait()
            cross(layer, 6).start()
            grad, gain_sum, shift_sum = standard_back(
                m.gy[...], m.norm_small[1], m.scales[3][:, :1], small_vec(6), narrow
            )
            put_small(6, gain_sum)
            put_small(7, shift_sum)
            m.gy[...] = grad
            m.down_low_small[...] = grad.astype(low)
            cross(layer, 7).start()
            put_small(3, total(m.down_low_small[...]))

        def own_down():
            cross(layer, 1).wait_recv()
            cross(layer, 2).wait_recv()
            own_sums(
                k,
                m.turned,
                m.rows_land.at[layer, 0],
                lambda owner: m.down_low[...],
                lambda owner: m.in_land[layer, 3],
            )

        cut = 3 * LANE

        def hidden(block, carry):
            m.wide[...] = dot_nt(m.down_low[...], unit_rows(slot(0), block))
            for side in range(width // cut):
                inside = pl.ds(side * cut, cut)
                columns = pl.ds(pl.multiple_of(block * width + side * cut, LANE), cut)
                rows = m.slope[:, columns] * m.wide[:, inside]
                rows_low = rows.astype(low)
                m.upper_low[:, columns] = rows_low
                m.sums[pl.ds(layer * VECTOR_ROWS + 8 + block, 1), inside] = total(rows_low)
                levels = depth * cut // width
                m.rows_up[block, pl.ds(side * levels, levels)] = (
                    rows.T.astype(low).reshape(levels, 2, -1, tokens)
                )
            return carry


        def hidden_blocks(first, number):
            if first == 0:
                for name in names[5:]:
                    saved_load(name, layer).wait()
                cross(layer, 0).start()
                cross(layer, 5).start()
                weight_load(3 * turn).wait()
            lax.fori_loop(first, first + number, hidden, 0)
            if first + number == PLANE:
                cross(layer, 3).start()
                if 3 * turn + 2 < 3 * layers:
                    weight_load(3 * turn + 2).start()

        def hide_small():
            m.wide[...] = dot_nt(m.down_low_small[...], m.small_ff[1])

            for side in range(hidden_small // cut):
                columns = pl.ds(side * cut, cut)
                rows = m.slope_small[:, columns] * m.wide[:, columns]
                rows_low = rows.astype(low)
                m.upper_low_small[:, columns] = rows_low
                m.rows_small[0, columns, :] = rows.T.astype(low)
                m.sums[
                    pl.ds(layer * VECTOR_ROWS + SMALL_HIDDEN_ROW, 1), columns
                ] = total(rows_low)
            cross(layer, 8).start()

        def own_up():
            cross(layer, 0).wait_recv()
            cross(layer, 3).wait_recv()
            own_sums(
                k + 1,
                m.rows_up,
                m.rows_land.at[layer, 1],
                lambda owner: m.low[2],
                lambda owner: m.in_land[layer, 2],
            )

        def lower_text():
            weight_load(3 * turn + 1).wait()

            def lower(block, carry):
                columns = pl.ds(pl.multiple_of(block * width, LANE), width)
                m.gx[...] += dot_nn(m.upper_low[:, columns], unit_rows(slot(1), block))
                return carry

            lax.fori_loop(0, PLANE, lower, 0)
            if 3 * turn + 3 < 3 * layers:
                weight_load(3 * turn + 3).start()
            grad, gain_sum, shift_sum = standard_back(
                m.gx[...], m.norm[0], m.scales[0][:, :1], vec(4), width
            )
            put(4, gain_sum)
            put(5, shift_sum)
            m.gx[...] = grad
            m.branch_low[...] = grad.astype(low)
            put(2, total(m.branch_low[...]))
            for side in range(width // cut):
                levels = depth * cut // width
                tile = m.gx[:, side * cut : (side + 1) * cut]
                m.rows_attn[3, pl.ds(side * levels, levels)] = (
                    tile.T.astype(low).reshape(levels, 2, -1, tokens)
                )

        def lower_small():
            grad = m.gy[...] + dot_nn(m.upper_low_small[...], m.small_ff[0])
            grad, gain_sum, shift_sum = standard_back(
                grad, m.norm_small[0], m.scales[1][:, :1], small_vec(4), narrow
            )
            put_small(4, gain_sum)
            put_small(5, shift_sum)
            m.gy[...] = grad
            m.branch_low_small[...] = grad.astype(low)
            put_small(2, total(m.branch_low_small[...]))
            m.rows_small[1, pl.ds(3 * narrow, narrow), :] = grad.T[:narrow].astype(low)

        def contexts():
            weight_load(3 * turn + 2).wait()
            m.context[...] = dot_nn(m.branch_low[...], unit_rows(slot(2), 3)).astype(low)
            m.context_small[...] = dot_nn(m.branch_low_small[...], m.small_attn[3]).astype(low)
            m.mixed[...] = jnp.zeros_like(m.mixed)

        def pair_back(pair, carry):
            lanes = pl.ds(pl.multiple_of(pair * LANE, LANE), LANE)
            query, keyed, valued = (m.heads[n, :, lanes] for n in range(3))
            small_query, small_keyed, small_valued = (m.heads_small[n] for n in range(3))
            context, context_small = m.context[:, lanes], m.context_small[...]
            lane, small_lane = lane_of((1, LANE)), lane_of((1, PAD))
            results = []
            for side in range(2):
                head = 2 * pair + side
                chosen = (lane >= 64 * side) & (lane < 64 * side + 64)
                small_chosen = (small_lane >= 16 * head) & (small_lane < 16 * head + 16)
                mask = jnp.where(chosen, 1.0, 0.0).astype(low)
                small_mask = jnp.where(small_chosen, 1.0, 0.0).astype(low)
                probs = m.probs[head]
                grad_probs = dot_nt(context * mask, valued) + dot_nt(
                    context_small * small_mask, small_valued
                )
                inner = jnp.sum(grad_probs * probs, axis=1, keepdims=True)
                scores = probs * (grad_probs - inner)
                scores_low = scores.astype(low)
                scores_turned = scores.T.astype(low)
                probs_turned = probs.T.astype(low)
                results.append(
                    (
                        dot_nn(scores_low, keyed) * 0.125,
                        dot_nn(scores_turned, query) * 0.125,
                        dot_nn(probs_turned, context),
                    )
                )
                small = (
                    dot_nn(scores_low, small_keyed) * 0.25,
                    dot_nn(scores_turned, small_query) * 0.25,
                    dot_nn(probs_turned, context_small),
                )
                for n in range(3):
                    m.mixed[n] += jnp.where(small_chosen, small[n], 0.0)
            for n in range(3):
                m.joined[n, :, lanes] = jnp.where(lane < 64, results[0][n], results[1][n]).astype(
                    low
                )
            return carry


        def pairs(first, number):
            lax.fori_loop(first, first + number, pair_back, 0)

        def turn_rows():
            for part in range(3):
                for side in range(width // cut):
                    levels = depth * cut // width
                    tile = m.joined[part, :, side * cut : (side + 1) * cut].astype(jnp.float32)
                    m.rows_attn[part, pl.ds(side * levels, levels)] = (
                        tile.T.astype(low).reshape(levels, 2, -1, tokens)
                    )
                tile = m.mixed[part].astype(low).astype(jnp.float32)
                m.rows_small[1, pl.ds(part * narrow, narrow), :] = tile.T[:narrow].astype(low)
            cross(layer, 4).start()
            cross(layer, 9).start()
            put(0, total(m.joined[0]))
            put(1, total(m.joined[2]))
            put_small(0, total(m.mixed[0].astype(low)))
            put_small(1, total(m.mixed[2].astype(low)))

        def entering(part, carry):
            m.gx[...] += dot_nn(m.joined[part], unit_rows(slot(2), part))
            return carry


        def attn_sums():
            cross(layer, 4).wait_recv()
            own_sums(
                k + 2,
                m.rows_attn,
                m.rows_land.at[layer, 2],
                lambda owner: m.low[jnp.where(owner == PLANE - 1, 1, 0)],
                lambda owner: m.in_land[layer, jnp.where(owner == PLANE - 1, 1, 0)],
            )


        def enter():
            lax.fori_loop(0, 3, entering, 0)
            if 3 * turn + 4 < 3 * layers:
                weight_load(3 * turn + 4).start()
            grad = m.gy[...]
            for part in range(3):
                grad = grad + dot_nn(m.mixed[part].astype(low), m.small_attn[part])
            m.gy[...] = grad
            for group in range(LANGS):
                put(TABLE_ROW + group, total(onehot[:, group : group + 1] * m.gx[...]))
            if layer == 0:
                text_out[...] = m.gx[...]
                layout_out[...] = m.gy[:, 0:narrow].T
                vector_out[...] = m.sums[...]
                vectors.send(0)

        def small_sums():
            for link in (5, 6, 7, 8, 9):
                cross(layer, link).wait_recv()
            arrange = padded_rows_of_core(span, step, core).astype(low)
            small_rows = (m.rows_small.at[1], m.rows_small.at[0], m.turned_small)
            small_land = (2, 1, 0)
            for member in range(3):
                for block in range(PLANE):
                    rows = pl.ds(block * narrow, narrow)
                    source = (1 if block == PLANE - 1 else 0, 2, 3)[member]
                    own_in = m.down_low_small[...] if member == 2 else m.low_small[source]
                    left = jnp.concatenate(
                        [
                            small_rows[member][rows, :],
                            m.rows_land_small[layer, small_land[member], rows, :],
                        ],
                        axis=1,
                    )
                    right = jnp.concatenate([own_in, m.in_land_small[layer, source]], axis=0)
                    placed = dot_nn(arrange, dot_nn(left, right).astype(low)).astype(low)
                    mine(k + 3)[block, :, :, pl.ds(member * PAD, PAD)] = placed.reshape(
                        depth, step, PAD
                    )
            if layer > 0:
                for link in range(LINKS):
                    cross(layer, link).wait_send()
                for name in names:
                    saved_load(name, layer - 1).start()
            for index in range(4):
                plane(k + 3, index).start()

        own = lambda n: ("o", k + n)
        crossed = lambda link: ("c", layer, link)
        free = lambda n: done(reuse[k + n]) if k + n in reuse else []
        then(("t", 0, turn), tail, 1.7, sends=[("c", 1.0, crossed(1)), ("c", 0.5, crossed(2))])
        then(("t", 1, turn), tail_small, 0.2, sends=[("c", 0.8, crossed(6))])
        then(own(0), own_down, 1.4, [crossed(1), crossed(2)], own_sends(k), free(0))
        add_scatter(k, 4 * k)
        then(
            ("h", 0, turn), functools.partial(hidden_blocks, 0, 2), 1.4, sends=[("c", 1.5, crossed(0))]
        )
        then(
            ("h", 1, turn), functools.partial(hidden_blocks, 2, 2), 1.3, sends=[("c", 1.0, crossed(3))]
        )
        then(("h", 2, turn), hide_small, 0.4, sends=[("c", 0.5, crossed(8))])
        then(own(1), own_up, 1.4, [crossed(0), crossed(3)], own_sends(k + 1), free(1))
        add_scatter(k + 1, 4 * k + 4)
        then(("n", 0, turn), lower_text, 1.7)
        then(("n", 1, turn), lower_small, 0.4)
        then(("n", 2, turn), contexts, 0.4)
        then(("p", 0, turn), functools.partial(pairs, 0, H // 4), 2.7)
        then(("p", 1, turn), functools.partial(pairs, H // 4, H // 4), 2.7)
        then(("r", turn), turn_rows, 0.4, sends=[("c", 1.0, crossed(4)), ("c", 0.5, crossed(9))])
        then(own(2), attn_sums, 1.4, [crossed(4)], own_sends(k + 2), free(2))
        add_scatter(k + 2, 4 * k + 8)
        then(("e", turn), enter, 1.4, sends=[("c", 0.3, ("v", 0))] if layer == 0 else [])
        late = [("s", 2, k + 2)] if layer == 0 else []
        then(own(3), small_sums, 2.6, [crossed(9)], own_sends(k + 3), late)
        add_scatter(k + 3, 4 * k + 12)

    for turn, layer in enumerate(reversed(range(layers))):
        add_layer(turn, layer)
    for n in range(AllSum.STEPS):
        sends = [((("z", 0), 2.2), (("z", 0), 4.4), ("x", 2.2), ("x", 2.2), ("c", 0.0))[n] + (("v", n + 1),)]
        after = [("v", n - 1)] if n else [("e", layers - 1)]
        plan.add(("v", n), functools.partial(vectors.advance, n), after, [("v", n)], sends, 0.2, -1)
    plan.run()
    vectors.close()
    for link in range(LINKS):
        cross(0, link).wait_send()
    drained = list(reuse.values())
    for k in range(count):
        put_out(k).wait()
    for k in range(count):
        if k not in drained:
            drain(k)


def run_backward(depth, layers, narrow, span, step, gathered, saved, vectors, text_cot, layout_cot, onehot):
    dma = pltpu.SemaphoreType.DMA
    tokens, width = text_cot.shape
    low, full = jnp.bfloat16, jnp.float32
    shapes = back_shapes(layers, depth, tokens, width, 4 * narrow)
    unit = gathered[0].shape[3:]
    small_unit = (step, width)
    units = [small_unit if k % 4 == 3 else unit for k in range(4 * layers)]
    count = len(units)
    whole = (layers, PLANE, depth, 2, -1, tokens)
    kept = [
        array.reshape(whole) if array.ndim == 3 and array.shape[1] == 4 * width else array
        for array in saved
    ]
    scratch = [pltpu.VMEM(array.shape[1:], array.dtype) for array in kept]
    scratch += [pltpu.VMEM(*shapes[name]) for name in BACK_SCRATCH]
    scratch += [
        pltpu.VMEM((4, PLANE, depth) + unit, low),
        pltpu.VMEM((layers, PLANE, depth) + small_unit, low),
    ]
    fill = 1
    landing = [((2, depth // 2) + one, (2, depth) + one, (depth + 1, 1) + one) for one in units]
    landing[fill] = (
        (2, unit[0] // 2, width),
        (2,) + unit,
        (depth + 1, PLANE) + unit,
    )
    for n in range(3):
        scratch += [pltpu.VMEM(shapes_of[n], low) for shapes_of in landing]
    scratch += [pltpu.VMEM(one, full) for one in units]
    scratch += [
        dma((len(gathered),)),
        dma((len(SAVED), layers)),
        dma((count,)),
        dma((layers, LINKS)),
        dma((layers, LINKS)),
        dma((count, 6)),
        dma((count, 6)),
        dma((count + 3, 2, depth)),
        dma((count + 3, 2, depth)),
    ]
    scratch += AllSum.scratch(vectors.shape)
    results = pl.pallas_call(
        functools.partial(backward_kernel, depth, layers, narrow, span, step),
        out_shape=[jax.ShapeDtypeStruct(one, full) for one in units]
        + [
            jax.ShapeDtypeStruct(vectors.shape, full),
            jax.ShapeDtypeStruct((tokens, width), full),
            jax.ShapeDtypeStruct((narrow, tokens), full),
        ],
        in_specs=[ANY] * (len(gathered) + len(kept)) + [IN_VMEM] * 4,
        out_specs=[ANY] * count + [IN_VMEM] * 3,
        scratch_shapes=scratch,
        compiler_params=pltpu.CompilerParams(
            collective_id=1, has_side_effects=True, vmem_limit_bytes=67000000
        ),
        name="backward_blocks",
    )(*gathered, *kept, vectors, text_cot, layout_cot, onehot)
    return results


def finish_kernel(depth, layers, narrow, span, small_span, *refs):
    count = 4 * layers
    summed, totals, ins = refs[:count], refs[count], refs[count + 1 : count + 5]
    outs = refs[count + 5 :]
    width = ins[0].shape[1]
    at, unused = place(depth)
    for n in range(4):
        outs[n][...] = ins[n][...]
    attn, up, down = outs[4:7]
    pieces = outs[7:9] + outs[12:13]
    small_attn, small_up, small_down = outs[9:12]
    for layer in range(layers):
        parts = summed[4 * (layers - 1 - layer) :]
        down[layer] = parts[0][...]
        up[layer] = parts[1][...]
        attn[layer] = parts[2][...]
        small = parts[3]
        small_attn[layer] = small[0:small_span, 0:narrow]
        small_up[layer] = small[0:small_span, PAD : PAD + narrow]
        small_down[layer] = small[0:small_span, 2 * PAD : 2 * PAD + narrow]
    lane = lane_of((layers, width))
    found = [jnp.zeros((layers, width), jnp.float32) for piece in pieces]
    for row, n, base, lanes in flat_rows(width, narrow):
        first = at.me * pieces[n].shape[1] - base
        rows = jnp.concatenate(
            [totals[pl.ds(layer * VECTOR_ROWS + row, 1), :] for layer in range(layers)], axis=0
        )
        rolled = pltpu.roll(rows, lax.rem(16 * width - first, width), 1)
        index = lane + first
        found[n] = found[n] + jnp.where((index >= 0) & (index < lanes), rolled, 0.0)
    for n, piece in enumerate(pieces):
        piece[...] = found[n][:, : piece.shape[1]]


def run_finish(depth, layers, narrow, span, small_span, lengths, results, text_out, layout_out):
    count = 4 * layers
    summed, (totals, text_grad, layout_grad) = results[:count], results[count:]
    tokens, width = text_out.shape
    shapes = [
        (tokens, width),
        (narrow, tokens),
        (tokens, width),
        (narrow, tokens),
        (layers, span, width),
        (layers, span, width),
        (layers, span, width),
        (layers, lengths[0]),
        (layers, lengths[1]),
        (layers, small_span, narrow),
        (layers, small_span, narrow),
        (layers, small_span, narrow),
        (layers, lengths[2]),
    ]
    return pl.pallas_call(
        functools.partial(finish_kernel, depth, layers, narrow, span, small_span),
        out_shape=[jax.ShapeDtypeStruct(shape, jnp.float32) for shape in shapes],
        in_specs=[IN_VMEM] * (count + 5),
        out_specs=[IN_VMEM] * len(shapes),
        name="finish",
    )(*summed, totals, text_out, layout_out, text_grad, layout_grad)


def block_shards(
    depth,
    text_input,
    layout_input,
    text_cot,
    layout_cot,
    segment_ids,
    page_groups,
    lang_table,
    text_attn,
    text_up,
    text_down,
    text_vector,
    layout_attn,
    layout_up,
    layout_down,
    layout_vector,
):
    layers, unused, span = text_attn.shape
    narrow, small_span = layout_input.shape[1], layout_down.shape[1]
    step = PAD * PLANE // (PLANE * depth * 2)

    def turned(array):
        return jnp.swapaxes(array, -1, -2)

    weights = (
        turned(text_attn),
        turned(text_up),
        text_down,
        turned(layout_attn),
        turned(layout_up),
        layout_down,
    )
    pieces = (text_vector, lang_table, layout_vector)
    gathered, (vectors, onehot, text_out, layout_out), saved = run_forward(
        depth,
        narrow,
        step,
        weights,
        pieces,
        text_input,
        turned(layout_input),
        segment_ids.reshape(1, -1),
        page_groups.reshape(1, -1),
    )
    text_gathered = [part for n, part in enumerate(gathered) if n != 1]
    results = run_backward(
        depth,
        layers,
        narrow,
        small_span,
        step,
        text_gathered,
        saved,
        vectors,
        text_cot,
        turned(layout_cot),
        onehot,
    )
    lengths = [piece.shape[1] for piece in pieces]
    outs = run_finish(
        depth, layers, narrow, span, small_span, lengths, results, text_out, layout_out
    )
    return tuple(turned(out) if n in (1, 3, 4, 5, 9, 10) else out for n, out in enumerate(outs))


def solution(mesh):
    in_specs = (
        P(AXES, None),
        P(AXES, None),
        P(AXES, None),
        P(AXES, None),
        P(AXES),
        P(AXES),
        P(None, AXES),
        P(None, None, AXES),
        P(None, None, AXES),
        P(None, AXES, None),
        P(None, AXES),
        P(None, None, AXES),
        P(None, None, AXES),
        P(None, AXES, None),
        P(None, AXES),
    )
    out_specs = (
        P(AXES, None),
        P(AXES, None),
        P(AXES, None),
        P(AXES, None),
        P(None, None, AXES),
        P(None, None, AXES),
        P(None, AXES, None),
        P(None, AXES),
        P(None, AXES),
        P(None, None, AXES),
        P(None, None, AXES),
        P(None, AXES, None),
        P(None, AXES),
    )
    plan = functools.partial(block_shards, mesh.shape[AXES[1]] // 2) if fits_blocks(mesh) else generic_shards
    return jax.shard_map(plan, mesh=mesh, in_specs=in_specs, out_specs=out_specs, check_vma=False)
```

```python
import functools
import math
from types import SimpleNamespace

import jax
import jax.numpy as jnp
from jax import lax
from jax.experimental import pallas as pl
from jax.experimental.pallas import tpu as pltpu
from jax.sharding import PartitionSpec as P

H = 12
LANGS = 8


EPSILON = 1e-05
MASKED = -1e30


def norm_rows(residual, norm_gain, norm_shift):
    average = jnp.mean(residual, axis=-1, keepdims=True)
    centred = residual - average
    variance = jnp.mean(centred * centred, axis=-1, keepdims=True)
    return centred * lax.rsqrt(variance + EPSILON) * norm_gain + norm_shift


def exact_gelu(values):
    return jax.nn.gelu(values, approximate=False)


def norm_back(residual, norm_gain, norm_shift, grad_rows):
    unused, pullback = jax.vjp(norm_rows, residual, norm_gain, norm_shift)
    return pullback(grad_rows)


def gelu_back(upper, grad_rows):
    unused, pullback = jax.vjp(exact_gelu, upper)
    return pullback(grad_rows)[0]


def column_sum(matrix):
    return jnp.sum(matrix.astype(jnp.float32), axis=0)


def unpack(vector, stream_width, hidden_width):
    values = vector.astype(jnp.float32)
    pieces = [values[member * stream_width : (member + 1) * stream_width] for member in range(8)]
    return pieces + [values[8 * stream_width : 8 * stream_width + hidden_width]]


def project(stream_low, attn_weight, pieces):
    stream_width = stream_low.shape[1]
    joined = jnp.dot(
        stream_low, attn_weight[:, : 3 * stream_width], preferred_element_type=jnp.float32
    )
    head_shape = (stream_low.shape[0], H, stream_width // H)
    query = (joined[:, :stream_width] + pieces[0]).astype(jnp.bfloat16).reshape(head_shape)
    keyed = joined[:, stream_width : 2 * stream_width].astype(jnp.bfloat16).reshape(head_shape)
    valued = (joined[:, 2 * stream_width :] + pieces[1]).astype(jnp.bfloat16).reshape(head_shape)
    return (query, keyed, valued)


def joint_scores(text_heads, layout_heads, same_page):
    text_part = jnp.einsum(
        "shd,thd->hst", text_heads[0], text_heads[1], preferred_element_type=jnp.float32
    )
    layout_part = jnp.einsum(
        "shd,thd->hst", layout_heads[0], layout_heads[1], preferred_element_type=jnp.float32
    )
    combined = text_part * (1.0 / math.sqrt(text_heads[0].shape[2])) + layout_part * (
        1.0 / math.sqrt(layout_heads[0].shape[2])
    )
    return jnp.where(same_page[None], combined, MASKED)


def attend(probs_low, valued):
    context = jnp.einsum("hst,thd->shd", probs_low, valued, preferred_element_type=jnp.float32)
    return context.reshape(context.shape[0], -1).astype(jnp.bfloat16)


def tail_forward(stream_rows, context_low, attn_weight, up_weight, down_weight, pieces):
    stream_width = stream_rows.shape[1]
    branch = (
        jnp.dot(context_low, attn_weight[:, 3 * stream_width :], preferred_element_type=jnp.float32)
        + pieces[2]
    )
    first_sum = stream_rows + branch
    normed = norm_rows(first_sum, pieces[4], pieces[5])
    normed_low = normed.astype(jnp.bfloat16)
    upper = jnp.dot(normed_low, up_weight, preferred_element_type=jnp.float32) + pieces[8]
    active_low = exact_gelu(upper).astype(jnp.bfloat16)
    second_sum = (
        normed + jnp.dot(active_low, down_weight, preferred_element_type=jnp.float32) + pieces[3]
    )
    result = norm_rows(second_sum, pieces[6], pieces[7])
    return (result, (first_sum, normed_low, upper, active_low, second_sum))


def layer_forward(text_rows, layout_rows, text_weights, layout_weights, same_page, onehot):
    group_table = text_weights[4].astype(jnp.float32).reshape(onehot.shape[1], -1)
    text_rows = text_rows + jnp.dot(onehot, group_table, precision=lax.Precision.HIGHEST)
    text_pieces = unpack(text_weights[3], text_rows.shape[1], text_weights[1].shape[1])
    layout_pieces = unpack(layout_weights[3], layout_rows.shape[1], layout_weights[1].shape[1])
    text_low = text_rows.astype(jnp.bfloat16)
    layout_low = layout_rows.astype(jnp.bfloat16)
    text_heads = project(text_low, text_weights[0], text_pieces)
    layout_heads = project(layout_low, layout_weights[0], layout_pieces)
    scores = joint_scores(text_heads, layout_heads, same_page)
    row_peak = jnp.max(scores, axis=-1, keepdims=True)
    log_total = row_peak + jnp.log(jnp.sum(jnp.exp(scores - row_peak), axis=-1, keepdims=True))
    probs_low = jnp.exp(scores - log_total).astype(jnp.bfloat16)
    text_context = attend(probs_low, text_heads[2])
    layout_context = attend(probs_low, layout_heads[2])
    text_next, text_stored = tail_forward(
        text_rows, text_context, text_weights[0], text_weights[1], text_weights[2], text_pieces
    )
    layout_next, layout_stored = tail_forward(
        layout_rows,
        layout_context,
        layout_weights[0],
        layout_weights[1],
        layout_weights[2],
        layout_pieces,
    )
    stored = (
        text_low,
        layout_low,
        text_heads,
        layout_heads,
        log_total,
        text_context,
        layout_context,
        text_stored,
        layout_stored,
    )
    return (text_next, layout_next, stored)


def tail_backward(grad_result, stored, context_low, attn_weight, up_weight, down_weight, pieces):
    first_sum, normed_low, upper, active_low, second_sum = stored
    stream_width = first_sum.shape[1]
    grad_second, grad_gain_two, grad_shift_two = norm_back(
        second_sum, pieces[6], pieces[7], grad_result
    )
    grad_down_low = grad_second.astype(jnp.bfloat16)
    grad_down_bias = column_sum(grad_down_low)
    grad_down = jnp.einsum(
        "sf,sd->fd", active_low, grad_down_low, preferred_element_type=jnp.float32
    )
    grad_active = jnp.einsum(
        "sd,fd->sf", grad_down_low, down_weight, preferred_element_type=jnp.float32
    )
    grad_upper_low = gelu_back(upper, grad_active).astype(jnp.bfloat16)
    grad_up_bias = column_sum(grad_upper_low)
    grad_up = jnp.einsum(
        "sd,sf->df", normed_low, grad_upper_low, preferred_element_type=jnp.float32
    )
    grad_normed = grad_second + jnp.einsum(
        "sf,df->sd", grad_upper_low, up_weight, preferred_element_type=jnp.float32
    )
    grad_first, grad_gain_one, grad_shift_one = norm_back(
        first_sum, pieces[4], pieces[5], grad_normed
    )
    grad_branch_low = grad_first.astype(jnp.bfloat16)
    grad_out_bias = column_sum(grad_branch_low)
    output_weight = attn_weight[:, 3 * stream_width :]
    grad_output_proj = jnp.einsum(
        "sd,se->de", context_low, grad_branch_low, preferred_element_type=jnp.float32
    )
    grad_context = jnp.einsum(
        "se,de->sd", grad_branch_low, output_weight, preferred_element_type=jnp.float32
    ).astype(jnp.bfloat16)
    matrices = (grad_output_proj, grad_up, grad_down)
    vectors = (
        grad_out_bias,
        grad_down_bias,
        grad_gain_one,
        grad_shift_one,
        grad_gain_two,
        grad_shift_two,
        grad_up_bias,
    )
    return (grad_first, grad_context, matrices, vectors)


def head_grads(head_set, grad_context_low, probs_low, grad_scores_low):
    inverse_root = 1.0 / math.sqrt(head_set[0].shape[2])
    grad_heads = grad_context_low.reshape(head_set[2].shape)
    grad_query = (
        jnp.einsum("hst,thd->shd", grad_scores_low, head_set[1], preferred_element_type=jnp.float32)
        * inverse_root
    )
    grad_key = (
        jnp.einsum("hst,shd->thd", grad_scores_low, head_set[0], preferred_element_type=jnp.float32)
        * inverse_root
    )
    grad_value = jnp.einsum(
        "hst,shd->thd", probs_low, grad_heads, preferred_element_type=jnp.float32
    )
    row_count = head_set[0].shape[0]
    joined = jnp.concatenate(
        [
            grad_query.reshape(row_count, -1),
            grad_key.reshape(row_count, -1),
            grad_value.reshape(row_count, -1),
        ],
        axis=1,
    )
    return joined.astype(jnp.bfloat16)


def attention_backward(
    text_heads, layout_heads, log_total, same_page, grad_text_context, grad_layout_context
):
    scores = joint_scores(text_heads, layout_heads, same_page)
    probs = jnp.exp(scores - log_total)
    probs_low = probs.astype(jnp.bfloat16)
    grad_text_heads = grad_text_context.reshape(text_heads[2].shape)
    grad_layout_heads = grad_layout_context.reshape(layout_heads[2].shape)
    grad_probs = jnp.einsum(
        "shd,thd->hst", grad_text_heads, text_heads[2], preferred_element_type=jnp.float32
    )
    grad_probs = grad_probs + jnp.einsum(
        "shd,thd->hst", grad_layout_heads, layout_heads[2], preferred_element_type=jnp.float32
    )
    inner = jnp.sum(grad_probs * probs, axis=-1, keepdims=True)
    grad_scores_low = (probs * (grad_probs - inner)).astype(jnp.bfloat16)
    text_joined = head_grads(text_heads, grad_text_context, probs_low, grad_scores_low)
    layout_joined = head_grads(layout_heads, grad_layout_context, probs_low, grad_scores_low)
    return (text_joined, layout_joined)


def head_backward(stream_low, grad_joined_low, attn_weight, grad_first, matrices, vectors):
    stream_width = stream_low.shape[1]
    grad_in_proj = jnp.einsum(
        "sd,se->de", stream_low, grad_joined_low, preferred_element_type=jnp.float32
    )
    grad_bias_query = column_sum(grad_joined_low[:, :stream_width])
    grad_bias_value = column_sum(grad_joined_low[:, 2 * stream_width :])
    grad_stream = grad_first + jnp.einsum(
        "se,de->sd",
        grad_joined_low,
        attn_weight[:, : 3 * stream_width],
        preferred_element_type=jnp.float32,
    )
    grad_attn = jnp.concatenate([grad_in_proj, matrices[0]], axis=1)
    grad_vector = jnp.concatenate([grad_bias_query, grad_bias_value] + list(vectors))
    return (grad_stream, (grad_attn, matrices[1], matrices[2], grad_vector))


def layer_backward(grad_text, grad_layout, stored, text_weights, layout_weights, same_page, onehot):
    (
        text_low,
        layout_low,
        text_heads,
        layout_heads,
        log_total,
        text_context,
        layout_context,
        text_stored,
        layout_stored,
    ) = stored
    text_pieces = unpack(text_weights[3], text_low.shape[1], text_weights[1].shape[1])
    layout_pieces = unpack(layout_weights[3], layout_low.shape[1], layout_weights[1].shape[1])
    text_first, grad_text_context, text_mats, text_vecs = tail_backward(
        grad_text,
        text_stored,
        text_context,
        text_weights[0],
        text_weights[1],
        text_weights[2],
        text_pieces,
    )
    layout_first, grad_layout_context, layout_mats, layout_vecs = tail_backward(
        grad_layout,
        layout_stored,
        layout_context,
        layout_weights[0],
        layout_weights[1],
        layout_weights[2],
        layout_pieces,
    )
    text_joined, layout_joined = attention_backward(
        text_heads, layout_heads, log_total, same_page, grad_text_context, grad_layout_context
    )
    grad_text_in, text_terms = head_backward(
        text_low, text_joined, text_weights[0], text_first, text_mats, text_vecs
    )
    grad_layout_in, layout_terms = head_backward(
        layout_low, layout_joined, layout_weights[0], layout_first, layout_mats, layout_vecs
    )
    grad_group = jnp.einsum(
        "sg,sd->gd", onehot, grad_text_in, precision=lax.Precision.HIGHEST
    ).reshape(-1)
    return (grad_text_in, grad_layout_in, text_terms + (grad_group,), layout_terms)


def fetch_layer(
    text_attn,
    text_up,
    text_down,
    text_vector,
    lang_table,
    layout_attn,
    layout_up,
    layout_down,
    layout_vector,
    layer_index,
):
    fetched = (
        lax.all_gather(text_attn[layer_index], AXES, axis=1, tiled=True),
        lax.all_gather(text_up[layer_index], AXES, axis=1, tiled=True),
        lax.all_gather(text_down[layer_index], AXES, axis=0, tiled=True),
        lax.all_gather(text_vector[layer_index], AXES, axis=0, tiled=True),
        lax.all_gather(lang_table[layer_index], AXES, axis=0, tiled=True),
        lax.all_gather(layout_attn[layer_index], AXES, axis=1, tiled=True),
        lax.all_gather(layout_up[layer_index], AXES, axis=1, tiled=True),
        lax.all_gather(layout_down[layer_index], AXES, axis=0, tiled=True),
        lax.all_gather(layout_vector[layer_index], AXES, axis=0, tiled=True),
    )
    return (fetched[:5], fetched[5:])


def fetch_layer_back(
    text_attn,
    text_up,
    text_down,
    text_vector,
    lang_table,
    layout_attn,
    layout_up,
    layout_down,
    layout_vector,
    layer_index,
):
    fetched = (
        lax.all_gather(text_attn[layer_index], AXES, axis=1, tiled=True),
        lax.all_gather(text_up[layer_index], AXES, axis=1, tiled=True),
        lax.all_gather(text_down[layer_index], AXES, axis=0, tiled=True),
        lax.all_gather(text_vector[layer_index], AXES, axis=0, tiled=True),
        lax.all_gather(lang_table[layer_index], AXES, axis=0, tiled=True),
        lax.all_gather(layout_attn[layer_index], AXES, axis=1, tiled=True),
        lax.all_gather(layout_up[layer_index], AXES, axis=1, tiled=True),
        lax.all_gather(layout_down[layer_index], AXES, axis=0, tiled=True),
        lax.all_gather(layout_vector[layer_index], AXES, axis=0, tiled=True),
    )
    return (fetched[:5], fetched[5:])


def generic_shards(
    text_input,
    layout_input,
    text_cot,
    layout_cot,
    segment_ids,
    page_groups,
    lang_table,
    text_attn,
    text_up,
    text_down,
    text_vector,
    layout_attn,
    layout_up,
    layout_down,
    layout_vector,
):
    layer_count = text_attn.shape[0]
    same_page = segment_ids[:, None] == segment_ids[None, :]
    page_slot = segment_ids % 2
    token_group = jnp.where(page_slot == 0, page_groups[0], page_groups[1])
    onehot = (token_group[:, None] == jnp.arange(LANGS, dtype=jnp.int32)[None, :]).astype(
        jnp.float32
    )
    text_rows = text_input.astype(jnp.float32)
    layout_rows = layout_input.astype(jnp.float32)
    saved_layers = []
    for layer_index in range(layer_count):
        text_fetched, layout_fetched = fetch_layer(
            text_attn,
            text_up,
            text_down,
            text_vector,
            lang_table,
            layout_attn,
            layout_up,
            layout_down,
            layout_vector,
            layer_index,
        )
        text_rows, layout_rows, stored = layer_forward(
            text_rows, layout_rows, text_fetched, layout_fetched, same_page, onehot
        )
        saved_layers.append(stored)
    grad_text = text_cot.astype(jnp.float32)
    grad_layout = layout_cot.astype(jnp.float32)
    owned_all = [None] * layer_count
    for layer_index in reversed(range(layer_count)):
        text_fetched, layout_fetched = fetch_layer_back(
            text_attn,
            text_up,
            text_down,
            text_vector,
            lang_table,
            layout_attn,
            layout_up,
            layout_down,
            layout_vector,
            layer_index,
        )
        grad_text, grad_layout, text_terms, layout_terms = layer_backward(
            grad_text,
            grad_layout,
            saved_layers[layer_index],
            text_fetched,
            layout_fetched,
            same_page,
            onehot,
        )
        joined_terms = tuple(text_terms) + tuple(layout_terms)
        owned_all[layer_index] = (
            lax.psum_scatter(joined_terms[0], AXES, scatter_dimension=1, tiled=True),
            lax.psum_scatter(joined_terms[1], AXES, scatter_dimension=1, tiled=True),
            lax.psum_scatter(joined_terms[2], AXES, scatter_dimension=0, tiled=True),
            lax.psum_scatter(joined_terms[3], AXES, scatter_dimension=0, tiled=True),
            lax.psum_scatter(joined_terms[4], AXES, scatter_dimension=0, tiled=True),
            lax.psum_scatter(joined_terms[5], AXES, scatter_dimension=1, tiled=True),
            lax.psum_scatter(joined_terms[6], AXES, scatter_dimension=1, tiled=True),
            lax.psum_scatter(joined_terms[7], AXES, scatter_dimension=0, tiled=True),
            lax.psum_scatter(joined_terms[8], AXES, scatter_dimension=0, tiled=True),
        )
    stacks = [jnp.stack([owned[member] for owned in owned_all]) for member in range(9)]
    return (
        text_rows,
        layout_rows,
        grad_text,
        grad_layout,
        stacks[0],
        stacks[1],
        stacks[2],
        stacks[3],
        stacks[4],
        stacks[5],
        stacks[6],
        stacks[7],
        stacks[8],
    )


MESH = pl.DeviceIdType.MESH
AXES = ("dp", "shard")
ANY = pl.BlockSpec(memory_space=pl.ANY)
IN_VMEM = pl.BlockSpec(memory_space=pltpu.VMEM)
PLANE = 4
SUBLANES = 8
VECTOR_ROWS = 32


def fits_blocks(mesh):
    return mesh.shape[AXES[0]] == PLANE and mesh.shape[AXES[1]] == 2 * PLANE


def place(depth):
    dp, shard = lax.axis_index(AXES[0]), lax.axis_index(AXES[1])
    core, level = lax.rem(shard, 2), shard // 2
    dx = dp + 1 - 2 * lax.rem(dp, 2)
    dy = lax.rem(dp + 2, PLANE)
    me = dp * (2 * depth) + shard
    at = SimpleNamespace(dp=dp, z=level, core=core, dx=dx, dy=dy, dd=PLANE - 1 - dp, me=me)

    def device(plane_index, shard_index):
        return dict(zip(AXES, (plane_index, shard_index)))

    devices = SimpleNamespace(
        x=device(dx, shard),
        y=device(dy, shard),
        up=device(dp, lax.rem(shard + 2, 2 * depth)),
        down=device(dp, lax.rem(shard + 2 * depth - 2, 2 * depth)),
        far=device(dp, lax.rem(shard + depth, 2 * depth)),
        pair=device(dp, 2 * (level + 1 - 2 * lax.rem(level, 2)) + core),
        core=device(dp, shard + 1 - 2 * core),
    )
    return at, devices


def signal(devices):
    barrier = pltpu.get_barrier_semaphore()
    partners = (devices.x, devices.y, devices.up, devices.down, devices.far, devices.core)
    for partner in partners:
        pl.semaphore_signal(barrier, inc=1, device_id=partner, device_id_type=MESH)


def greeted():
    pl.semaphore_wait(pltpu.get_barrier_semaphore(), 6)


def remote(source, target, send_sem, recv_sem, device):
    return pltpu.make_async_remote_copy(
        src_ref=source,
        dst_ref=target,
        send_sem=send_sem,
        recv_sem=recv_sem,
        device_id=device,
        device_id_type=MESH,
    )


class AllSum:
    STEPS = 5

    def __init__(self, devices, running, held, landed, send_sem, recv_sem):
        self.partners = (devices.core, devices.pair, devices.far, devices.x, devices.y)
        self.running, self.held, self.landed = running, held, landed
        self.send_sem, self.recv_sem = send_sem, recv_sem

    def copy(self, step):
        return remote(
            self.held.at[step],
            self.landed.at[step],
            self.send_sem.at[step],
            self.recv_sem.at[step],
            self.partners[step],
        )

    def send(self, step):
        self.held[step] = self.running[...].astype(self.held.dtype)
        self.copy(step).start()

    def advance(self, step):
        self.copy(step).wait_recv()
        self.running[...] += self.landed[step].astype(jnp.float32)
        if step + 1 < self.STEPS:
            self.send(step + 1)

    def close(self):
        for step in range(self.STEPS):
            self.copy(step).wait_send()

    @classmethod
    def scratch(cls, shape):
        return [
            pltpu.VMEM((cls.STEPS,) + shape, jnp.bfloat16),
            pltpu.VMEM((cls.STEPS,) + shape, jnp.bfloat16),
            pltpu.SemaphoreType.DMA((cls.STEPS,)),
            pltpu.SemaphoreType.DMA((cls.STEPS,)),
        ]


class Plan:
    LAG = dict(x=2.4, z=2.4, c=1.0, h=0.3)
    PATIENCE = 1.0

    def __init__(self):
        self.tasks = []

    def add(self, name, run, after=(), needs=(), sends=(), time=0.2, rank=0, patient=False):
        self.tasks.append((name, run, tuple(after), tuple(needs), tuple(sends), time, rank, patient))

    def order(self):
        now, free, landed, done = 0.0, {}, {}, set()
        waiting, result = list(self.tasks), []
        while waiting:
            best = None
            for place_in_list, task in enumerate(waiting):
                name, run, after, needs, sends, time, rank, patient = task
                if any(other not in done for other in after):
                    continue
                if any(event not in landed for event in needs):
                    continue
                start = max([now] + [landed[event] for event in needs])
                key = (start + (self.PATIENCE if patient else 0.0), rank, place_in_list)
                if best is None or key < best[0]:
                    best = (key, task, start)
            assert best is not None
            task, start = best[1:]
            waiting.remove(task)
            result.append(task)
            name, run, after, needs, sends, time, rank, patient = task
            now = start + time
            done.add(name)
            for link, amount, event in sends:
                free[link] = max(now, free.get(link, 0.0)) + amount
                landed[event] = free[link] + self.LAG[link[0]]
        return result

    def run(self):
        for task in self.order():
            task[1]()


UNIT_ROWS_PER_US = 96 / 3.26


def add_rows(target, term):
    total = target[...].astype(jnp.float32) + term[...].astype(jnp.float32)
    target[...] = total.astype(target.dtype)


def add_units(target, *terms):
    def body(index, carry):
        total = target[index].astype(jnp.float32)
        for term in terms:
            total = total + term[index].astype(jnp.float32)
        target[index] = total.astype(target.dtype)
        return carry

    lax.fori_loop(0, target.shape[0], body, 0)


LANE = 128
PAD = 256
PIECE_ROWS = 12
TABLE_ROW = 12
SMALL_ROW = 20
SMALL_HIDDEN_ROW = 28


def dot_nt(left, right):
    return lax.dot_general(
        left, right, (((1,), (1,)), ((), ())), preferred_element_type=jnp.float32
    )


def dot_nn(left, right):
    return jnp.dot(left, right, preferred_element_type=jnp.float32)


def lane_of(shape):
    return lax.broadcasted_iota(jnp.int32, shape, len(shape) - 1)


def unit_rows(ref, dp):
    block = ref[dp]
    return block.reshape(-1, block.shape[-1])


def standard(residual, width):
    padded = residual.shape[1] != width
    average = jnp.sum(residual, axis=1, keepdims=True) * (1.0 / width)
    centred = residual - average
    if padded:
        centred = jnp.where(lane_of(residual.shape) < width, centred, 0.0)
    variance = jnp.sum(centred * centred, axis=1, keepdims=True) * (1.0 / width)
    scale = lax.rsqrt(variance + EPSILON)
    return centred * scale, scale


def gelu_parts(upper):
    cdf = 0.5 * (1.0 + lax.erf(upper * math.sqrt(0.5)))
    density = jnp.exp(upper * upper * -0.5) * (1.0 / math.sqrt(2.0 * math.pi))
    return upper * cdf, cdf + upper * density


def unit_of(index, size, count):
    unit = jnp.zeros(index.shape, jnp.int32)
    for n in range(1, count):
        unit = unit + jnp.where(index >= n * size, 1, 0)
    return unit


def natural_rows(span, layers, layer):
    units = 8
    shape = (PAD, units * layers * span)
    row = lax.broadcasted_iota(jnp.int32, shape, 0)
    column = lax.broadcasted_iota(jnp.int32, shape, 1)
    unit = unit_of(row, span, units)
    source = unit * (layers - 1) * span + layer * span + row
    return jnp.where((source == column) & (row < units * span), 1.0, 0.0)


def saved_shapes(layers, tokens, width, narrow_hidden):
    low, full = jnp.bfloat16, jnp.float32
    hidden = 4 * width
    return dict(
        low=((layers, 3, tokens, width), low),
        low_small=((layers, 3, tokens, PAD), low),
        heads=((layers, 3, tokens, width), low),
        heads_small=((layers, 3, tokens, PAD), low),
        probs=((layers, H, tokens, tokens), full),
        norm=((layers, 2, tokens, width), full),
        norm_small=((layers, 2, tokens, PAD), full),
        scales=((layers, 4, tokens, LANE), full),
        slope=((layers, tokens, hidden), full),
        slope_small=((layers, tokens, narrow_hidden), full),
        turned=((layers, hidden, tokens), low),
        turned_small=((layers, narrow_hidden, tokens), low),
        small_attn=((layers, 4, PAD, PAD), low),
        small_ff=((layers, 2, narrow_hidden, PAD), low),
    )


SAVED = tuple(saved_shapes(1, 1, 1, 1))


def forward_steps(layer, m, narrow, span):
    tokens, width = m.x.shape
    low = jnp.bfloat16
    vec = lambda row, count=1: m.vectors[pl.ds(layer * VECTOR_ROWS + row, count), :]
    small_vec = lambda row: vec(SMALL_ROW + row)[:, :PAD]

    def embed():
        rows = m.x[...]
        for group in range(LANGS):
            rows = rows + m.onehot[:, group : group + 1] * vec(TABLE_ROW + group)
        m.x[...] = rows
        m.low[layer, 0] = rows.astype(low)
        m.low_small[layer, 0] = m.y[...].astype(low)

    def project_text():
        def body(part, carry):
            joined = dot_nt(m.low[layer, 0], unit_rows(m.attn_w, part))
            bias = jnp.where(part == 0, vec(0), jnp.where(part == 2, vec(1), 0.0))
            m.heads[layer, part] = (joined + bias).astype(low)
            return carry

        lax.fori_loop(0, 3, body, 0)

    def prepare_small():
        permute = natural_rows(span, m.small_raw_layers, layer).astype(low)

        def body(block, carry):
            for member in range(3):
                raw = m.small_raw[block, :, :, :, pl.ds(member * PAD, PAD)].reshape(-1, PAD)
                rows = dot_nn(permute, raw).astype(low)
                if member == 0:
                    m.small_attn[layer, block] = rows
                else:
                    start = pl.multiple_of(block * narrow, 64)
                    m.small_ff[layer, member - 1, pl.ds(start, narrow), :] = rows[:narrow]
            return carry

        lax.fori_loop(0, PLANE, body, 0)

    def project_small():
        for part in range(3):
            joined = dot_nt(m.low_small[layer, 0], m.small_attn[layer, part])
            if part == 0:
                joined = joined + small_vec(0)
            if part == 2:
                joined = joined + small_vec(1)
            m.heads_small[layer, part] = joined.astype(low)
        m.mixed[...] = jnp.zeros_like(m.mixed)

    def attend_pairs(first, count):
        def body(pair, carry):
            lanes = pl.ds(pl.multiple_of(pair * LANE, LANE), LANE)
            query, keyed, valued = (m.heads[layer, n, :, lanes] for n in range(3))
            small_query, small_keyed, small_valued = (m.heads_small[layer, n] for n in range(3))
            lane, small_lane = lane_of((1, LANE)), lane_of((1, PAD))
            same = m.same[...] > 0.0
            contexts = []
            for side in range(2):
                head = 2 * pair + side
                chosen = (lane >= 64 * side) & (lane < 64 * side + 64)
                small_chosen = (small_lane >= 16 * head) & (small_lane < 16 * head + 16)
                mask = jnp.where(chosen, 0.125, 0.0).astype(low)
                small_mask = jnp.where(small_chosen, 0.25, 0.0).astype(low)
                scores = dot_nt(query * mask, keyed) + dot_nt(small_query * small_mask, small_keyed)
                scores = jnp.where(same, scores, MASKED)
                peak = jnp.max(scores, axis=1, keepdims=True)
                powers = jnp.exp(scores - peak)
                probs = powers * (1.0 / jnp.sum(powers, axis=1, keepdims=True))
                m.probs[layer, head] = probs
                probs_low = probs.astype(low)
                contexts.append(dot_nn(probs_low, valued))
                m.mixed[...] += jnp.where(small_chosen, dot_nn(probs_low, small_valued), 0.0)
            m.low[layer, 1, :, lanes] = jnp.where(lane < 64, contexts[0], contexts[1]).astype(low)
            return carry

        lax.fori_loop(first, first + count, body, 0)

    def first_norm():
        m.low_small[layer, 1] = m.mixed[...].astype(low)
        residual = m.x[...] + dot_nt(m.low[layer, 1], unit_rows(m.attn_w, 3)) + vec(2)
        normed, scale = standard(residual, width)
        m.norm[layer, 0] = normed
        m.scales[layer, 0] = jnp.broadcast_to(scale, (tokens, LANE))
        result = normed * vec(4) + vec(5)
        m.normed[...] = result
        m.low[layer, 2] = result.astype(low)

    def first_norm_small():
        branch = dot_nt(m.low_small[layer, 1], m.small_attn[layer, 3]) + small_vec(2)
        normed, scale = standard(m.y[...] + branch, narrow)
        m.norm_small[layer, 0] = normed
        m.scales[layer, 1] = jnp.broadcast_to(scale, (tokens, LANE))
        result = normed * small_vec(4) + small_vec(5)
        m.normed_small[...] = result
        m.low_small[layer, 2] = result.astype(low)

    def activate(column, upper_ref, source, active, slope, turned):
        here = pl.ds(column, LANE)
        value, rate = gelu_parts(upper_ref[:, source])
        slope[layer, :, here] = rate
        value_low = value.astype(low)
        active[:, here] = value_low
        turned[layer, here, :] = value.T.astype(low)

    def up_small():
        m.upper[...] = dot_nt(m.low_small[layer, 2], m.small_ff[layer, 0]) + vec(SMALL_HIDDEN_ROW)

        def body(tile, carry):
            column = pl.multiple_of(tile * LANE, LANE)
            activate(
                column, m.upper, pl.ds(column, LANE), m.active_small, m.slope_small, m.turned_small
            )
            return carry

        lax.fori_loop(0, m.active_small.shape[1] // LANE, body, 0)

    def down_small():
        second = dot_nn(m.active_small[...], m.small_ff[layer, 1]) + small_vec(3)
        normed, scale = standard(m.normed_small[...] + second, narrow)
        m.norm_small[layer, 1] = normed
        m.scales[layer, 3] = jnp.broadcast_to(scale, (tokens, LANE))
        m.y[...] = normed * small_vec(6) + small_vec(7)

    def up_text(first, count):
        def body(block, carry):
            m.upper[...] = dot_nt(m.low[layer, 2], unit_rows(m.up_w, block)) + vec(8 + block)

            def tile_body(tile, inner):
                column = pl.multiple_of(tile * LANE, LANE)
                activate(
                    pl.multiple_of(block * width + column, LANE),
                    m.upper,
                    pl.ds(column, LANE),
                    m.active,
                    m.slope,
                    m.turned,
                )
                return inner

            return lax.fori_loop(0, width // LANE, tile_body, carry)

        lax.fori_loop(first, first + count, body, 0)

    def down_text(first, count):
        def body(block, carry):
            columns = pl.ds(pl.multiple_of(block * width, LANE), width)
            m.second[...] += dot_nn(m.active[:, columns], unit_rows(m.down_w, block))
            return carry

        if first == 0:
            m.second[...] = m.normed[...] + vec(3)
        lax.fori_loop(first, first + count, body, 0)

    def second_norm():
        normed, scale = standard(m.second[...], width)
        m.norm[layer, 1] = normed
        m.scales[layer, 2] = jnp.broadcast_to(scale, (tokens, LANE))
        m.x[...] = normed * vec(6) + vec(7)

    part = H // 4
    after_attn = [(embed, 0.4), (project_text, 1.6)]
    after_small = [(prepare_small, 0.8), (project_small, 0.3)]
    for first in range(0, H // 2, part):
        after_small.append((functools.partial(attend_pairs, first, part), 2.5))
    after_small += [(first_norm, 0.8), (first_norm_small, 0.4), (up_small, 1.0), (down_small, 0.4)]
    after_up = [(functools.partial(up_text, first, 2), 2.4) for first in (0, 2)]
    after_down = [(functools.partial(down_text, first, 2), 0.7) for first in (0, 2)]
    after_down.append((second_norm, 0.3))
    return after_attn, after_small, after_up, after_down


def forward_shapes(layers, depth, tokens, width, narrow, small_span):
    low, full = jnp.bfloat16, jnp.float32
    span = 4 * width // (PLANE * depth * 2)
    whole = (PLANE, depth, 2, span, width)
    return dict(
        attn_w=(whole, low),
        up_w=(whole, low),
        down_w=(whole, low),
        small_raw=((PLANE, depth, 2, layers * small_span, width), low),
        own_small=((layers * small_span, width), low),
        own_small_full=((layers * small_span, width), full),
        same=((tokens, tokens), full),
        x=((tokens, width), full),
        y=((tokens, PAD), full),
        mixed=((tokens, PAD), full),
        normed=((tokens, width), full),
        normed_small=((tokens, PAD), full),
        upper=((tokens, width), full),
        active=((tokens, 4 * width), low),
        active_small=((tokens, 4 * narrow), low),
        second=((tokens, width), full),
        spread=((3 * SUBLANES, width), full),
    )


FORWARD_SCRATCH = tuple(forward_shapes(1, 1, 1, 1, 1, 1))


def flat_rows(width, narrow):
    rows = [(n, 0, n * width, width) for n in range(PIECE_ROWS)]
    rows += [(TABLE_ROW + n, 1, n * width, width) for n in range(LANGS)]
    rows += [(SMALL_ROW + n, 2, n * narrow, narrow) for n in range(8)]
    return rows + [(SMALL_HIDDEN_ROW, 2, 8 * narrow, 4 * narrow)]


def forward_kernel(depth, layers, narrow, span, *refs):
    refs = list(refs)

    def take(number):
        taken = refs[:number]
        del refs[:number]
        return taken

    count = 3 * layers + 1
    fill = count - 2
    text_attn, text_up, text_down, layout_attn, layout_up, layout_down = take(6)
    pieces = take(3)
    text_in, layout_in, page_row, groups = take(4)
    outs = take(count)
    vector_out, onehot_out, text_out, layout_out = take(4)
    kept = take(len(SAVED))
    own_sem, zs, zr, ps, pr, us, ur, cs, cr, load_sem, keep_sem = take(11)
    all_sum = take(4)
    m = SimpleNamespace()
    for name in SAVED + FORWARD_SCRATCH:
        setattr(m, name, refs.pop(0))
    m.vectors, m.onehot, m.small_raw_layers = vector_out, onehot_out, layers
    at, devices = place(depth)
    dp, z, core, dx, dy, dd = at.dp, at.z, at.core, at.dx, at.dy, at.dd
    half = depth // 2
    low, full = jnp.bfloat16, jnp.float32
    tokens, width = m.x.shape
    vectors = AllSum(devices, vector_out, *all_sum)

    sources = [text_attn.at[0], m.own_small]
    for layer in range(layers):
        if layer > 0:
            sources.append(text_attn.at[layer])
        sources += [text_up.at[layer], text_down.at[layer]]

    def own(k):
        return pltpu.make_async_copy(sources[k], outs[k].at[dp, z, core], own_sem.at[k])

    def line(k, rising, hop, side=0):
        level = z - hop if rising else z + hop
        owner = (dp, dx, dy, dd)[side]
        target = outs[k].at[owner, level, core]
        row = k if side == 0 else count - 1 + side
        return remote(
            sources[k] if hop == 0 and side == 0 else target,
            target,
            zs.at[row, int(rising), hop],
            zr.at[row, level],
            devices.up if rising else devices.down,
        )

    def exists(rising, hop):
        return (z - hop >= 0) if rising else (z + hop < depth)

    def goes_on(rising, hop):
        return exists(rising, hop) & ((z < depth - 1) if rising else (z > 0))

    def unit(rising, hop, to_x):
        level = z - hop if rising else z + hop
        target = outs[0].at[dp, level, core]
        return remote(
            sources[0] if hop == 0 else target,
            target,
            us.at[int(to_x), level],
            ur.at[int(to_x), level],
            devices.x if to_x else devices.y,
        )

    def unit_landed(to_x, level):
        target = outs[0].at[dx if to_x else dy, level, core]
        return remote(
            target, target, us.at[int(to_x), level], ur.at[int(to_x), level], devices.x
        )

    def line_start(k, hop, side=0):
        for rising in (True, False):

            @pl.when(goes_on(rising, hop))
            def start():
                line(k, rising, hop, side).start()

    def line_wait(k, hop, side=0, then=None):
        for rising in (True, False):

            @pl.when(exists(rising, hop))
            def wait():
                line(k, rising, hop, side).wait_recv()
                if then is not None:
                    then(rising, hop)

    def unit_start(rising, hop):
        unit(rising, hop, True).start()
        unit(rising, hop, False).start()

    def plane(k, index, sending=True):
        if k == fill:
            rows = span // 2
            lower, upper = pl.ds(0, rows), pl.ds(rows, rows)
            if sending:
                blocks = ((dp, None), (dp, None), (dx, lower), (dy, upper))
            else:
                blocks = ((dx, None), (dy, None), (dd, lower), (dd, upper))
            owner, rows = blocks[index]
            block = outs[k].at[owner, z, core]
            block = block if rows is None else block.at[rows]
            source = sources[k] if sending and index < 2 else block
        else:
            lower, upper, every = pl.ds(0, half), pl.ds(half, half), pl.ds(0, depth)
            if sending:
                blocks = ((dp, every), (dp, every), (dx, lower), (dy, upper))
            else:
                blocks = ((dx, every), (dy, every), (dd, lower), (dd, upper))
            owner, levels = blocks[index]
            block = outs[k].at[owner, levels, core]
            source = block
        device = (devices.x, devices.y, devices.y, devices.x)[index]
        return remote(source, block, ps.at[k, index], pr.at[k, index], device)

    def across(k, index, side):
        lower, upper, every = pl.ds(0, half), pl.ds(half, half), pl.ds(0, depth)
        if k == fill:
            blocks = ((dp, every), (dx, every), (dy, every), (dd, every))
        else:
            blocks = ((dp, every), (dx, every), (dy, every), (dd, lower), (dd, upper))
        owner, levels = blocks[index]
        block = outs[k].at[owner, levels, side]
        return remote(block, block, cs.at[k, index], cr.at[k, index], devices.core)

    def landed_across(k):
        return range(4 if k == fill else 5)

    held = [m.attn_w, m.small_raw, m.up_w, m.down_w] + [m.attn_w, m.up_w, m.down_w] * (layers - 1)

    def load(k, side):
        owner = (dp, dx, dy, dd)[side]
        return pltpu.make_async_copy(
            outs[k].at[owner], held[k].at[owner], load_sem.at[k, side]
        )

    def loaded(k):
        for side in range(PLANE):
            load(k, side).wait()

    def keep(index, layer):
        source = getattr(m, SAVED[index])
        return pltpu.make_async_copy(
            source.at[layer], kept[index].at[layer], keep_sem.at[index, layer]
        )

    def keep_some(layer, names):
        for name in names:
            keep(SAVED.index(name), layer).start()

    def then_keep(step, layer, names):
        def run():
            step[0]()
            keep_some(layer, names)

        return (run, step[1])

    stages = []
    for layer in range(layers):
        steps = forward_steps(layer, m, narrow, layout_down.shape[1])
        if layer == 0:
            stages += [steps[0], steps[1], steps[2], steps[3]]
        else:
            stages += [steps[0] + steps[1], steps[2], steps[3]]
        stages[-2][-1] = then_keep(stages[-2][-1], layer, SAVED[:5] + SAVED[8:])
        stages[-1][-1] = then_keep(stages[-1][-1], layer, SAVED[5:8])

    def make_small():
        m.own_small_full[...] = jnp.zeros_like(m.own_small_full)
        units = layout_down.shape[1]
        for layer in range(layers):
            rows = pl.ds(layer * units, units)
            m.own_small_full[rows, 0:narrow] = layout_attn[layer].astype(full)
            m.own_small_full[rows, PAD : PAD + narrow] = layout_up[layer].astype(full)
            m.own_small_full[rows, 2 * PAD : 2 * PAD + narrow] = layout_down[layer].astype(full)
        m.own_small[...] = m.own_small_full[...].astype(low)

    def spread_vectors():
        m.spread[...] = jnp.zeros_like(m.spread)
        for n, piece in enumerate(pieces):
            m.spread[pl.ds(SUBLANES * n, layers), 0 : piece.shape[1]] = piece[...].astype(full)
        start = vector_out
        start[...] = jnp.zeros_like(start)
        lane = lane_of((SUBLANES, width))
        for row, n, base, lanes in flat_rows(width, narrow):
            length = pieces[n].shape[1]
            shift = lax.rem(at.me * length - base + 16 * width, width)
            rolled = pltpu.roll(m.spread[pl.ds(SUBLANES * n, SUBLANES), :], shift, 1)
            index = lane + (base - at.me * length)
            inside = (index >= 0) & (index < length) & (lane < lanes)
            rolled = jnp.where(inside, rolled, 0.0)
            for layer in range(layers):
                start[pl.ds(layer * VECTOR_ROWS + row, 1), :] = rolled[layer : layer + 1]
        vectors.send(0)

    def make_masks():
        pages = jnp.broadcast_to(page_row[...].astype(full), (tokens, tokens))
        turned = pages.T
        m.same[...] = jnp.where(pages == turned, 1.0, 0.0)
        group = jnp.where(
            turned == (2 * at.me).astype(full),
            jnp.broadcast_to(groups[:, 0:1], (tokens, tokens)),
            jnp.broadcast_to(groups[:, 1:2], (tokens, tokens)),
        )
        m.onehot[...] = jnp.where(group == lane_of((tokens, tokens)), 1.0, 0.0)

    def take_in():
        m.x[...] = text_in[...].astype(full)
        m.y[...] = jnp.zeros_like(m.y)
        m.y[:, 0:narrow] = layout_in[...].astype(full).T

    def land(k, sides):
        for side in sides:
            across(k, side, 1 - core).wait_recv()
            if side == 3 and k != fill:
                across(k, 4, 1 - core).wait_recv()
            load(k, side).start()

    signal(devices)
    make_small()
    greeted()
    for k in (0, fill, 1):
        own(k).start()
    line_start(0, 0)
    unit_start(True, 0)
    plane(fill, 0).start()
    plane(fill, 1).start()
    for k in range(2, count):
        if k != fill:
            own(k).start()

    plan = Plan()
    chain = [k for k in range(count) if k != fill]
    size = [sources[k].shape[0] / UNIT_ROWS_PER_US for k in range(count)]

    def begin_line(k, side):
        if side == 0:
            own(k).wait()
        if k > 0:
            line_start(k, 0, side)

    def next_line(k, hop, side):
        line_wait(k, hop, side, unit_start if k == 0 else None)
        if hop < depth - 1:
            line_start(k, hop, side)

    def add_line(k, side, after, needs, rank):
        sends = [("z", size[k], ("z", 1, k, side))]
        if k == 0:
            sends += [("x", size[k], ("u", 0)), ("x", size[fill], ("f", 1))]
        plan.add(("z", 0, k, side), functools.partial(begin_line, k, side), after, needs, sends, 0.3, rank)
        for hop in range(1, depth):
            sends = []
            if hop < depth - 1:
                sends.append(("z", size[k], ("z", hop + 1, k, side)))
            if k == 0:
                sends.append(("x", size[k], ("u", hop)))
            plan.add(
                ("z", hop, k, side),
                functools.partial(next_line, k, hop, side),
                [("z", hop - 1, k, side)],
                [("z", hop, k, side)],
                sends,
                0.3,
                rank,
            )

    def plane_first(k):
        if k > 0:
            plane(k, 0).start()
            plane(k, 1).start()
        across(k, 0, core).start()

    def plane_second(k):
        for index in (0, 1):
            if k == 0:
                for level in range(depth):
                    unit_landed(index == 0, level).wait_recv()
            else:
                plane(k, index, False).wait_recv()
            plane(k, index + 2).start()
            if k != fill:
                across(k, index + 1, core).start()

    def plane_third(k):
        for index in (2, 3):
            plane(k, index, False).wait_recv()
            if k != fill:
                across(k, index + 1, core).start()

    def cross_fill(side):
        across(fill, side, core).start()

    last = {}
    lines = [(k, 0) for k in chain]
    for side in range(4):
        lines.insert((4, 6, 7, 9)[side], (fill, side))
    for n, (k, side) in enumerate(lines):
        after = [("z", 1 if n > 1 else 2) + lines[n - 1]] if n else []
        if k == fill:
            after.append(("p", 2 if side < 3 else 3, fill))
        add_line(k, side, after, [], 10 * n)
    for n, k in enumerate(chain):
        arrive = ("x", k) if k else ("u", depth - 1)
        sends = [("c", 0.4 * size[k], ("c", 0, k))]
        if k:
            sends.append(("x", 4 * size[k], arrive))
        plan.add(("p", 1, k), functools.partial(plane_first, k), [("z", depth - 1, k, 0)], [], sends, 0.2, 10 * n + 1)
        sends = [("x", 2 * size[k], ("d", k)), ("c", 0.8 * size[k], ("c", 1, k))]
        plan.add(("p", 2, k), functools.partial(plane_second, k), [("p", 1, k)], [arrive], sends, 0.2, 10 * n + 2)
        sends = [("c", 0.4 * size[k], ("c", 2, k))]
        plan.add(("p", 3, k), functools.partial(plane_third, k), [("p", 2, k)], [("d", k)], sends, 0.2, 10 * n + 3)
    plan.add(
        ("p", 2, fill),
        functools.partial(plane_second, fill),
        [("z", 1, 0, 0)],
        [("f", 1)],
        [("x", size[fill] / 2, ("f", 2))],
        0.2,
        5,
    )
    plan.add(("p", 3, fill), functools.partial(plane_third, fill), [("p", 2, fill)], [("f", 2)], rank=6)
    for side in range(4):
        plan.add(
            ("a", side),
            functools.partial(cross_fill, side),
            [("z", depth - 1, fill, side)],
            [],
            [("c", 0.4 * size[fill], ("a", side))],
            0.1,
            25 + 10 * side,
        )
    previous = None
    vector_steps = [spread_vectors]
    vector_steps += [functools.partial(vectors.advance, n) for n in range(AllSum.STEPS)]
    for n, step_of in enumerate(vector_steps):
        link, amount = (("c", 0.3), ("z", 2.2), ("z", 6.0), ("x", 2.2), ("x", 2.2), ("h", 0.0))[n]
        sends = [(link, amount, ("v", n))]
        needs = [("v", n - 1)] if n else []
        after = [("v", n - 1)] if n else []
        if n == 1:
            after.append(("z", 2, 0, 0))
        plan.add(("v", n), step_of, after, needs, sends, 0.1 if n else 0.5, 2)
    plan.add("i", take_in, [("v", 0)], time=0.1, rank=3)
    plan.add("m", make_masks, ["i"], time=0.1, rank=3)
    previous = [("v", AllSum.STEPS), "m"]
    for k in range(count):
        vacant = [last[k - 3]] if k > 3 else []
        if k == fill:
            landed = [("a", side) for side in range(4)]
            plan.add(("l", k), functools.partial(land, k, range(4)), landed + vacant, landed, [("h", 2.4, ("h", k))], 0.2, 10 * k)
        else:
            landed = [("c", 0, k), ("c", 1, k)]
            plan.add(("k", k), functools.partial(land, k, range(3)), [("p", 2, k)] + vacant, landed, [("h", 2.0, ("k", k))], 0.2, 10 * k)
            plan.add(("l", k), functools.partial(land, k, (3,)), [("p", 3, k), ("k", k)], [("c", 2, k)], [("h", 0.7, ("h", k))], 0.2, 10 * k)
        for n, (closure, time) in enumerate(stages[k]):
            run = closure
            if n == 0:
                run = functools.partial(lambda k, closure: (loaded(k), closure()), k, closure)
            plan.add(("s", k, n), run, previous + [("l", k)], [("h", k)], (), time, 1000 + k, True)
            previous = [("s", k, n)]
        last[k] = previous[0]
    plan.run()
    text_out[...] = m.x[...]
    layout_out[...] = m.y[:, 0:narrow].T
    vectors.close()
    for index in range(len(SAVED)):
        for layer in range(layers):
            keep(index, layer).wait()
    for level in range(depth):
        for to_x in (True, False):
            unit_landed(to_x, level).wait_send()
    for k in range(count):
        for index in landed_across(k):
            across(k, index, core).wait_send()
        for index in range(4):
            if k > 0 or index > 1:
                plane(k, index).wait_send()
        for rising in (True, False):
            for hop in range(depth):

                @pl.when(goes_on(rising, hop))
                def drain():
                    for side in range(4 if k == fill else 1):
                        line(k, rising, hop, side).wait_send()


def run_forward(depth, narrow, weights, pieces, text_in, layout_in, page_row, groups):
    dma = pltpu.SemaphoreType.DMA
    tokens, width = text_in.shape
    layers, span, unused = weights[0].shape
    count = 3 * layers + 1
    full = jnp.float32
    saved = saved_shapes(layers, tokens, width, 4 * narrow)
    small_span = weights[5].shape[1]
    scratch = forward_shapes(layers, depth, tokens, width, narrow, small_span)
    rows = [span, layers * small_span] + [span] * (count - 2)
    vector_shape = (layers * VECTOR_ROWS, width)
    results = pl.pallas_call(
        functools.partial(forward_kernel, depth, layers, narrow, span),
        out_shape=[
            jax.ShapeDtypeStruct((PLANE, depth, 2, row, width), weights[0].dtype) for row in rows
        ]
        + [
            jax.ShapeDtypeStruct(vector_shape, full),
            jax.ShapeDtypeStruct((tokens, LANE), full),
            jax.ShapeDtypeStruct((tokens, width), full),
            jax.ShapeDtypeStruct((narrow, tokens), full),
        ]
        + [jax.ShapeDtypeStruct(*saved[name]) for name in SAVED],
        in_specs=[IN_VMEM] * 13,
        out_specs=[ANY] * count + [IN_VMEM] * 4 + [ANY] * len(SAVED),
        scratch_shapes=[
            dma((count,)),
            dma((count + 3, 2, depth)),
            dma((count + 3, depth)),
            dma((count, 4)),
            dma((count, 4)),
            dma((2, depth)),
            dma((2, depth)),
            dma((count, 5)),
            dma((count, 5)),
            dma((count, PLANE)),
            dma((len(SAVED), layers)),
        ]
        + AllSum.scratch(vector_shape)
        + [pltpu.VMEM(*saved[name]) for name in SAVED]
        + [pltpu.VMEM(*scratch[name]) for name in FORWARD_SCRATCH],
        compiler_params=pltpu.CompilerParams(
            collective_id=0, has_side_effects=True, vmem_limit_bytes=66000000
        ),
        name="forward_blocks",
    )(*weights, *pieces, text_in, layout_in, page_row, groups)
    return results[:count], results[count : count + 4], results[count + 4 :]


TEXT_MEMBERS = 3
LINKS = 10


def back_shapes(layers, depth, tokens, width, narrow_hidden):
    low, full = jnp.bfloat16, jnp.float32
    span = 4 * width // (PLANE * depth * 2)
    unit = (PLANE, depth, span, LANE)
    whole = (PLANE, depth, 2, span, LANE)
    return dict(
        weights=((2, PLANE, depth, 2, span, width), low),
        gx=((tokens, width), full),
        gy=((tokens, PAD), full),
        down_low=((tokens, width), low),
        down_low_small=((tokens, PAD), low),
        branch_low=((tokens, width), low),
        branch_low_small=((tokens, PAD), low),
        wide=((tokens, width), full),
        upper_low=((tokens, 4 * width), low),
        upper_low_small=((tokens, narrow_hidden), low),
        context=((tokens, width), low),
        context_small=((tokens, PAD), low),
        joined=((3, tokens, width), low),
        mixed=((3, tokens, PAD), full),
        rows_up=(whole, low),
        rows_attn=(whole, low),
        rows_small=((2, narrow_hidden, tokens), low),
        in_land=((layers, 4, tokens, width), low),
        in_land_small=((layers, 4, tokens, PAD), low),
        rows_land=((layers, 3) + unit, low),
        rows_land_small=((layers, 3, narrow_hidden, tokens), low),
        sums=((layers * VECTOR_ROWS, width), full),
    )


BACK_SCRATCH = tuple(back_shapes(1, 1, 1, 1, 1))


def standard_back(grad, normed, scale, gain, width):
    pushed = grad * gain
    average = jnp.sum(pushed, axis=1, keepdims=True) * (1.0 / width)
    along = jnp.sum(pushed * normed, axis=1, keepdims=True) * (1.0 / width)
    result = scale * (pushed - average - normed * along)
    if grad.shape[1] != width:
        result = jnp.where(lane_of(grad.shape) < width, result, 0.0)
    return result, total(grad * normed), total(grad)


def total(rows):
    return jnp.sum(rows.astype(jnp.float32), axis=0, keepdims=True)


def rows_of_core(span, layers, layer, depth, core):
    shape = (depth * layers * span, 2 * depth * span)
    row = lax.broadcasted_iota(jnp.int32, shape, 0)
    column = lax.broadcasted_iota(jnp.int32, shape, 1)
    unit = unit_of(row, layers * span, depth)
    inside = row - unit * layers * span - layer * span
    source = (2 * unit + core) * span + inside
    return jnp.where((source == column) & (inside >= 0) & (inside < span), 1.0, 0.0)


def backward_kernel(depth, layers, narrow, span, *refs):
    refs = list(refs)

    def take(number):
        taken = refs[:number]
        del refs[:number]
        return taken

    text_count = TEXT_MEMBERS * layers
    count = text_count + 1
    gathered = take(text_count)
    kept = take(len(SAVED))
    vec_ref, text_cot, layout_cot, onehot = take(4)
    finals = take(count)
    vector_out, text_out, layout_out = take(3)
    layout_turned, early_sem = refs[-2:]
    del refs[-2:]
    m = SimpleNamespace()
    for name in SAVED + BACK_SCRATCH:
        setattr(m, name, refs.pop(0))
    mine_text, mine_small = take(2)
    landed_diag, landed_plane, landed_line = take(count), take(count), take(count)
    outs = take(count)
    weight_sem, keep_sem, out_sem, xs, xr, ps, pr, zs, zr = take(9)
    all_sum = take(4)
    at, devices = place(depth)
    dp, z, core, dx, dy, dd = at.dp, at.z, at.core, at.dx, at.dy, at.dd
    fill = 1
    owners = (dp, dx, dy, dd)
    half = depth // 2
    low = jnp.bfloat16
    tokens, width = m.gx.shape
    hidden_small = m.upper_low_small.shape[1]
    signal(devices)
    vectors = AllSum(devices, vector_out, *all_sum)

    slots, reuse = {}, {}
    for k in range(count):
        if k < text_count:
            spare = [n for n in range(mine_text.shape[0]) if n not in slots.values()]
            if spare:
                slots[k] = spare[0]
            else:
                reuse[k] = min(n for n in slots if n != fill and n not in reuse.values())
                slots[k] = slots[reuse[k]]

    def mine(k):
        if k == text_count:
            return mine_small
        return mine_text.at[slots[k]]

    order = []
    for layer in reversed(range(layers)):
        order += [3 * layer + 2, 3 * layer + 1, 3 * layer]

    def weight_load(index):
        return pltpu.make_async_copy(
            gathered[order[index]], m.weights.at[index % 2], weight_sem.at[index]
        )

    def saved_load(name, layer):
        index = SAVED.index(name)
        return pltpu.make_async_copy(
            kept[index].at[layer], getattr(m, name), keep_sem.at[index, layer]
        )

    def cross(layer, link):
        moves = (
            (m.low, m.in_land.at[layer, pl.ds(0, 3)]),
            (m.turned.at[:, :, 1 - core], m.rows_land.at[layer, 0]),
            (m.down_low, m.in_land.at[layer, 3]),
            (m.rows_up.at[:, :, 1 - core], m.rows_land.at[layer, 1]),
            (m.rows_attn.at[:, :, 1 - core], m.rows_land.at[layer, 2]),
            (m.low_small, m.in_land_small.at[layer, pl.ds(0, 3)]),
            (m.turned_small, m.rows_land_small.at[layer, 0]),
            (m.down_low_small, m.in_land_small.at[layer, 3]),
            (m.rows_small.at[0], m.rows_land_small.at[layer, 1]),
            (m.rows_small.at[1], m.rows_land_small.at[layer, 2]),
        )
        source, target = moves[link]
        return remote(
            source, target, xs.at[layer, link], xr.at[layer, link], devices.core
        )

    def plane(k, index):
        if k == fill:
            size = landed_diag[k].shape[1]
            lower, upper = pl.ds(0, size), pl.ds(size, size)
            own = lambda owner, rows: mine(k).at[owner, z, rows]
        else:
            lower, upper = pl.ds(0, half), pl.ds(half, half)
            own = lambda owner, levels: mine(k).at[owner, levels]
        diag, direct = landed_diag[k], landed_plane[k]
        moves = (
            (dd, lower, diag.at[0], devices.y),
            (dd, upper, diag.at[1], devices.x),
            (dx, upper, direct.at[0, upper], devices.x),
            (dy, lower, direct.at[1, lower], devices.y),
            (dx, lower, direct.at[0, lower], devices.x),
            (dy, upper, direct.at[1, upper], devices.y),
        )
        owner, part, target, device = moves[index]
        return remote(own(owner, part), target, ps.at[k, index], pr.at[k, index], device)

    def line(k, rising, level, slot, side=0):
        row = k if side == 0 else count - 1 + side
        return remote(
            mine(k).at[owners[side], level],
            landed_line[k].at[slot, side],
            zs.at[row, int(rising), level],
            zr.at[row, int(rising), level],
            devices.up if rising else devices.down,
        )

    def second_sums(k):
        if k == fill:
            size = landed_diag[k].shape[1]
            lower, upper = pl.ds(0, size), pl.ds(size, size)
            one, other = mine(k).at[dx, z, lower], mine(k).at[dy, z, upper]
            add = add_rows
        else:
            one = mine(k).at[dx, pl.ds(0, half)]
            other = mine(k).at[dy, pl.ds(half, half)]
            add = add_units
        plane(k, 0).wait_recv()
        add(one, landed_diag[k].at[0])
        plane(k, 4).start()
        plane(k, 1).wait_recv()
        add(other, landed_diag[k].at[1])
        plane(k, 5).start()

    def third_sums(k):
        for index in (2, 3, 4, 5):
            plane(k, index).wait_recv()
        if k == fill:
            result = mine(k)[dp, z].astype(jnp.float32)
            for side in range(2):
                result = result + landed_plane[k][side].astype(jnp.float32)
            outs[k][...] = result
            put_out(k).start()
        else:
            add_units(mine(k).at[dp], landed_plane[k].at[0], landed_plane[k].at[1])
            line_step(k, 0)

    def passed(rising, hop):
        return range(hop + 1, depth) if rising else range(depth - 1 - hop)

    def line_step(k, hop, side=0):
        for rising in (True, False):

            @pl.when(z == (hop if rising else depth - 1 - hop))
            def move():
                for level in passed(rising, hop):
                    if hop > 0:
                        line(k, rising, level, level, side).wait_recv()
                        add_rows(mine(k).at[owners[side], level], landed_line[k].at[level, side])
                    last = rising and level == hop + 1
                    line(k, rising, level, depth if last else level, side).start()

    def last_sums(k, side=0):
        if k != fill:
            outs[k][...] = mine(k)[dp, z].astype(jnp.float32)
        for rising in (True, False):

            @pl.when((z > 0) if rising else (z < depth - 1))
            def add():
                slot = depth if rising else z
                line(k, rising, z, slot, side).wait_recv()
                if k == fill:
                    add_rows(mine(k).at[owners[side], z], landed_line[k].at[slot, side])
                else:
                    outs[k][...] += landed_line[k][slot, side].astype(jnp.float32)

        if k != fill:
            put_out(k).start()

    def early():
        return (
            pltpu.make_async_copy(m.gx, text_out, early_sem.at[0]),
            pltpu.make_async_copy(layout_turned, layout_out, early_sem.at[1]),
        )

    def put_out(k):
        return pltpu.make_async_copy(outs[k], finals[k], out_sem.at[k])

    def fill_plane():
        for index in range(4):
            plane(fill, index).start()

    def drain(k):
        for index in range(6):
            plane(k, index).wait_send()
        for hop in range(depth - 1):
            for rising in (True, False):

                @pl.when(z == (hop if rising else depth - 1 - hop))
                def wait():
                    for level in passed(rising, hop):
                        for side in range(PLANE if k == fill else 1):
                            line(k, rising, level, level, side).wait_send()

    plan = Plan()
    size = [outs[k].shape[0] / UNIT_ROWS_PER_US for k in range(count)]

    def add_scatter(k, rank):
        one = size[k]

        def step(hop, side):
            if hop < depth - 1:
                line_step(k, hop, side)
            else:
                last_sums(k, side)

        for side in range(PLANE if k == fill else 1):
            for hop in range(0 if k == fill else 1, depth):
                sends = []
                if hop < depth - 1:
                    sends.append((("z", hop), (depth - 1 - hop) * one, ("z", hop + 1, k, side)))
                after = [("z", hop - 1, k, side)] if hop else [("o", k)]
                if k != fill and hop == 1:
                    after = [("s", 3, k)]
                if k == fill and hop == 0 and side:
                    after.append(("z", 1, k, side - 1))
                needs = [("z", hop, k, side)] if hop else []
                plan.add(
                    ("z", hop, k, side), functools.partial(step, hop, side), after, needs, sends, 0.3, rank
                )
        first = ("o", k)
        share = 2 * one
        if k == fill:
            first, share = ("f", 0), one / 2
            sends = [("x", share, ("d", k)), ("x", share, ("e", k))]
            ends = [("z", depth - 1, k, side) for side in range(PLANE)]
            plan.add(first, fill_plane, ends, [], sends, 0.2, rank)
        plan.add(
            ("s", 2, k), functools.partial(second_sums, k), [first], [("d", k)], [("x", share, ("g", k))], 0.5, rank
        )
        sends = [(("z", 0), (depth - 1) * one, ("z", 1, k, 0))] if k != fill else []
        plan.add(
            ("s", 3, k), functools.partial(third_sums, k), [("s", 2, k)], [("e", k), ("g", k)], sends, 1.0, rank
        )

    def own_sends(k):
        if k == fill:
            return []
        return [("x", 2 * size[k], ("d", k)), ("x", 2 * size[k], ("e", k))]

    previous = []

    def then(name, run, time, needs=(), sends=(), after=()):
        plan.add(name, run, previous + list(after), needs, sends, time, 1000, True)
        previous[:] = [name]

    def done(k):
        return [("s", 3, k), ("z", depth - 1, k, 0)]

    def own_sums(k, rows, rows_land, ins, ins_land):
        if k in reuse:
            drain(reuse[k])

        def block(turn, carry):
            owner = jnp.where(turn == 0, dd, jnp.where(turn == 1, dx, jnp.where(turn == 2, dy, dp)))
            left = jnp.concatenate(
                [
                    rows[owner, :, core].reshape(-1, tokens),
                    rows_land[owner].reshape(-1, tokens),
                ],
                axis=1,
            )
            right = jnp.concatenate([ins(owner), ins_land(owner)], axis=0)
            result = dot_nn(left, right)
            mine(k)[owner] = result.astype(low).reshape(depth, -1, width)
            if k != fill:
                for index, when in enumerate((0, 0, 1, 2)):

                    @pl.when(turn == when)
                    def send():
                        plane(k, index).start()

            return carry

        lax.fori_loop(0, PLANE, block, 0)

    m.gx[...] = text_cot[...].astype(jnp.float32)
    m.gy[...] = jnp.zeros_like(m.gy)
    m.gy[:, 0:narrow] = layout_cot[...].astype(jnp.float32).T
    first_names = ("norm", "scales", "turned", "norm_small", "turned_small", "slope", "low")
    names = first_names + tuple(name for name in SAVED if name not in first_names)
    weight_load(0).start()
    for name in names:
        saved_load(name, layers - 1).start()
    weight_load(1).start()
    greeted()

    def add_layer(turn, layer):
        k = TEXT_MEMBERS * turn
        vec = lambda row, n=1: vec_ref[pl.ds(layer * VECTOR_ROWS + row, n), :]
        small_vec = lambda row: vec(SMALL_ROW + row)[:, :PAD]
        slot = lambda member: m.weights.at[(3 * turn + member) % 2]

        def put(row, value):
            m.sums[pl.ds(layer * VECTOR_ROWS + row, 1), :] = value

        def put_small(row, value):
            m.sums[pl.ds(layer * VECTOR_ROWS + SMALL_ROW + row, 1), :PAD] = value


        def tail():
            m.sums[pl.ds(layer * VECTOR_ROWS + SMALL_ROW, VECTOR_ROWS - SMALL_ROW), :] = jnp.zeros(
                (VECTOR_ROWS - SMALL_ROW, width), jnp.float32
            )
            for name in ("norm", "scales", "turned"):
                saved_load(name, layer).wait()
            cross(layer, 1).start()
            grad, gain_sum, shift_sum = standard_back(
                m.gx[...], m.norm[1], m.scales[2][:, :1], vec(6), width
            )
            put(6, gain_sum)
            put(7, shift_sum)
            m.gx[...] = grad
            m.down_low[...] = grad.astype(low)
            cross(layer, 2).start()
            put(3, total(m.down_low[...]))

        def tail_small():
            for name in ("norm_small", "turned_small"):
                saved_load(name, layer).wait()
            cross(layer, 6).start()
            grad, gain_sum, shift_sum = standard_back(
                m.gy[...], m.norm_small[1], m.scales[3][:, :1], small_vec(6), narrow
            )
            put_small(6, gain_sum)
            put_small(7, shift_sum)
            m.gy[...] = grad
            m.down_low_small[...] = grad.astype(low)
            cross(layer, 7).start()
            put_small(3, total(m.down_low_small[...]))

        def own_down():
            cross(layer, 1).wait_recv()
            cross(layer, 2).wait_recv()
            own_sums(
                k,
                m.turned,
                m.rows_land.at[layer, 0],
                lambda owner: m.down_low[...],
                lambda owner: m.in_land[layer, 3],
            )

        cut = 3 * LANE

        def hidden(block, carry):
            m.wide[...] = dot_nt(m.down_low[...], unit_rows(slot(0), block))
            for side in range(width // cut):
                inside = pl.ds(side * cut, cut)
                columns = pl.ds(pl.multiple_of(block * width + side * cut, LANE), cut)
                rows = m.slope[:, columns] * m.wide[:, inside]
                rows_low = rows.astype(low)
                m.upper_low[:, columns] = rows_low
                m.sums[pl.ds(layer * VECTOR_ROWS + 8 + block, 1), inside] = total(rows_low)
                levels = depth * cut // width
                m.rows_up[block, pl.ds(side * levels, levels)] = (
                    rows.T.astype(low).reshape(levels, 2, -1, tokens)
                )
            return carry


        def hidden_blocks(first, number):
            if first == 0:
                for name in names[5:]:
                    saved_load(name, layer).wait()
                cross(layer, 0).start()
                cross(layer, 5).start()
                weight_load(3 * turn).wait()
            lax.fori_loop(first, first + number, hidden, 0)
            if first + number == PLANE:
                cross(layer, 3).start()
                if 3 * turn + 2 < 3 * layers:
                    weight_load(3 * turn + 2).start()

        def hide_small():
            m.wide[...] = dot_nt(m.down_low_small[...], m.small_ff[1])

            for side in range(hidden_small // cut):
                columns = pl.ds(side * cut, cut)
                rows = m.slope_small[:, columns] * m.wide[:, columns]
                rows_low = rows.astype(low)
                m.upper_low_small[:, columns] = rows_low
                m.rows_small[0, columns, :] = rows.T.astype(low)
                m.sums[
                    pl.ds(layer * VECTOR_ROWS + SMALL_HIDDEN_ROW, 1), columns
                ] = total(rows_low)
            cross(layer, 8).start()

        def own_up():
            cross(layer, 0).wait_recv()
            cross(layer, 3).wait_recv()
            own_sums(
                k + 1,
                m.rows_up,
                m.rows_land.at[layer, 1],
                lambda owner: m.low[2],
                lambda owner: m.in_land[layer, 2],
            )

        def lower_text():
            weight_load(3 * turn + 1).wait()

            def lower(block, carry):
                columns = pl.ds(pl.multiple_of(block * width, LANE), width)
                m.gx[...] += dot_nn(m.upper_low[:, columns], unit_rows(slot(1), block))
                return carry

            lax.fori_loop(0, PLANE, lower, 0)
            if 3 * turn + 3 < 3 * layers:
                weight_load(3 * turn + 3).start()
            grad, gain_sum, shift_sum = standard_back(
                m.gx[...], m.norm[0], m.scales[0][:, :1], vec(4), width
            )
            put(4, gain_sum)
            put(5, shift_sum)
            m.gx[...] = grad
            m.branch_low[...] = grad.astype(low)
            put(2, total(m.branch_low[...]))
            for side in range(width // cut):
                levels = depth * cut // width
                tile = m.gx[:, side * cut : (side + 1) * cut]
                m.rows_attn[3, pl.ds(side * levels, levels)] = (
                    tile.T.astype(low).reshape(levels, 2, -1, tokens)
                )

        def lower_small():
            grad = m.gy[...] + dot_nn(m.upper_low_small[...], m.small_ff[0])
            grad, gain_sum, shift_sum = standard_back(
                grad, m.norm_small[0], m.scales[1][:, :1], small_vec(4), narrow
            )
            put_small(4, gain_sum)
            put_small(5, shift_sum)
            m.gy[...] = grad
            m.branch_low_small[...] = grad.astype(low)
            put_small(2, total(m.branch_low_small[...]))
            m.rows_small[1, pl.ds(3 * narrow, narrow), :] = grad.T[:narrow].astype(low)

        def contexts():
            weight_load(3 * turn + 2).wait()
            m.context[...] = dot_nn(m.branch_low[...], unit_rows(slot(2), 3)).astype(low)
            m.context_small[...] = dot_nn(m.branch_low_small[...], m.small_attn[3]).astype(low)
            m.mixed[...] = jnp.zeros_like(m.mixed)

        def pair_back(pair, carry):
            lanes = pl.ds(pl.multiple_of(pair * LANE, LANE), LANE)
            query, keyed, valued = (m.heads[n, :, lanes] for n in range(3))
            small_query, small_keyed, small_valued = (m.heads_small[n] for n in range(3))
            context, context_small = m.context[:, lanes], m.context_small[...]
            lane, small_lane = lane_of((1, LANE)), lane_of((1, PAD))
            results = []
            for side in range(2):
                head = 2 * pair + side
                chosen = (lane >= 64 * side) & (lane < 64 * side + 64)
                small_chosen = (small_lane >= 16 * head) & (small_lane < 16 * head + 16)
                mask = jnp.where(chosen, 1.0, 0.0).astype(low)
                small_mask = jnp.where(small_chosen, 1.0, 0.0).astype(low)
                probs = m.probs[head]
                grad_probs = dot_nt(context * mask, valued) + dot_nt(
                    context_small * small_mask, small_valued
                )
                inner = jnp.sum(grad_probs * probs, axis=1, keepdims=True)
                scores = probs * (grad_probs - inner)
                scores_low = scores.astype(low)
                scores_turned = scores.T.astype(low)
                probs_turned = probs.T.astype(low)
                results.append(
                    (
                        dot_nn(scores_low, keyed) * 0.125,
                        dot_nn(scores_turned, query) * 0.125,
                        dot_nn(probs_turned, context),
                    )
                )
                small = (
                    dot_nn(scores_low, small_keyed) * 0.25,
                    dot_nn(scores_turned, small_query) * 0.25,
                    dot_nn(probs_turned, context_small),
                )
                for n in range(3):
                    m.mixed[n] += jnp.where(small_chosen, small[n], 0.0)
            for n in range(3):
                m.joined[n, :, lanes] = jnp.where(lane < 64, results[0][n], results[1][n]).astype(
                    low
                )
            return carry


        def pairs(first, number):
            lax.fori_loop(first, first + number, pair_back, 0)

        def turn_rows():
            for part in range(3):
                for side in range(width // cut):
                    levels = depth * cut // width
                    tile = m.joined[part, :, side * cut : (side + 1) * cut].astype(jnp.float32)
                    m.rows_attn[part, pl.ds(side * levels, levels)] = (
                        tile.T.astype(low).reshape(levels, 2, -1, tokens)
                    )
                tile = m.mixed[part].astype(low).astype(jnp.float32)
                m.rows_small[1, pl.ds(part * narrow, narrow), :] = tile.T[:narrow].astype(low)
            cross(layer, 4).start()
            cross(layer, 9).start()
            put(0, total(m.joined[0]))
            put(1, total(m.joined[2]))
            put_small(0, total(m.mixed[0].astype(low)))
            put_small(1, total(m.mixed[2].astype(low)))

        def entering(part, carry):
            m.gx[...] += dot_nn(m.joined[part], unit_rows(slot(2), part))
            return carry


        def attn_sums():
            cross(layer, 4).wait_recv()
            own_sums(
                k + 2,
                m.rows_attn,
                m.rows_land.at[layer, 2],
                lambda owner: m.low[jnp.where(owner == PLANE - 1, 1, 0)],
                lambda owner: m.in_land[layer, jnp.where(owner == PLANE - 1, 1, 0)],
            )


        def enter():
            lax.fori_loop(0, 3, entering, 0)
            if 3 * turn + 4 < 3 * layers:
                weight_load(3 * turn + 4).start()
            grad = m.gy[...]
            for part in range(3):
                grad = grad + dot_nn(m.mixed[part].astype(low), m.small_attn[part])
            m.gy[...] = grad
            for group in range(LANGS):
                put(TABLE_ROW + group, total(onehot[:, group : group + 1] * m.gx[...]))
            if layer == 0:
                layout_turned[...] = m.gy[:, 0:narrow].T
                for one in early():
                    one.start()
                vector_out[...] = m.sums[...]
                vectors.send(0)

        def small_sums():
            for link in (5, 6, 7, 8, 9):
                cross(layer, link).wait_recv()
            arrange = rows_of_core(span, layers, layer, depth, core).astype(low)
            small_rows = (m.rows_small.at[1], m.rows_small.at[0], m.turned_small)
            small_land = (2, 1, 0)
            for member in range(3):
                for block in range(PLANE):
                    rows = pl.ds(block * narrow, narrow)
                    source = (1 if block == PLANE - 1 else 0, 2, 3)[member]
                    own_in = m.down_low_small[...] if member == 2 else m.low_small[source]
                    left = jnp.concatenate(
                        [
                            small_rows[member][rows, :],
                            m.rows_land_small[layer, small_land[member], rows, :],
                        ],
                        axis=1,
                    )
                    right = jnp.concatenate([own_in, m.in_land_small[layer, source]], axis=0)
                    placed = dot_nn(arrange, dot_nn(left, right).astype(low)).astype(low)
                    placed = placed.reshape(depth, layers * span, PAD)
                    lanes = pl.ds(member * PAD, PAD)
                    if turn > 0:
                        placed = mine_small[block, :, :, lanes] + placed
                    mine_small[block, :, :, lanes] = placed
            if layer > 0:
                for link in range(LINKS):
                    cross(layer, link).wait_send()
                for name in names:
                    saved_load(name, layer - 1).start()
            if layer == 0:
                for index in range(4):
                    plane(text_count, index).start()

        own = lambda n: ("o", k + n)
        crossed = lambda link: ("c", layer, link)
        free = lambda n: done(reuse[k + n]) if k + n in reuse else []
        then(("t", 0, turn), tail, 1.7, sends=[("c", 1.0, crossed(1)), ("c", 0.5, crossed(2))])
        then(("t", 1, turn), tail_small, 0.2, sends=[("c", 0.8, crossed(6))])
        then(own(0), own_down, 1.4, [crossed(1), crossed(2)], own_sends(k), free(0))
        add_scatter(k, k)
        then(
            ("h", 0, turn), functools.partial(hidden_blocks, 0, 2), 1.4, sends=[("c", 1.5, crossed(0))]
        )
        then(
            ("h", 1, turn), functools.partial(hidden_blocks, 2, 2), 1.3, sends=[("c", 1.0, crossed(3))]
        )
        then(("h", 2, turn), hide_small, 0.4, sends=[("c", 0.5, crossed(8))])
        then(own(1), own_up, 1.4, [crossed(0), crossed(3)], own_sends(k + 1), free(1))
        add_scatter(k + 1, k + 1)
        then(("n", 0, turn), lower_text, 1.7)
        then(("n", 1, turn), lower_small, 0.4)
        then(("n", 2, turn), contexts, 0.4)
        then(("p", 0, turn), functools.partial(pairs, 0, H // 4), 2.7)
        then(("p", 1, turn), functools.partial(pairs, H // 4, H // 4), 2.7)
        then(("r", turn), turn_rows, 0.4, sends=[("c", 1.0, crossed(4)), ("c", 0.5, crossed(9))])
        then(own(2), attn_sums, 1.4, [crossed(4)], own_sends(k + 2), free(2))
        add_scatter(k + 2, k + 2)
        then(("e", turn), enter, 1.4, sends=[("c", 0.3, ("v", 0))] if layer == 0 else [])
        if layer > 0:
            then(("w", turn), small_sums, 2.6, [crossed(9)])
        else:
            late = [("s", 2, k + 2)]
            then(("o", text_count), small_sums, 2.6, [crossed(9)], own_sends(text_count), late)
            add_scatter(text_count, text_count)

    for turn, layer in enumerate(reversed(range(layers))):
        add_layer(turn, layer)
    for n in range(AllSum.STEPS):
        sends = [((("z", 0), 2.2), (("z", 0), 4.4), ("x", 2.2), ("x", 2.2), ("c", 0.0))[n] + (("v", n + 1),)]
        after = [("v", n - 1)] if n else [("e", layers - 1)]
        plan.add(("v", n), functools.partial(vectors.advance, n), after, [("v", n)], sends, 0.2, -1)
    plan.run()
    vectors.close()
    for link in range(LINKS):
        cross(0, link).wait_send()
    drained = list(reuse.values())
    for k in range(count):
        put_out(k).wait()
    for one in early():
        one.wait()
    for k in range(count):
        if k not in drained:
            drain(k)


def run_backward(depth, layers, narrow, span, gathered, saved, vectors, text_cot, layout_cot, onehot):
    dma = pltpu.SemaphoreType.DMA
    tokens, width = text_cot.shape
    low, full = jnp.bfloat16, jnp.float32
    shapes = back_shapes(layers, depth, tokens, width, 4 * narrow)
    unit = gathered[0].shape[3:]
    small_unit = (layers * span, width)
    units = [unit] * (TEXT_MEMBERS * layers) + [small_unit]
    count = len(units)
    whole = (layers, PLANE, depth, 2, -1, tokens)
    kept = [
        array.reshape(whole) if array.ndim == 3 and array.shape[1] == 4 * width else array
        for array in saved
    ]
    scratch = [pltpu.VMEM(array.shape[1:], array.dtype) for array in kept]
    scratch += [pltpu.VMEM(*shapes[name]) for name in BACK_SCRATCH]
    scratch += [
        pltpu.VMEM((4, PLANE, depth) + unit, low),
        pltpu.VMEM((PLANE, depth) + small_unit, low),
    ]
    fill = 1
    landing = [((2, depth // 2) + one, (2, depth) + one, (depth + 1, 1) + one) for one in units]
    landing[fill] = (
        (2, unit[0] // 2, width),
        (2,) + unit,
        (depth + 1, PLANE) + unit,
    )
    for n in range(3):
        scratch += [pltpu.VMEM(shapes_of[n], low) for shapes_of in landing]
    scratch += [pltpu.VMEM(one, full) for one in units]
    scratch += [
        dma((len(gathered),)),
        dma((len(SAVED), layers)),
        dma((count,)),
        dma((layers, LINKS)),
        dma((layers, LINKS)),
        dma((count, 6)),
        dma((count, 6)),
        dma((count + 3, 2, depth)),
        dma((count + 3, 2, depth)),
    ]
    scratch += AllSum.scratch(vectors.shape)
    scratch += [pltpu.VMEM((narrow, tokens), full), dma((2,))]
    results = pl.pallas_call(
        functools.partial(backward_kernel, depth, layers, narrow, span),
        out_shape=[jax.ShapeDtypeStruct(one, full) for one in units]
        + [
            jax.ShapeDtypeStruct(vectors.shape, full),
            jax.ShapeDtypeStruct((tokens, width), full),
            jax.ShapeDtypeStruct((narrow, tokens), full),
        ],
        in_specs=[ANY] * (len(gathered) + len(kept)) + [IN_VMEM] * 4,
        out_specs=[ANY] * count + [IN_VMEM, ANY, ANY],
        scratch_shapes=scratch,
        compiler_params=pltpu.CompilerParams(
            collective_id=1, has_side_effects=True, vmem_limit_bytes=67000000
        ),
        name="backward_blocks",
    )(*gathered, *kept, vectors, text_cot, layout_cot, onehot)
    return results


def finish_kernel(depth, layers, narrow, span, small_span, *refs):
    count = TEXT_MEMBERS * layers + 1
    summed, totals, ins = refs[:count], refs[count], refs[count + 1 : count + 5]
    outs = refs[count + 5 :]
    width = ins[0].shape[1]
    at, unused = place(depth)
    for n in range(4):
        outs[n][...] = ins[n][...]
    attn, up, down = outs[4:7]
    pieces = outs[7:9] + outs[12:13]
    small_attn, small_up, small_down = outs[9:12]
    for layer in range(layers):
        parts = summed[TEXT_MEMBERS * (layers - 1 - layer) :]
        down[layer] = parts[0][...]
        up[layer] = parts[1][...]
        attn[layer] = parts[2][...]
        rows = summed[count - 1][layer * small_span : (layer + 1) * small_span, :]
        small_attn[layer] = rows[:, 0:narrow]
        small_up[layer] = rows[:, PAD : PAD + narrow]
        small_down[layer] = rows[:, 2 * PAD : 2 * PAD + narrow]
    lane = lane_of((layers, width))
    found = [jnp.zeros((layers, width), jnp.float32) for piece in pieces]
    for row, n, base, lanes in flat_rows(width, narrow):
        first = at.me * pieces[n].shape[1] - base
        rows = jnp.concatenate(
            [totals[pl.ds(layer * VECTOR_ROWS + row, 1), :] for layer in range(layers)], axis=0
        )
        rolled = pltpu.roll(rows, lax.rem(16 * width - first, width), 1)
        index = lane + first
        found[n] = found[n] + jnp.where((index >= 0) & (index < lanes), rolled, 0.0)
    for n, piece in enumerate(pieces):
        piece[...] = found[n][:, : piece.shape[1]]


def run_finish(depth, layers, narrow, span, small_span, lengths, results, text_out, layout_out):
    count = TEXT_MEMBERS * layers + 1
    summed, (totals, text_grad, layout_grad) = results[:count], results[count:]
    tokens, width = text_out.shape
    shapes = [
        (tokens, width),
        (narrow, tokens),
        (tokens, width),
        (narrow, tokens),
        (layers, span, width),
        (layers, span, width),
        (layers, span, width),
        (layers, lengths[0]),
        (layers, lengths[1]),
        (layers, small_span, narrow),
        (layers, small_span, narrow),
        (layers, small_span, narrow),
        (layers, lengths[2]),
    ]
    return pl.pallas_call(
        functools.partial(finish_kernel, depth, layers, narrow, span, small_span),
        out_shape=[jax.ShapeDtypeStruct(shape, jnp.float32) for shape in shapes],
        in_specs=[IN_VMEM] * (count + 5),
        out_specs=[IN_VMEM] * len(shapes),
        name="finish",
    )(*summed, totals, text_out, layout_out, text_grad, layout_grad)


def block_shards(
    depth,
    text_input,
    layout_input,
    text_cot,
    layout_cot,
    segment_ids,
    page_groups,
    lang_table,
    text_attn,
    text_up,
    text_down,
    text_vector,
    layout_attn,
    layout_up,
    layout_down,
    layout_vector,
):
    layers, unused, span = text_attn.shape
    narrow, small_span = layout_input.shape[1], layout_down.shape[1]

    def turned(array):
        return jnp.swapaxes(array, -1, -2)

    weights = (
        turned(text_attn),
        turned(text_up),
        text_down,
        turned(layout_attn),
        turned(layout_up),
        layout_down,
    )
    pieces = (text_vector, lang_table, layout_vector)
    gathered, (vectors, onehot, text_out, layout_out), saved = run_forward(
        depth,
        narrow,
        weights,
        pieces,
        text_input,
        turned(layout_input),
        segment_ids.reshape(1, -1),
        page_groups.reshape(1, -1),
    )
    text_gathered = [part for n, part in enumerate(gathered) if n != 1]
    results = run_backward(
        depth,
        layers,
        narrow,
        small_span,
        text_gathered,
        saved,
        vectors,
        text_cot,
        turned(layout_cot),
        onehot,
    )
    lengths = [piece.shape[1] for piece in pieces]
    outs = run_finish(
        depth, layers, narrow, span, small_span, lengths, results, text_out, layout_out
    )
    return tuple(turned(out) if n in (1, 3, 4, 5, 9, 10) else out for n, out in enumerate(outs))


def solution(mesh):
    in_specs = (
        P(AXES, None),
        P(AXES, None),
        P(AXES, None),
        P(AXES, None),
        P(AXES),
        P(AXES),
        P(None, AXES),
        P(None, None, AXES),
        P(None, None, AXES),
        P(None, AXES, None),
        P(None, AXES),
        P(None, None, AXES),
        P(None, None, AXES),
        P(None, AXES, None),
        P(None, AXES),
    )
    out_specs = (
        P(AXES, None),
        P(AXES, None),
        P(AXES, None),
        P(AXES, None),
        P(None, None, AXES),
        P(None, None, AXES),
        P(None, AXES, None),
        P(None, AXES),
        P(None, AXES),
        P(None, None, AXES),
        P(None, None, AXES),
        P(None, AXES, None),
        P(None, AXES),
    )
    plan = functools.partial(block_shards, mesh.shape[AXES[1]] // 2) if fits_blocks(mesh) else generic_shards
    return jax.shard_map(plan, mesh=mesh, in_specs=in_specs, out_specs=out_specs, check_vma=False)
```

```python
import functools
import math
from types import SimpleNamespace

import jax
import jax.numpy as jnp
from jax import lax
from jax.experimental import pallas as pl
from jax.experimental.pallas import tpu as pltpu
from jax.sharding import PartitionSpec as P

H = 12
LANGS = 8


EPSILON = 1e-05
MASKED = -1e30


def norm_rows(residual, norm_gain, norm_shift):
    average = jnp.mean(residual, axis=-1, keepdims=True)
    centred = residual - average
    variance = jnp.mean(centred * centred, axis=-1, keepdims=True)
    return centred * lax.rsqrt(variance + EPSILON) * norm_gain + norm_shift


def exact_gelu(values):
    return jax.nn.gelu(values, approximate=False)


def norm_back(residual, norm_gain, norm_shift, grad_rows):
    unused, pullback = jax.vjp(norm_rows, residual, norm_gain, norm_shift)
    return pullback(grad_rows)


def gelu_back(upper, grad_rows):
    unused, pullback = jax.vjp(exact_gelu, upper)
    return pullback(grad_rows)[0]


def column_sum(matrix):
    return jnp.sum(matrix.astype(jnp.float32), axis=0)


def unpack(vector, stream_width, hidden_width):
    values = vector.astype(jnp.float32)
    pieces = [values[member * stream_width : (member + 1) * stream_width] for member in range(8)]
    return pieces + [values[8 * stream_width : 8 * stream_width + hidden_width]]


def project(stream_low, attn_weight, pieces):
    stream_width = stream_low.shape[1]
    joined = jnp.dot(
        stream_low, attn_weight[:, : 3 * stream_width], preferred_element_type=jnp.float32
    )
    head_shape = (stream_low.shape[0], H, stream_width // H)
    query = (joined[:, :stream_width] + pieces[0]).astype(jnp.bfloat16).reshape(head_shape)
    keyed = joined[:, stream_width : 2 * stream_width].astype(jnp.bfloat16).reshape(head_shape)
    valued = (joined[:, 2 * stream_width :] + pieces[1]).astype(jnp.bfloat16).reshape(head_shape)
    return (query, keyed, valued)


def joint_scores(text_heads, layout_heads, same_page):
    text_part = jnp.einsum(
        "shd,thd->hst", text_heads[0], text_heads[1], preferred_element_type=jnp.float32
    )
    layout_part = jnp.einsum(
        "shd,thd->hst", layout_heads[0], layout_heads[1], preferred_element_type=jnp.float32
    )
    combined = text_part * (1.0 / math.sqrt(text_heads[0].shape[2])) + layout_part * (
        1.0 / math.sqrt(layout_heads[0].shape[2])
    )
    return jnp.where(same_page[None], combined, MASKED)


def attend(probs_low, valued):
    context = jnp.einsum("hst,thd->shd", probs_low, valued, preferred_element_type=jnp.float32)
    return context.reshape(context.shape[0], -1).astype(jnp.bfloat16)


def tail_forward(stream_rows, context_low, attn_weight, up_weight, down_weight, pieces):
    stream_width = stream_rows.shape[1]
    branch = (
        jnp.dot(context_low, attn_weight[:, 3 * stream_width :], preferred_element_type=jnp.float32)
        + pieces[2]
    )
    first_sum = stream_rows + branch
    normed = norm_rows(first_sum, pieces[4], pieces[5])
    normed_low = normed.astype(jnp.bfloat16)
    upper = jnp.dot(normed_low, up_weight, preferred_element_type=jnp.float32) + pieces[8]
    active_low = exact_gelu(upper).astype(jnp.bfloat16)
    second_sum = (
        normed + jnp.dot(active_low, down_weight, preferred_element_type=jnp.float32) + pieces[3]
    )
    result = norm_rows(second_sum, pieces[6], pieces[7])
    return (result, (first_sum, normed_low, upper, active_low, second_sum))


def layer_forward(text_rows, layout_rows, text_weights, layout_weights, same_page, onehot):
    group_table = text_weights[4].astype(jnp.float32).reshape(onehot.shape[1], -1)
    text_rows = text_rows + jnp.dot(onehot, group_table, precision=lax.Precision.HIGHEST)
    text_pieces = unpack(text_weights[3], text_rows.shape[1], text_weights[1].shape[1])
    layout_pieces = unpack(layout_weights[3], layout_rows.shape[1], layout_weights[1].shape[1])
    text_low = text_rows.astype(jnp.bfloat16)
    layout_low = layout_rows.astype(jnp.bfloat16)
    text_heads = project(text_low, text_weights[0], text_pieces)
    layout_heads = project(layout_low, layout_weights[0], layout_pieces)
    scores = joint_scores(text_heads, layout_heads, same_page)
    row_peak = jnp.max(scores, axis=-1, keepdims=True)
    log_total = row_peak + jnp.log(jnp.sum(jnp.exp(scores - row_peak), axis=-1, keepdims=True))
    probs_low = jnp.exp(scores - log_total).astype(jnp.bfloat16)
    text_context = attend(probs_low, text_heads[2])
    layout_context = attend(probs_low, layout_heads[2])
    text_next, text_stored = tail_forward(
        text_rows, text_context, text_weights[0], text_weights[1], text_weights[2], text_pieces
    )
    layout_next, layout_stored = tail_forward(
        layout_rows,
        layout_context,
        layout_weights[0],
        layout_weights[1],
        layout_weights[2],
        layout_pieces,
    )
    stored = (
        text_low,
        layout_low,
        text_heads,
        layout_heads,
        log_total,
        text_context,
        layout_context,
        text_stored,
        layout_stored,
    )
    return (text_next, layout_next, stored)


def tail_backward(grad_result, stored, context_low, attn_weight, up_weight, down_weight, pieces):
    first_sum, normed_low, upper, active_low, second_sum = stored
    stream_width = first_sum.shape[1]
    grad_second, grad_gain_two, grad_shift_two = norm_back(
        second_sum, pieces[6], pieces[7], grad_result
    )
    grad_down_low = grad_second.astype(jnp.bfloat16)
    grad_down_bias = column_sum(grad_down_low)
    grad_down = jnp.einsum(
        "sf,sd->fd", active_low, grad_down_low, preferred_element_type=jnp.float32
    )
    grad_active = jnp.einsum(
        "sd,fd->sf", grad_down_low, down_weight, preferred_element_type=jnp.float32
    )
    grad_upper_low = gelu_back(upper, grad_active).astype(jnp.bfloat16)
    grad_up_bias = column_sum(grad_upper_low)
    grad_up = jnp.einsum(
        "sd,sf->df", normed_low, grad_upper_low, preferred_element_type=jnp.float32
    )
    grad_normed = grad_second + jnp.einsum(
        "sf,df->sd", grad_upper_low, up_weight, preferred_element_type=jnp.float32
    )
    grad_first, grad_gain_one, grad_shift_one = norm_back(
        first_sum, pieces[4], pieces[5], grad_normed
    )
    grad_branch_low = grad_first.astype(jnp.bfloat16)
    grad_out_bias = column_sum(grad_branch_low)
    output_weight = attn_weight[:, 3 * stream_width :]
    grad_output_proj = jnp.einsum(
        "sd,se->de", context_low, grad_branch_low, preferred_element_type=jnp.float32
    )
    grad_context = jnp.einsum(
        "se,de->sd", grad_branch_low, output_weight, preferred_element_type=jnp.float32
    ).astype(jnp.bfloat16)
    matrices = (grad_output_proj, grad_up, grad_down)
    vectors = (
        grad_out_bias,
        grad_down_bias,
        grad_gain_one,
        grad_shift_one,
        grad_gain_two,
        grad_shift_two,
        grad_up_bias,
    )
    return (grad_first, grad_context, matrices, vectors)


def head_grads(head_set, grad_context_low, probs_low, grad_scores_low):
    inverse_root = 1.0 / math.sqrt(head_set[0].shape[2])
    grad_heads = grad_context_low.reshape(head_set[2].shape)
    grad_query = (
        jnp.einsum("hst,thd->shd", grad_scores_low, head_set[1], preferred_element_type=jnp.float32)
        * inverse_root
    )
    grad_key = (
        jnp.einsum("hst,shd->thd", grad_scores_low, head_set[0], preferred_element_type=jnp.float32)
        * inverse_root
    )
    grad_value = jnp.einsum(
        "hst,shd->thd", probs_low, grad_heads, preferred_element_type=jnp.float32
    )
    row_count = head_set[0].shape[0]
    joined = jnp.concatenate(
        [
            grad_query.reshape(row_count, -1),
            grad_key.reshape(row_count, -1),
            grad_value.reshape(row_count, -1),
        ],
        axis=1,
    )
    return joined.astype(jnp.bfloat16)


def attention_backward(
    text_heads, layout_heads, log_total, same_page, grad_text_context, grad_layout_context
):
    scores = joint_scores(text_heads, layout_heads, same_page)
    probs = jnp.exp(scores - log_total)
    probs_low = probs.astype(jnp.bfloat16)
    grad_text_heads = grad_text_context.reshape(text_heads[2].shape)
    grad_layout_heads = grad_layout_context.reshape(layout_heads[2].shape)
    grad_probs = jnp.einsum(
        "shd,thd->hst", grad_text_heads, text_heads[2], preferred_element_type=jnp.float32
    )
    grad_probs = grad_probs + jnp.einsum(
        "shd,thd->hst", grad_layout_heads, layout_heads[2], preferred_element_type=jnp.float32
    )
    inner = jnp.sum(grad_probs * probs, axis=-1, keepdims=True)
    grad_scores_low = (probs * (grad_probs - inner)).astype(jnp.bfloat16)
    text_joined = head_grads(text_heads, grad_text_context, probs_low, grad_scores_low)
    layout_joined = head_grads(layout_heads, grad_layout_context, probs_low, grad_scores_low)
    return (text_joined, layout_joined)


def head_backward(stream_low, grad_joined_low, attn_weight, grad_first, matrices, vectors):
    stream_width = stream_low.shape[1]
    grad_in_proj = jnp.einsum(
        "sd,se->de", stream_low, grad_joined_low, preferred_element_type=jnp.float32
    )
    grad_bias_query = column_sum(grad_joined_low[:, :stream_width])
    grad_bias_value = column_sum(grad_joined_low[:, 2 * stream_width :])
    grad_stream = grad_first + jnp.einsum(
        "se,de->sd",
        grad_joined_low,
        attn_weight[:, : 3 * stream_width],
        preferred_element_type=jnp.float32,
    )
    grad_attn = jnp.concatenate([grad_in_proj, matrices[0]], axis=1)
    grad_vector = jnp.concatenate([grad_bias_query, grad_bias_value] + list(vectors))
    return (grad_stream, (grad_attn, matrices[1], matrices[2], grad_vector))


def layer_backward(grad_text, grad_layout, stored, text_weights, layout_weights, same_page, onehot):
    (
        text_low,
        layout_low,
        text_heads,
        layout_heads,
        log_total,
        text_context,
        layout_context,
        text_stored,
        layout_stored,
    ) = stored
    text_pieces = unpack(text_weights[3], text_low.shape[1], text_weights[1].shape[1])
    layout_pieces = unpack(layout_weights[3], layout_low.shape[1], layout_weights[1].shape[1])
    text_first, grad_text_context, text_mats, text_vecs = tail_backward(
        grad_text,
        text_stored,
        text_context,
        text_weights[0],
        text_weights[1],
        text_weights[2],
        text_pieces,
    )
    layout_first, grad_layout_context, layout_mats, layout_vecs = tail_backward(
        grad_layout,
        layout_stored,
        layout_context,
        layout_weights[0],
        layout_weights[1],
        layout_weights[2],
        layout_pieces,
    )
    text_joined, layout_joined = attention_backward(
        text_heads, layout_heads, log_total, same_page, grad_text_context, grad_layout_context
    )
    grad_text_in, text_terms = head_backward(
        text_low, text_joined, text_weights[0], text_first, text_mats, text_vecs
    )
    grad_layout_in, layout_terms = head_backward(
        layout_low, layout_joined, layout_weights[0], layout_first, layout_mats, layout_vecs
    )
    grad_group = jnp.einsum(
        "sg,sd->gd", onehot, grad_text_in, precision=lax.Precision.HIGHEST
    ).reshape(-1)
    return (grad_text_in, grad_layout_in, text_terms + (grad_group,), layout_terms)


def fetch_layer(
    text_attn,
    text_up,
    text_down,
    text_vector,
    lang_table,
    layout_attn,
    layout_up,
    layout_down,
    layout_vector,
    layer_index,
):
    fetched = (
        lax.all_gather(text_attn[layer_index], AXES, axis=1, tiled=True),
        lax.all_gather(text_up[layer_index], AXES, axis=1, tiled=True),
        lax.all_gather(text_down[layer_index], AXES, axis=0, tiled=True),
        lax.all_gather(text_vector[layer_index], AXES, axis=0, tiled=True),
        lax.all_gather(lang_table[layer_index], AXES, axis=0, tiled=True),
        lax.all_gather(layout_attn[layer_index], AXES, axis=1, tiled=True),
        lax.all_gather(layout_up[layer_index], AXES, axis=1, tiled=True),
        lax.all_gather(layout_down[layer_index], AXES, axis=0, tiled=True),
        lax.all_gather(layout_vector[layer_index], AXES, axis=0, tiled=True),
    )
    return (fetched[:5], fetched[5:])


def fetch_layer_back(
    text_attn,
    text_up,
    text_down,
    text_vector,
    lang_table,
    layout_attn,
    layout_up,
    layout_down,
    layout_vector,
    layer_index,
):
    fetched = (
        lax.all_gather(text_attn[layer_index], AXES, axis=1, tiled=True),
        lax.all_gather(text_up[layer_index], AXES, axis=1, tiled=True),
        lax.all_gather(text_down[layer_index], AXES, axis=0, tiled=True),
        lax.all_gather(text_vector[layer_index], AXES, axis=0, tiled=True),
        lax.all_gather(lang_table[layer_index], AXES, axis=0, tiled=True),
        lax.all_gather(layout_attn[layer_index], AXES, axis=1, tiled=True),
        lax.all_gather(layout_up[layer_index], AXES, axis=1, tiled=True),
        lax.all_gather(layout_down[layer_index], AXES, axis=0, tiled=True),
        lax.all_gather(layout_vector[layer_index], AXES, axis=0, tiled=True),
    )
    return (fetched[:5], fetched[5:])


def generic_shards(
    text_input,
    layout_input,
    text_cot,
    layout_cot,
    segment_ids,
    page_groups,
    lang_table,
    text_attn,
    text_up,
    text_down,
    text_vector,
    layout_attn,
    layout_up,
    layout_down,
    layout_vector,
):
    layer_count = text_attn.shape[0]
    same_page = segment_ids[:, None] == segment_ids[None, :]
    page_slot = segment_ids % 2
    token_group = jnp.where(page_slot == 0, page_groups[0], page_groups[1])
    onehot = (token_group[:, None] == jnp.arange(LANGS, dtype=jnp.int32)[None, :]).astype(
        jnp.float32
    )
    text_rows = text_input.astype(jnp.float32)
    layout_rows = layout_input.astype(jnp.float32)
    saved_layers = []
    for layer_index in range(layer_count):
        text_fetched, layout_fetched = fetch_layer(
            text_attn,
            text_up,
            text_down,
            text_vector,
            lang_table,
            layout_attn,
            layout_up,
            layout_down,
            layout_vector,
            layer_index,
        )
        text_rows, layout_rows, stored = layer_forward(
            text_rows, layout_rows, text_fetched, layout_fetched, same_page, onehot
        )
        saved_layers.append(stored)
    grad_text = text_cot.astype(jnp.float32)
    grad_layout = layout_cot.astype(jnp.float32)
    owned_all = [None] * layer_count
    for layer_index in reversed(range(layer_count)):
        text_fetched, layout_fetched = fetch_layer_back(
            text_attn,
            text_up,
            text_down,
            text_vector,
            lang_table,
            layout_attn,
            layout_up,
            layout_down,
            layout_vector,
            layer_index,
        )
        grad_text, grad_layout, text_terms, layout_terms = layer_backward(
            grad_text,
            grad_layout,
            saved_layers[layer_index],
            text_fetched,
            layout_fetched,
            same_page,
            onehot,
        )
        joined_terms = tuple(text_terms) + tuple(layout_terms)
        owned_all[layer_index] = (
            lax.psum_scatter(joined_terms[0], AXES, scatter_dimension=1, tiled=True),
            lax.psum_scatter(joined_terms[1], AXES, scatter_dimension=1, tiled=True),
            lax.psum_scatter(joined_terms[2], AXES, scatter_dimension=0, tiled=True),
            lax.psum_scatter(joined_terms[3], AXES, scatter_dimension=0, tiled=True),
            lax.psum_scatter(joined_terms[4], AXES, scatter_dimension=0, tiled=True),
            lax.psum_scatter(joined_terms[5], AXES, scatter_dimension=1, tiled=True),
            lax.psum_scatter(joined_terms[6], AXES, scatter_dimension=1, tiled=True),
            lax.psum_scatter(joined_terms[7], AXES, scatter_dimension=0, tiled=True),
            lax.psum_scatter(joined_terms[8], AXES, scatter_dimension=0, tiled=True),
        )
    stacks = [jnp.stack([owned[member] for owned in owned_all]) for member in range(9)]
    return (
        text_rows,
        layout_rows,
        grad_text,
        grad_layout,
        stacks[0],
        stacks[1],
        stacks[2],
        stacks[3],
        stacks[4],
        stacks[5],
        stacks[6],
        stacks[7],
        stacks[8],
    )


MESH = pl.DeviceIdType.MESH
AXES = ("dp", "shard")
ANY = pl.BlockSpec(memory_space=pl.ANY)
IN_VMEM = pl.BlockSpec(memory_space=pltpu.VMEM)
PLANE = 4
SUBLANES = 8
VECTOR_ROWS = 32


def fits_blocks(mesh):
    return mesh.shape[AXES[0]] == PLANE and mesh.shape[AXES[1]] == 2 * PLANE


def place(depth):
    dp, shard = lax.axis_index(AXES[0]), lax.axis_index(AXES[1])
    core, level = lax.rem(shard, 2), shard // 2
    dx = dp + 1 - 2 * lax.rem(dp, 2)
    dy = lax.rem(dp + 2, PLANE)
    me = dp * (2 * depth) + shard
    at = SimpleNamespace(dp=dp, z=level, core=core, dx=dx, dy=dy, dd=PLANE - 1 - dp, me=me)

    def device(plane_index, shard_index):
        return dict(zip(AXES, (plane_index, shard_index)))

    devices = SimpleNamespace(
        x=device(dx, shard),
        y=device(dy, shard),
        up=device(dp, lax.rem(shard + 2, 2 * depth)),
        down=device(dp, lax.rem(shard + 2 * depth - 2, 2 * depth)),
        far=device(dp, lax.rem(shard + depth, 2 * depth)),
        pair=device(dp, 2 * (level + 1 - 2 * lax.rem(level, 2)) + core),
        core=device(dp, shard + 1 - 2 * core),
    )
    return at, devices


def signal(devices):
    barrier = pltpu.get_barrier_semaphore()
    partners = (devices.x, devices.y, devices.up, devices.down, devices.far, devices.core)
    for partner in partners:
        pl.semaphore_signal(barrier, inc=1, device_id=partner, device_id_type=MESH)


def greeted():
    pl.semaphore_wait(pltpu.get_barrier_semaphore(), 6)


def remote(source, target, send_sem, recv_sem, device):
    return pltpu.make_async_remote_copy(
        src_ref=source,
        dst_ref=target,
        send_sem=send_sem,
        recv_sem=recv_sem,
        device_id=device,
        device_id_type=MESH,
    )


class AllSum:
    STEPS = 5

    def __init__(self, devices, running, held, landed, send_sem, recv_sem):
        self.partners = (devices.core, devices.pair, devices.far, devices.x, devices.y)
        self.running, self.held, self.landed = running, held, landed
        self.send_sem, self.recv_sem = send_sem, recv_sem

    def copy(self, step):
        return remote(
            self.held.at[step],
            self.landed.at[step],
            self.send_sem.at[step],
            self.recv_sem.at[step],
            self.partners[step],
        )

    def send(self, step):
        self.held[step] = self.running[...].astype(self.held.dtype)
        self.copy(step).start()

    def advance(self, step):
        self.copy(step).wait_recv()
        self.running[...] += self.landed[step].astype(jnp.float32)
        if step + 1 < self.STEPS:
            self.send(step + 1)

    def close(self):
        for step in range(self.STEPS):
            self.copy(step).wait_send()

    @classmethod
    def scratch(cls, shape):
        return [
            pltpu.VMEM((cls.STEPS,) + shape, jnp.bfloat16),
            pltpu.VMEM((cls.STEPS,) + shape, jnp.bfloat16),
            pltpu.SemaphoreType.DMA((cls.STEPS,)),
            pltpu.SemaphoreType.DMA((cls.STEPS,)),
        ]


class Plan:
    LAG = dict(x=2.4, z=2.4, c=1.0, h=0.3)
    PATIENCE = 1.0

    def __init__(self):
        self.tasks = []

    def add(self, name, run, after=(), needs=(), sends=(), time=0.2, rank=0, patient=False):
        self.tasks.append((name, run, tuple(after), tuple(needs), tuple(sends), time, rank, patient))

    def order(self):
        now, free, landed, done = 0.0, {}, {}, set()
        waiting, result = list(self.tasks), []
        while waiting:
            best = None
            for place_in_list, task in enumerate(waiting):
                name, run, after, needs, sends, time, rank, patient = task
                if any(other not in done for other in after):
                    continue
                if any(event not in landed for event in needs):
                    continue
                start = max([now] + [landed[event] for event in needs])
                key = (start + (self.PATIENCE if patient else 0.0), rank, place_in_list)
                if best is None or key < best[0]:
                    best = (key, task, start)
            assert best is not None
            task, start = best[1:]
            waiting.remove(task)
            result.append(task)
            name, run, after, needs, sends, time, rank, patient = task
            now = start + time
            done.add(name)
            for link, amount, event in sends:
                free[link] = max(now, free.get(link, 0.0)) + amount
                landed[event] = free[link] + self.LAG[link[0]]
        return result

    def run(self):
        for task in self.order():
            task[1]()


UNIT_ROWS_PER_US = 96 / 3.26


def add_rows(target, term):
    total = target[...].astype(jnp.float32) + term[...].astype(jnp.float32)
    target[...] = total.astype(target.dtype)


def add_units(target, *terms):
    def body(index, carry):
        total = target[index].astype(jnp.float32)
        for term in terms:
            total = total + term[index].astype(jnp.float32)
        target[index] = total.astype(target.dtype)
        return carry

    lax.fori_loop(0, target.shape[0], body, 0)


LANE = 128
PAD = 256
PIECE_ROWS = 12
TABLE_ROW = 12
SMALL_ROW = 20
SMALL_HIDDEN_ROW = 28


def dot_nt(left, right):
    return lax.dot_general(
        left, right, (((1,), (1,)), ((), ())), preferred_element_type=jnp.float32
    )


def dot_nn(left, right):
    return jnp.dot(left, right, preferred_element_type=jnp.float32)


def lane_of(shape):
    return lax.broadcasted_iota(jnp.int32, shape, len(shape) - 1)


def unit_rows(ref, dp):
    block = ref[dp]
    return block.reshape(-1, block.shape[-1])


def standard(residual, width):
    padded = residual.shape[1] != width
    average = jnp.sum(residual, axis=1, keepdims=True) * (1.0 / width)
    centred = residual - average
    if padded:
        centred = jnp.where(lane_of(residual.shape) < width, centred, 0.0)
    variance = jnp.sum(centred * centred, axis=1, keepdims=True) * (1.0 / width)
    scale = lax.rsqrt(variance + EPSILON)
    return centred * scale, scale


def gelu_parts(upper):
    cdf = 0.5 * (1.0 + lax.erf(upper * math.sqrt(0.5)))
    density = jnp.exp(upper * upper * -0.5) * (1.0 / math.sqrt(2.0 * math.pi))
    return upper * cdf, cdf + upper * density


def unit_of(index, size, count):
    unit = jnp.zeros(index.shape, jnp.int32)
    for n in range(1, count):
        unit = unit + jnp.where(index >= n * size, 1, 0)
    return unit


def natural_rows(span, layers, layer):
    units = 8
    shape = (PAD, units * layers * span)
    row = lax.broadcasted_iota(jnp.int32, shape, 0)
    column = lax.broadcasted_iota(jnp.int32, shape, 1)
    unit = unit_of(row, span, units)
    source = unit * (layers - 1) * span + layer * span + row
    return jnp.where((source == column) & (row < units * span), 1.0, 0.0)


def saved_shapes(layers, tokens, width, narrow_hidden):
    low, full = jnp.bfloat16, jnp.float32
    hidden = 4 * width
    return dict(
        low=((layers, 3, tokens, width), low),
        low_small=((layers, 3, tokens, PAD), low),
        heads=((layers, 3, tokens, width), low),
        heads_small=((layers, 3, tokens, PAD), low),
        probs=((layers, H, tokens, tokens), full),
        norm=((layers, 2, tokens, width), full),
        norm_small=((layers, 2, tokens, PAD), full),
        scales=((layers, 4, tokens, LANE), full),
        slope=((layers, tokens, hidden), full),
        slope_small=((layers, tokens, narrow_hidden), full),
        turned=((layers, hidden, tokens), low),
        turned_small=((layers, narrow_hidden, tokens), low),
        small_attn=((layers, 4, PAD, PAD), low),
        small_ff=((layers, 2, narrow_hidden, PAD), low),
    )


SAVED = tuple(saved_shapes(1, 1, 1, 1))


def forward_steps(layer, m, narrow, span):
    tokens, width = m.x.shape
    low = jnp.bfloat16
    vec = lambda row, count=1: m.vectors[pl.ds(layer * VECTOR_ROWS + row, count), :]
    small_vec = lambda row: vec(SMALL_ROW + row)[:, :PAD]

    def embed():
        rows = m.x[...]
        for group in range(LANGS):
            rows = rows + m.onehot[:, group : group + 1] * vec(TABLE_ROW + group)
        m.x[...] = rows
        m.low[layer, 0] = rows.astype(low)
        m.low_small[layer, 0] = m.y[...].astype(low)

    def project_text():
        def body(part, carry):
            joined = dot_nt(m.low[layer, 0], unit_rows(m.attn_w, part))
            bias = jnp.where(part == 0, vec(0), jnp.where(part == 2, vec(1), 0.0))
            m.heads[layer, part] = (joined + bias).astype(low)
            return carry

        lax.fori_loop(0, 3, body, 0)

    def prepare_small():
        permute = natural_rows(span, m.small_raw_layers, layer).astype(low)

        def body(block, carry):
            for member in range(3):
                raw = m.small_raw[block, :, :, :, pl.ds(member * PAD, PAD)].reshape(-1, PAD)
                rows = dot_nn(permute, raw).astype(low)
                if member == 0:
                    m.small_attn[layer, block] = rows
                else:
                    start = pl.multiple_of(block * narrow, 64)
                    m.small_ff[layer, member - 1, pl.ds(start, narrow), :] = rows[:narrow]
            return carry

        lax.fori_loop(0, PLANE, body, 0)

    def project_small():
        for part in range(3):
            joined = dot_nt(m.low_small[layer, 0], m.small_attn[layer, part])
            if part == 0:
                joined = joined + small_vec(0)
            if part == 2:
                joined = joined + small_vec(1)
            m.heads_small[layer, part] = joined.astype(low)
        m.mixed[...] = jnp.zeros_like(m.mixed)

    def attend_pairs(first, count):
        def body(pair, carry):
            lanes = pl.ds(pl.multiple_of(pair * LANE, LANE), LANE)
            query, keyed, valued = (m.heads[layer, n, :, lanes] for n in range(3))
            small_query, small_keyed, small_valued = (m.heads_small[layer, n] for n in range(3))
            lane, small_lane = lane_of((1, LANE)), lane_of((1, PAD))
            same = m.same[...] > 0.0
            contexts = []
            for side in range(2):
                head = 2 * pair + side
                chosen = (lane >= 64 * side) & (lane < 64 * side + 64)
                small_chosen = (small_lane >= 16 * head) & (small_lane < 16 * head + 16)
                mask = jnp.where(chosen, 0.125, 0.0).astype(low)
                small_mask = jnp.where(small_chosen, 0.25, 0.0).astype(low)
                scores = dot_nt(query * mask, keyed) + dot_nt(small_query * small_mask, small_keyed)
                scores = jnp.where(same, scores, MASKED)
                peak = jnp.max(scores, axis=1, keepdims=True)
                powers = jnp.exp(scores - peak)
                probs = powers * (1.0 / jnp.sum(powers, axis=1, keepdims=True))
                m.probs[layer, head] = probs
                probs_low = probs.astype(low)
                contexts.append(dot_nn(probs_low, valued))
                m.mixed[...] += jnp.where(small_chosen, dot_nn(probs_low, small_valued), 0.0)
            m.low[layer, 1, :, lanes] = jnp.where(lane < 64, contexts[0], contexts[1]).astype(low)
            return carry

        lax.fori_loop(first, first + count, body, 0)

    def first_norm():
        m.low_small[layer, 1] = m.mixed[...].astype(low)
        residual = m.x[...] + dot_nt(m.low[layer, 1], unit_rows(m.attn_w, 3)) + vec(2)
        normed, scale = standard(residual, width)
        m.norm[layer, 0] = normed
        m.scales[layer, 0] = jnp.broadcast_to(scale, (tokens, LANE))
        result = normed * vec(4) + vec(5)
        m.normed[...] = result
        m.low[layer, 2] = result.astype(low)

    def first_norm_small():
        branch = dot_nt(m.low_small[layer, 1], m.small_attn[layer, 3]) + small_vec(2)
        normed, scale = standard(m.y[...] + branch, narrow)
        m.norm_small[layer, 0] = normed
        m.scales[layer, 1] = jnp.broadcast_to(scale, (tokens, LANE))
        result = normed * small_vec(4) + small_vec(5)
        m.normed_small[...] = result
        m.low_small[layer, 2] = result.astype(low)

    def activate(column, upper_ref, source, active, slope, turned):
        here = pl.ds(column, LANE)
        value, rate = gelu_parts(upper_ref[:, source])
        slope[layer, :, here] = rate
        value_low = value.astype(low)
        active[:, here] = value_low
        turned[layer, here, :] = value.T.astype(low)

    def up_small():
        m.upper[...] = dot_nt(m.low_small[layer, 2], m.small_ff[layer, 0]) + vec(SMALL_HIDDEN_ROW)

        def body(tile, carry):
            column = pl.multiple_of(tile * LANE, LANE)
            activate(
                column, m.upper, pl.ds(column, LANE), m.active_small, m.slope_small, m.turned_small
            )
            return carry

        lax.fori_loop(0, m.active_small.shape[1] // LANE, body, 0)

    def down_small():
        second = dot_nn(m.active_small[...], m.small_ff[layer, 1]) + small_vec(3)
        normed, scale = standard(m.normed_small[...] + second, narrow)
        m.norm_small[layer, 1] = normed
        m.scales[layer, 3] = jnp.broadcast_to(scale, (tokens, LANE))
        m.y[...] = normed * small_vec(6) + small_vec(7)

    def up_text(first, count):
        def body(block, carry):
            m.upper[...] = dot_nt(m.low[layer, 2], unit_rows(m.up_w, block)) + vec(8 + block)

            def tile_body(tile, inner):
                column = pl.multiple_of(tile * LANE, LANE)
                activate(
                    pl.multiple_of(block * width + column, LANE),
                    m.upper,
                    pl.ds(column, LANE),
                    m.active,
                    m.slope,
                    m.turned,
                )
                return inner

            return lax.fori_loop(0, width // LANE, tile_body, carry)

        lax.fori_loop(first, first + count, body, 0)

    def down_text(first, count):
        def body(block, carry):
            columns = pl.ds(pl.multiple_of(block * width, LANE), width)
            m.second[...] += dot_nn(m.active[:, columns], unit_rows(m.down_w, block))
            return carry

        if first == 0:
            m.second[...] = m.normed[...] + vec(3)
        lax.fori_loop(first, first + count, body, 0)

    def second_norm():
        normed, scale = standard(m.second[...], width)
        m.norm[layer, 1] = normed
        m.scales[layer, 2] = jnp.broadcast_to(scale, (tokens, LANE))
        m.x[...] = normed * vec(6) + vec(7)

    part = H // 4
    after_attn = [(embed, 0.4), (project_text, 1.6)]
    after_small = [(prepare_small, 0.8), (project_small, 0.3)]
    for first in range(0, H // 2, part):
        after_small.append((functools.partial(attend_pairs, first, part), 2.5))
    after_small += [(first_norm, 0.8), (first_norm_small, 0.4), (up_small, 1.0), (down_small, 0.4)]
    after_up = [(functools.partial(up_text, first, 2), 2.4) for first in (0, 2)]
    after_down = [(functools.partial(down_text, first, 2), 0.7) for first in (0, 2)]
    after_down.append((second_norm, 0.3))
    return after_attn, after_small, after_up, after_down


def forward_shapes(layers, depth, tokens, width, narrow, small_span):
    low, full = jnp.bfloat16, jnp.float32
    span = 4 * width // (PLANE * depth * 2)
    whole = (PLANE, depth, 2, span, width)
    return dict(
        attn_w=(whole, low),
        up_w=(whole, low),
        down_w=(whole, low),
        small_raw=((PLANE, depth, 2, layers * small_span, width), low),
        own_small=((layers * small_span, width), low),
        own_small_full=((layers * small_span, width), full),
        same=((tokens, tokens), full),
        x=((tokens, width), full),
        y=((tokens, PAD), full),
        mixed=((tokens, PAD), full),
        normed=((tokens, width), full),
        normed_small=((tokens, PAD), full),
        upper=((tokens, width), full),
        active=((tokens, 4 * width), low),
        active_small=((tokens, 4 * narrow), low),
        second=((tokens, width), full),
        spread=((3 * SUBLANES, width), full),
    )


FORWARD_SCRATCH = tuple(forward_shapes(1, 1, 1, 1, 1, 1))


def flat_rows(width, narrow):
    rows = [(n, 0, n * width, width) for n in range(PIECE_ROWS)]
    rows += [(TABLE_ROW + n, 1, n * width, width) for n in range(LANGS)]
    rows += [(SMALL_ROW + n, 2, n * narrow, narrow) for n in range(8)]
    return rows + [(SMALL_HIDDEN_ROW, 2, 8 * narrow, 4 * narrow)]


def forward_kernel(depth, layers, narrow, span, *refs):
    refs = list(refs)

    def take(number):
        taken = refs[:number]
        del refs[:number]
        return taken

    count = 3 * layers + 1
    fill = count - 2
    text_attn, text_up, text_down, layout_attn, layout_up, layout_down = take(6)
    pieces = take(3)
    text_in, layout_in, page_row, groups = take(4)
    outs = take(count)
    vector_out, onehot_out, text_out, layout_out = take(4)
    kept = take(len(SAVED))
    own_sem, zs, zr, ps, pr, us, ur, cs, cr, load_sem, keep_sem = take(11)
    all_sum = take(4)
    m = SimpleNamespace()
    for name in SAVED + FORWARD_SCRATCH:
        setattr(m, name, refs.pop(0))
    m.vectors, m.onehot, m.small_raw_layers = vector_out, onehot_out, layers
    at, devices = place(depth)
    dp, z, core, dx, dy, dd = at.dp, at.z, at.core, at.dx, at.dy, at.dd
    half = depth // 2
    low, full = jnp.bfloat16, jnp.float32
    tokens, width = m.x.shape
    vectors = AllSum(devices, vector_out, *all_sum)

    sources = [text_attn.at[0], m.own_small]
    for layer in range(layers):
        if layer > 0:
            sources.append(text_attn.at[layer])
        sources += [text_up.at[layer], text_down.at[layer]]

    def own(k):
        return pltpu.make_async_copy(sources[k], outs[k].at[dp, z, core], own_sem.at[k])

    def line(k, rising, hop, side=0):
        level = z - hop if rising else z + hop
        owner = (dp, dx, dy, dd)[side]
        target = outs[k].at[owner, level, core]
        row = k if side == 0 else count - 1 + side
        return remote(
            sources[k] if hop == 0 and side == 0 else target,
            target,
            zs.at[row, int(rising), hop],
            zr.at[row, level],
            devices.up if rising else devices.down,
        )

    def exists(rising, hop):
        return (z - hop >= 0) if rising else (z + hop < depth)

    def goes_on(rising, hop):
        return exists(rising, hop) & ((z < depth - 1) if rising else (z > 0))

    def unit(rising, hop, to_x):
        level = z - hop if rising else z + hop
        target = outs[0].at[dp, level, core]
        return remote(
            sources[0] if hop == 0 else target,
            target,
            us.at[int(to_x), level],
            ur.at[int(to_x), level],
            devices.x if to_x else devices.y,
        )

    def unit_landed(to_x, level):
        target = outs[0].at[dx if to_x else dy, level, core]
        return remote(
            target, target, us.at[int(to_x), level], ur.at[int(to_x), level], devices.x
        )

    def line_start(k, hop, side=0):
        for rising in (True, False):

            @pl.when(goes_on(rising, hop))
            def start():
                line(k, rising, hop, side).start()

    def line_wait(k, hop, side=0, then=None):
        for rising in (True, False):

            @pl.when(exists(rising, hop))
            def wait():
                line(k, rising, hop, side).wait_recv()
                if then is not None:
                    then(rising, hop)

    def unit_start(rising, hop):
        unit(rising, hop, True).start()
        unit(rising, hop, False).start()

    def plane(k, index, sending=True):
        if k == fill:
            rows = span // 2
            lower, upper = pl.ds(0, rows), pl.ds(rows, rows)
            if sending:
                blocks = ((dp, None), (dp, None), (dx, lower), (dy, upper))
            else:
                blocks = ((dx, None), (dy, None), (dd, lower), (dd, upper))
            owner, rows = blocks[index]
            block = outs[k].at[owner, z, core]
            block = block if rows is None else block.at[rows]
            source = sources[k] if sending and index < 2 else block
        else:
            lower, upper, every = pl.ds(0, half), pl.ds(half, half), pl.ds(0, depth)
            if sending:
                blocks = ((dp, every), (dp, every), (dx, lower), (dy, upper))
            else:
                blocks = ((dx, every), (dy, every), (dd, lower), (dd, upper))
            owner, levels = blocks[index]
            block = outs[k].at[owner, levels, core]
            source = block
        device = (devices.x, devices.y, devices.y, devices.x)[index]
        return remote(source, block, ps.at[k, index], pr.at[k, index], device)

    def across(k, index, side):
        lower, upper, every = pl.ds(0, half), pl.ds(half, half), pl.ds(0, depth)
        if k == fill:
            blocks = ((dp, every), (dx, every), (dy, every), (dd, every))
        else:
            blocks = ((dp, every), (dx, every), (dy, every), (dd, lower), (dd, upper))
        owner, levels = blocks[index]
        block = outs[k].at[owner, levels, side]
        return remote(block, block, cs.at[k, index], cr.at[k, index], devices.core)

    def landed_across(k):
        return range(4 if k == fill else 5)

    held = [m.attn_w, m.small_raw, m.up_w, m.down_w] + [m.attn_w, m.up_w, m.down_w] * (layers - 1)

    def load(k, side):
        owner = (dp, dx, dy, dd)[side]
        return pltpu.make_async_copy(
            outs[k].at[owner], held[k].at[owner], load_sem.at[k, side]
        )

    def loaded(k):
        for side in range(PLANE):
            load(k, side).wait()

    def keep(index, layer):
        source = getattr(m, SAVED[index])
        return pltpu.make_async_copy(
            source.at[layer], kept[index].at[layer], keep_sem.at[index, layer]
        )

    def keep_some(layer, names):
        for name in names:
            keep(SAVED.index(name), layer).start()

    def then_keep(step, layer, names):
        def run():
            step[0]()
            keep_some(layer, names)

        return (run, step[1])

    stages = []
    for layer in range(layers):
        steps = forward_steps(layer, m, narrow, layout_down.shape[1])
        if layer == 0:
            stages += [steps[0], steps[1], steps[2], steps[3]]
        else:
            stages += [steps[0] + steps[1], steps[2], steps[3]]
        stages[-2][-1] = then_keep(stages[-2][-1], layer, SAVED[:5] + SAVED[8:])
        stages[-1][-1] = then_keep(stages[-1][-1], layer, SAVED[5:8])

    def make_small():
        m.own_small_full[...] = jnp.zeros_like(m.own_small_full)
        units = layout_down.shape[1]
        for layer in range(layers):
            rows = pl.ds(layer * units, units)
            m.own_small_full[rows, 0:narrow] = layout_attn[layer].astype(full)
            m.own_small_full[rows, PAD : PAD + narrow] = layout_up[layer].astype(full)
            m.own_small_full[rows, 2 * PAD : 2 * PAD + narrow] = layout_down[layer].astype(full)
        m.own_small[...] = m.own_small_full[...].astype(low)

    def spread_vectors():
        m.spread[...] = jnp.zeros_like(m.spread)
        for n, piece in enumerate(pieces):
            m.spread[pl.ds(SUBLANES * n, layers), 0 : piece.shape[1]] = piece[...].astype(full)
        start = vector_out
        start[...] = jnp.zeros_like(start)
        lane = lane_of((SUBLANES, width))
        for row, n, base, lanes in flat_rows(width, narrow):
            length = pieces[n].shape[1]
            shift = lax.rem(at.me * length - base + 16 * width, width)
            rolled = pltpu.roll(m.spread[pl.ds(SUBLANES * n, SUBLANES), :], shift, 1)
            index = lane + (base - at.me * length)
            inside = (index >= 0) & (index < length) & (lane < lanes)
            rolled = jnp.where(inside, rolled, 0.0)
            for layer in range(layers):
                start[pl.ds(layer * VECTOR_ROWS + row, 1), :] = rolled[layer : layer + 1]
        vectors.send(0)

    def make_masks():
        pages = jnp.broadcast_to(page_row[...].astype(full), (tokens, tokens))
        turned = pages.T
        m.same[...] = jnp.where(pages == turned, 1.0, 0.0)
        group = jnp.where(
            turned == (2 * at.me).astype(full),
            jnp.broadcast_to(groups[:, 0:1], (tokens, tokens)),
            jnp.broadcast_to(groups[:, 1:2], (tokens, tokens)),
        )
        m.onehot[...] = jnp.where(group == lane_of((tokens, tokens)), 1.0, 0.0)

    def take_in():
        m.x[...] = text_in[...].astype(full)
        m.y[...] = jnp.zeros_like(m.y)
        m.y[:, 0:narrow] = layout_in[...].astype(full).T

    def land(k, sides):
        for side in sides:
            across(k, side, 1 - core).wait_recv()
            if side == 3 and k != fill:
                across(k, 4, 1 - core).wait_recv()
            load(k, side).start()

    signal(devices)
    make_small()
    greeted()
    for k in (0, fill, 1):
        own(k).start()
    line_start(0, 0)
    unit_start(True, 0)
    plane(fill, 0).start()
    plane(fill, 1).start()
    for k in range(2, count):
        if k != fill:
            own(k).start()

    plan = Plan()
    chain = [k for k in range(count) if k != fill]
    size = [sources[k].shape[0] / UNIT_ROWS_PER_US for k in range(count)]

    def begin_line(k, side):
        if side == 0:
            own(k).wait()
        if k > 0:
            line_start(k, 0, side)

    def next_line(k, hop, side):
        line_wait(k, hop, side, unit_start if k == 0 else None)
        if hop < depth - 1:
            line_start(k, hop, side)

    def add_line(k, side, after, needs, rank):
        sends = [("z", size[k], ("z", 1, k, side))]
        if k == 0:
            sends += [("x", size[k], ("u", 0)), ("x", size[fill], ("f", 1))]
        plan.add(("z", 0, k, side), functools.partial(begin_line, k, side), after, needs, sends, 0.3, rank)
        for hop in range(1, depth):
            sends = []
            if hop < depth - 1:
                sends.append(("z", size[k], ("z", hop + 1, k, side)))
            if k == 0:
                sends.append(("x", size[k], ("u", hop)))
            plan.add(
                ("z", hop, k, side),
                functools.partial(next_line, k, hop, side),
                [("z", hop - 1, k, side)],
                [("z", hop, k, side)],
                sends,
                0.3,
                rank,
            )

    def plane_first(k):
        if k > 0:
            plane(k, 0).start()
            plane(k, 1).start()
        across(k, 0, core).start()

    def plane_second(k):
        for index in (0, 1):
            if k == 0:
                for level in range(depth):
                    unit_landed(index == 0, level).wait_recv()
            else:
                plane(k, index, False).wait_recv()
            plane(k, index + 2).start()
            if k != fill:
                across(k, index + 1, core).start()

    def plane_third(k):
        for index in (2, 3):
            plane(k, index, False).wait_recv()
            if k != fill:
                across(k, index + 1, core).start()

    def cross_fill(side):
        across(fill, side, core).start()

    last = {}
    lines = [(k, 0) for k in chain]
    for side in range(4):
        lines.insert((4, 6, 7, 9)[side], (fill, side))
    for n, (k, side) in enumerate(lines):
        after = [("z", 1 if n > 1 else 2) + lines[n - 1]] if n else []
        if k == fill:
            after.append(("p", 2 if side < 3 else 3, fill))
        add_line(k, side, after, [], 10 * n)
    for n, k in enumerate(chain):
        arrive = ("x", k) if k else ("u", depth - 1)
        sends = [("c", 0.4 * size[k], ("c", 0, k))]
        if k:
            sends.append(("x", 4 * size[k], arrive))
        plan.add(("p", 1, k), functools.partial(plane_first, k), [("z", depth - 1, k, 0)], [], sends, 0.2, 10 * n + 1)
        sends = [("x", 2 * size[k], ("d", k)), ("c", 0.8 * size[k], ("c", 1, k))]
        plan.add(("p", 2, k), functools.partial(plane_second, k), [("p", 1, k)], [arrive], sends, 0.2, 10 * n + 2)
        sends = [("c", 0.4 * size[k], ("c", 2, k))]
        plan.add(("p", 3, k), functools.partial(plane_third, k), [("p", 2, k)], [("d", k)], sends, 0.2, 10 * n + 3)
    plan.add(
        ("p", 2, fill),
        functools.partial(plane_second, fill),
        [("z", 1, 0, 0)],
        [("f", 1)],
        [("x", size[fill] / 2, ("f", 2))],
        0.2,
        5,
    )
    plan.add(("p", 3, fill), functools.partial(plane_third, fill), [("p", 2, fill)], [("f", 2)], rank=6)
    for side in range(4):
        plan.add(
            ("a", side),
            functools.partial(cross_fill, side),
            [("z", depth - 1, fill, side)],
            [],
            [("c", 0.4 * size[fill], ("a", side))],
            0.1,
            25 + 10 * side,
        )
    previous = None
    vector_steps = [spread_vectors]
    vector_steps += [functools.partial(vectors.advance, n) for n in range(AllSum.STEPS)]
    for n, step_of in enumerate(vector_steps):
        link, amount = (("c", 0.3), ("z", 2.2), ("z", 4.0), ("x", 2.2), ("x", 2.2), ("h", 0.0))[n]
        sends = [(link, amount, ("v", n))]
        needs = [("v", n - 1)] if n else []
        after = [("v", n - 1)] if n else []
        if n == 1:
            after.append(("z", 2, 0, 0))
        plan.add(("v", n), step_of, after, needs, sends, 0.1 if n else 0.5, 2)
    plan.add("i", take_in, [("v", 0)], time=0.1, rank=3)
    plan.add("m", make_masks, ["i"], time=0.1, rank=3)
    previous = [("v", AllSum.STEPS), "m"]
    for k in range(count):
        vacant = [last[k - 3]] if k > 3 else []
        if k == fill:
            landed = [("a", side) for side in range(4)]
            plan.add(("l", k), functools.partial(land, k, range(4)), landed + vacant, landed, [("h", 2.4, ("h", k))], 0.2, 10 * k)
        else:
            landed = [("c", 0, k), ("c", 1, k)]
            plan.add(("k", k), functools.partial(land, k, range(3)), [("p", 2, k)] + vacant, landed, [("h", 2.0, ("k", k))], 0.2, 10 * k)
            plan.add(("l", k), functools.partial(land, k, (3,)), [("p", 3, k), ("k", k)], [("c", 2, k)], [("h", 0.7, ("h", k))], 0.2, 10 * k)
        for n, (closure, time) in enumerate(stages[k]):
            run = closure
            if n == 0:
                run = functools.partial(lambda k, closure: (loaded(k), closure()), k, closure)
            plan.add(("s", k, n), run, previous + [("l", k)], [("h", k)], (), time, 1000 + k, True)
            previous = [("s", k, n)]
        last[k] = previous[0]
    plan.run()
    text_out[...] = m.x[...]
    layout_out[...] = m.y[:, 0:narrow].T
    vectors.close()
    for index in range(len(SAVED)):
        for layer in range(layers):
            keep(index, layer).wait()
    for level in range(depth):
        for to_x in (True, False):
            unit_landed(to_x, level).wait_send()
    for k in range(count):
        for index in landed_across(k):
            across(k, index, core).wait_send()
        for index in range(4):
            if k > 0 or index > 1:
                plane(k, index).wait_send()
        for rising in (True, False):
            for hop in range(depth):

                @pl.when(goes_on(rising, hop))
                def drain():
                    for side in range(4 if k == fill else 1):
                        line(k, rising, hop, side).wait_send()


def run_forward(depth, narrow, weights, pieces, text_in, layout_in, page_row, groups):
    dma = pltpu.SemaphoreType.DMA
    tokens, width = text_in.shape
    layers, span, unused = weights[0].shape
    count = 3 * layers + 1
    full = jnp.float32
    saved = saved_shapes(layers, tokens, width, 4 * narrow)
    small_span = weights[5].shape[1]
    scratch = forward_shapes(layers, depth, tokens, width, narrow, small_span)
    rows = [span, layers * small_span] + [span] * (count - 2)
    vector_shape = (layers * VECTOR_ROWS, width)
    results = pl.pallas_call(
        functools.partial(forward_kernel, depth, layers, narrow, span),
        out_shape=[
            jax.ShapeDtypeStruct((PLANE, depth, 2, row, width), weights[0].dtype) for row in rows
        ]
        + [
            jax.ShapeDtypeStruct(vector_shape, full),
            jax.ShapeDtypeStruct((tokens, LANE), full),
            jax.ShapeDtypeStruct((tokens, width), full),
            jax.ShapeDtypeStruct((narrow, tokens), full),
        ]
        + [jax.ShapeDtypeStruct(*saved[name]) for name in SAVED],
        in_specs=[IN_VMEM] * 13,
        out_specs=[ANY] * count + [IN_VMEM] * 4 + [ANY] * len(SAVED),
        scratch_shapes=[
            dma((count,)),
            dma((count + 3, 2, depth)),
            dma((count + 3, depth)),
            dma((count, 4)),
            dma((count, 4)),
            dma((2, depth)),
            dma((2, depth)),
            dma((count, 5)),
            dma((count, 5)),
            dma((count, PLANE)),
            dma((len(SAVED), layers)),
        ]
        + AllSum.scratch(vector_shape)
        + [pltpu.VMEM(*saved[name]) for name in SAVED]
        + [pltpu.VMEM(*scratch[name]) for name in FORWARD_SCRATCH],
        compiler_params=pltpu.CompilerParams(
            collective_id=0, has_side_effects=True, vmem_limit_bytes=66000000
        ),
        name="forward_blocks",
    )(*weights, *pieces, text_in, layout_in, page_row, groups)
    return results[:count], results[count : count + 4], results[count + 4 :]


TEXT_MEMBERS = 3
LINKS = 10


def back_shapes(layers, depth, tokens, width, narrow_hidden):
    low, full = jnp.bfloat16, jnp.float32
    span = 4 * width // (PLANE * depth * 2)
    unit = (PLANE, depth, span, LANE)
    whole = (PLANE, depth, 2, span, LANE)
    return dict(
        weights=((2, PLANE, depth, 2, span, width), low),
        gx=((tokens, width), full),
        gy=((tokens, PAD), full),
        down_low=((tokens, width), low),
        down_low_small=((tokens, PAD), low),
        branch_low=((tokens, width), low),
        branch_low_small=((tokens, PAD), low),
        wide=((tokens, width), full),
        upper_low=((tokens, 4 * width), low),
        upper_low_small=((tokens, narrow_hidden), low),
        context=((tokens, width), low),
        context_small=((tokens, PAD), low),
        joined=((3, tokens, width), low),
        mixed=((3, tokens, PAD), full),
        rows_up=(whole, low),
        rows_attn=(whole, low),
        rows_small=((2, narrow_hidden, tokens), low),
        in_land=((layers, 4, tokens, width), low),
        in_land_small=((layers, 4, tokens, PAD), low),
        rows_land=((layers, 3) + unit, low),
        rows_land_small=((layers, 3, narrow_hidden, tokens), low),
        sums=((layers * VECTOR_ROWS, width), full),
    )


BACK_SCRATCH = tuple(back_shapes(1, 1, 1, 1, 1))


def standard_back(grad, normed, scale, gain, width):
    pushed = grad * gain
    average = jnp.sum(pushed, axis=1, keepdims=True) * (1.0 / width)
    along = jnp.sum(pushed * normed, axis=1, keepdims=True) * (1.0 / width)
    result = scale * (pushed - average - normed * along)
    if grad.shape[1] != width:
        result = jnp.where(lane_of(grad.shape) < width, result, 0.0)
    return result, total(grad * normed), total(grad)


def total(rows):
    return jnp.sum(rows.astype(jnp.float32), axis=0, keepdims=True)


def rows_of_core(span, layers, layer, depth, core):
    shape = (depth * layers * span, 2 * depth * span)
    row = lax.broadcasted_iota(jnp.int32, shape, 0)
    column = lax.broadcasted_iota(jnp.int32, shape, 1)
    unit = unit_of(row, layers * span, depth)
    inside = row - unit * layers * span - layer * span
    source = (2 * unit + core) * span + inside
    return jnp.where((source == column) & (inside >= 0) & (inside < span), 1.0, 0.0)


def backward_kernel(depth, layers, narrow, span, *refs):
    refs = list(refs)

    def take(number):
        taken = refs[:number]
        del refs[:number]
        return taken

    text_count = TEXT_MEMBERS * layers
    count = text_count + 1
    gathered = take(text_count)
    kept = take(len(SAVED))
    vec_ref, text_cot, layout_cot, onehot = take(4)
    finals = take(count)
    vector_out, text_out, layout_out = take(3)
    layout_turned, early_sem = refs[-2:]
    del refs[-2:]
    m = SimpleNamespace()
    for name in SAVED + BACK_SCRATCH:
        setattr(m, name, refs.pop(0))
    mine_text, mine_small = take(2)
    landed_diag, landed_plane, landed_line = take(count), take(count), take(count)
    outs = take(count)
    weight_sem, keep_sem, out_sem, xs, xr, ps, pr, zs, zr = take(9)
    all_sum = take(4)
    at, devices = place(depth)
    dp, z, core, dx, dy, dd = at.dp, at.z, at.core, at.dx, at.dy, at.dd
    fill = 1
    owners = (dp, dx, dy, dd)
    half = depth // 2
    low = jnp.bfloat16
    tokens, width = m.gx.shape
    hidden_small = m.upper_low_small.shape[1]
    signal(devices)
    vectors = AllSum(devices, vector_out, *all_sum)

    slots, reuse = {}, {}
    for k in range(count):
        if k < text_count:
            spare = [n for n in range(mine_text.shape[0]) if n not in slots.values()]
            if spare:
                slots[k] = spare[0]
            else:
                reuse[k] = min(n for n in slots if n != fill and n not in reuse.values())
                slots[k] = slots[reuse[k]]

    def mine(k):
        if k == text_count:
            return mine_small
        return mine_text.at[slots[k]]

    order = []
    for layer in reversed(range(layers)):
        order += [3 * layer + 2, 3 * layer + 1, 3 * layer]

    def weight_load(index):
        return pltpu.make_async_copy(
            gathered[order[index]], m.weights.at[index % 2], weight_sem.at[index]
        )

    def saved_load(name, layer):
        index = SAVED.index(name)
        return pltpu.make_async_copy(
            kept[index].at[layer], getattr(m, name), keep_sem.at[index, layer]
        )

    def cross(layer, link):
        moves = (
            (m.low, m.in_land.at[layer, pl.ds(0, 3)]),
            (m.turned.at[:, :, 1 - core], m.rows_land.at[layer, 0]),
            (m.down_low, m.in_land.at[layer, 3]),
            (m.rows_up.at[:, :, 1 - core], m.rows_land.at[layer, 1]),
            (m.rows_attn.at[:, :, 1 - core], m.rows_land.at[layer, 2]),
            (m.low_small, m.in_land_small.at[layer, pl.ds(0, 3)]),
            (m.turned_small, m.rows_land_small.at[layer, 0]),
            (m.down_low_small, m.in_land_small.at[layer, 3]),
            (m.rows_small.at[0], m.rows_land_small.at[layer, 1]),
            (m.rows_small.at[1], m.rows_land_small.at[layer, 2]),
        )
        source, target = moves[link]
        return remote(
            source, target, xs.at[layer, link], xr.at[layer, link], devices.core
        )

    def plane(k, index):
        if k == fill:
            size = landed_diag[k].shape[1]
            lower, upper = pl.ds(0, size), pl.ds(size, size)
            own = lambda owner, rows: mine(k).at[owner, z, rows]
        else:
            lower, upper = pl.ds(0, half), pl.ds(half, half)
            own = lambda owner, levels: mine(k).at[owner, levels]
        diag, direct = landed_diag[k], landed_plane[k]
        moves = (
            (dd, lower, diag.at[0], devices.y),
            (dd, upper, diag.at[1], devices.x),
            (dx, upper, direct.at[0, upper], devices.x),
            (dy, lower, direct.at[1, lower], devices.y),
            (dx, lower, direct.at[0, lower], devices.x),
            (dy, upper, direct.at[1, upper], devices.y),
        )
        owner, part, target, device = moves[index]
        return remote(own(owner, part), target, ps.at[k, index], pr.at[k, index], device)

    def line(k, rising, level, slot, side=0):
        row = k if side == 0 else count - 1 + side
        return remote(
            mine(k).at[owners[side], level],
            landed_line[k].at[slot, side],
            zs.at[row, int(rising), level],
            zr.at[row, int(rising), level],
            devices.up if rising else devices.down,
        )

    def second_sums(k):
        if k == fill:
            size = landed_diag[k].shape[1]
            lower, upper = pl.ds(0, size), pl.ds(size, size)
            one, other = mine(k).at[dx, z, lower], mine(k).at[dy, z, upper]
            add = add_rows
        else:
            one = mine(k).at[dx, pl.ds(0, half)]
            other = mine(k).at[dy, pl.ds(half, half)]
            add = add_units
        plane(k, 0).wait_recv()
        add(one, landed_diag[k].at[0])
        plane(k, 4).start()
        plane(k, 1).wait_recv()
        add(other, landed_diag[k].at[1])
        plane(k, 5).start()

    def third_sums(k):
        for index in (2, 3, 4, 5):
            plane(k, index).wait_recv()
        if k == fill:
            result = mine(k)[dp, z].astype(jnp.float32)
            for side in range(2):
                result = result + landed_plane[k][side].astype(jnp.float32)
            outs[k][...] = result
            put_out(k).start()
        else:
            add_units(mine(k).at[dp], landed_plane[k].at[0], landed_plane[k].at[1])
            line_step(k, 0)

    def passed(rising, hop):
        return range(hop + 1, depth) if rising else range(depth - 1 - hop)

    def line_step(k, hop, side=0):
        for rising in (True, False):

            @pl.when(z == (hop if rising else depth - 1 - hop))
            def move():
                for level in passed(rising, hop):
                    if hop > 0:
                        line(k, rising, level, level, side).wait_recv()
                        add_rows(mine(k).at[owners[side], level], landed_line[k].at[level, side])
                    last = rising and level == hop + 1
                    line(k, rising, level, depth if last else level, side).start()

    def last_sums(k, side=0):
        if k != fill:
            outs[k][...] = mine(k)[dp, z].astype(jnp.float32)
        for rising in (True, False):

            @pl.when((z > 0) if rising else (z < depth - 1))
            def add():
                slot = depth if rising else z
                line(k, rising, z, slot, side).wait_recv()
                if k == fill:
                    add_rows(mine(k).at[owners[side], z], landed_line[k].at[slot, side])
                else:
                    outs[k][...] += landed_line[k][slot, side].astype(jnp.float32)

        if k != fill:
            put_out(k).start()

    def early():
        return (
            pltpu.make_async_copy(m.gx, text_out, early_sem.at[0]),
            pltpu.make_async_copy(layout_turned, layout_out, early_sem.at[1]),
        )

    def put_out(k):
        return pltpu.make_async_copy(outs[k], finals[k], out_sem.at[k])

    def fill_plane():
        for index in range(4):
            plane(fill, index).start()

    def drain(k):
        for index in range(6):
            plane(k, index).wait_send()
        for hop in range(depth - 1):
            for rising in (True, False):

                @pl.when(z == (hop if rising else depth - 1 - hop))
                def wait():
                    for level in passed(rising, hop):
                        for side in range(PLANE if k == fill else 1):
                            line(k, rising, level, level, side).wait_send()

    plan = Plan()
    size = [outs[k].shape[0] / UNIT_ROWS_PER_US for k in range(count)]

    def add_scatter(k, rank):
        one = size[k]

        def step(hop, side):
            if hop < depth - 1:
                line_step(k, hop, side)
            else:
                last_sums(k, side)

        for side in range(PLANE if k == fill else 1):
            for hop in range(0 if k == fill else 1, depth):
                sends = []
                if hop < depth - 1:
                    sends.append((("z", hop), (depth - 1 - hop) * one, ("z", hop + 1, k, side)))
                after = [("z", hop - 1, k, side)] if hop else [("o", k)]
                if k != fill and hop == 1:
                    after = [("s", 3, k)]
                if k == fill and hop == 0 and side:
                    after.append(("z", 1, k, side - 1))
                needs = [("z", hop, k, side)] if hop else []
                plan.add(
                    ("z", hop, k, side), functools.partial(step, hop, side), after, needs, sends, 0.3, rank
                )
        first = ("o", k)
        share = 2 * one
        if k == fill:
            first, share = ("f", 0), one / 2
            sends = [("x", share, ("d", k)), ("x", share, ("e", k))]
            ends = [("z", depth - 1, k, side) for side in range(PLANE)]
            ends.append(("s", 2, text_count))
            plan.add(first, fill_plane, ends, [], sends, 0.2, rank)
        plan.add(
            ("s", 2, k), functools.partial(second_sums, k), [first], [("d", k)], [("x", share, ("g", k))], 0.5, rank
        )
        sends = [(("z", 0), (depth - 1) * one, ("z", 1, k, 0))] if k != fill else []
        before = [("s", 2, k)]
        if k == fill:
            before.append(("z", 1, text_count - 1, 0))
        plan.add(
            ("s", 3, k), functools.partial(third_sums, k), before, [("e", k), ("g", k)], sends, 1.0, rank
        )

    def own_sends(k):
        if k == fill:
            return []
        return [("x", 2 * size[k], ("d", k)), ("x", 2 * size[k], ("e", k))]

    previous = []

    def then(name, run, time, needs=(), sends=(), after=()):
        plan.add(name, run, previous + list(after), needs, sends, time, 1000, True)
        previous[:] = [name]

    def done(k):
        return [("s", 3, k), ("z", depth - 1, k, 0)]

    def own_sums(k, rows, rows_land, ins, ins_land):
        if k in reuse:
            drain(reuse[k])

        def block(turn, carry):
            owner = jnp.where(turn == 0, dd, jnp.where(turn == 1, dx, jnp.where(turn == 2, dy, dp)))
            left = jnp.concatenate(
                [
                    rows[owner, :, core].reshape(-1, tokens),
                    rows_land[owner].reshape(-1, tokens),
                ],
                axis=1,
            )
            right = jnp.concatenate([ins(owner), ins_land(owner)], axis=0)
            result = dot_nn(left, right)
            mine(k)[owner] = result.astype(low).reshape(depth, -1, width)
            if k != fill:
                for index, when in enumerate((0, 0, 1, 2)):

                    @pl.when(turn == when)
                    def send():
                        plane(k, index).start()

            return carry

        lax.fori_loop(0, PLANE, block, 0)

    m.gx[...] = text_cot[...].astype(jnp.float32)
    m.gy[...] = jnp.zeros_like(m.gy)
    m.gy[:, 0:narrow] = layout_cot[...].astype(jnp.float32).T
    first_names = ("norm", "scales", "turned", "norm_small", "turned_small", "slope", "low")
    names = first_names + tuple(name for name in SAVED if name not in first_names)
    weight_load(0).start()
    for name in names:
        saved_load(name, layers - 1).start()
    weight_load(1).start()
    greeted()

    def add_layer(turn, layer):
        k = TEXT_MEMBERS * turn
        vec = lambda row, n=1: vec_ref[pl.ds(layer * VECTOR_ROWS + row, n), :]
        small_vec = lambda row: vec(SMALL_ROW + row)[:, :PAD]
        slot = lambda member: m.weights.at[(3 * turn + member) % 2]

        def put(row, value):
            m.sums[pl.ds(layer * VECTOR_ROWS + row, 1), :] = value

        def put_small(row, value):
            m.sums[pl.ds(layer * VECTOR_ROWS + SMALL_ROW + row, 1), :PAD] = value


        def tail():
            m.sums[pl.ds(layer * VECTOR_ROWS + SMALL_ROW, VECTOR_ROWS - SMALL_ROW), :] = jnp.zeros(
                (VECTOR_ROWS - SMALL_ROW, width), jnp.float32
            )
            for name in ("norm", "scales", "turned"):
                saved_load(name, layer).wait()
            cross(layer, 1).start()
            grad, gain_sum, shift_sum = standard_back(
                m.gx[...], m.norm[1], m.scales[2][:, :1], vec(6), width
            )
            put(6, gain_sum)
            put(7, shift_sum)
            m.gx[...] = grad
            m.down_low[...] = grad.astype(low)
            cross(layer, 2).start()
            put(3, total(m.down_low[...]))

        def tail_small():
            for name in ("norm_small", "turned_small"):
                saved_load(name, layer).wait()
            cross(layer, 6).start()
            grad, gain_sum, shift_sum = standard_back(
                m.gy[...], m.norm_small[1], m.scales[3][:, :1], small_vec(6), narrow
            )
            put_small(6, gain_sum)
            put_small(7, shift_sum)
            m.gy[...] = grad
            m.down_low_small[...] = grad.astype(low)
            cross(layer, 7).start()
            put_small(3, total(m.down_low_small[...]))

        def own_down():
            cross(layer, 1).wait_recv()
            cross(layer, 2).wait_recv()
            own_sums(
                k,
                m.turned,
                m.rows_land.at[layer, 0],
                lambda owner: m.down_low[...],
                lambda owner: m.in_land[layer, 3],
            )

        cut = 3 * LANE

        def hidden(block, carry):
            m.wide[...] = dot_nt(m.down_low[...], unit_rows(slot(0), block))
            for side in range(width // cut):
                inside = pl.ds(side * cut, cut)
                columns = pl.ds(pl.multiple_of(block * width + side * cut, LANE), cut)
                rows = m.slope[:, columns] * m.wide[:, inside]
                rows_low = rows.astype(low)
                m.upper_low[:, columns] = rows_low
                m.sums[pl.ds(layer * VECTOR_ROWS + 8 + block, 1), inside] = total(rows_low)
                levels = depth * cut // width
                m.rows_up[block, pl.ds(side * levels, levels)] = (
                    rows.T.astype(low).reshape(levels, 2, -1, tokens)
                )
            return carry


        def hidden_blocks(first, number):
            if first == 0:
                for name in names[5:]:
                    saved_load(name, layer).wait()
                cross(layer, 0).start()
                cross(layer, 5).start()
                weight_load(3 * turn).wait()
            lax.fori_loop(first, first + number, hidden, 0)
            if first + number == PLANE:
                cross(layer, 3).start()
                if 3 * turn + 2 < 3 * layers:
                    weight_load(3 * turn + 2).start()

        def hide_small():
            m.wide[...] = dot_nt(m.down_low_small[...], m.small_ff[1])

            for side in range(hidden_small // cut):
                columns = pl.ds(side * cut, cut)
                rows = m.slope_small[:, columns] * m.wide[:, columns]
                rows_low = rows.astype(low)
                m.upper_low_small[:, columns] = rows_low
                m.rows_small[0, columns, :] = rows.T.astype(low)
                m.sums[
                    pl.ds(layer * VECTOR_ROWS + SMALL_HIDDEN_ROW, 1), columns
                ] = total(rows_low)
            cross(layer, 8).start()

        def own_up():
            cross(layer, 0).wait_recv()
            cross(layer, 3).wait_recv()
            own_sums(
                k + 1,
                m.rows_up,
                m.rows_land.at[layer, 1],
                lambda owner: m.low[2],
                lambda owner: m.in_land[layer, 2],
            )

        def lower_text():
            weight_load(3 * turn + 1).wait()

            def lower(block, carry):
                columns = pl.ds(pl.multiple_of(block * width, LANE), width)
                m.gx[...] += dot_nn(m.upper_low[:, columns], unit_rows(slot(1), block))
                return carry

            lax.fori_loop(0, PLANE, lower, 0)
            if 3 * turn + 3 < 3 * layers:
                weight_load(3 * turn + 3).start()
            grad, gain_sum, shift_sum = standard_back(
                m.gx[...], m.norm[0], m.scales[0][:, :1], vec(4), width
            )
            put(4, gain_sum)
            put(5, shift_sum)
            m.gx[...] = grad
            m.branch_low[...] = grad.astype(low)
            put(2, total(m.branch_low[...]))
            for side in range(width // cut):
                levels = depth * cut // width
                tile = m.gx[:, side * cut : (side + 1) * cut]
                m.rows_attn[3, pl.ds(side * levels, levels)] = (
                    tile.T.astype(low).reshape(levels, 2, -1, tokens)
                )

        def lower_small():
            grad = m.gy[...] + dot_nn(m.upper_low_small[...], m.small_ff[0])
            grad, gain_sum, shift_sum = standard_back(
                grad, m.norm_small[0], m.scales[1][:, :1], small_vec(4), narrow
            )
            put_small(4, gain_sum)
            put_small(5, shift_sum)
            m.gy[...] = grad
            m.branch_low_small[...] = grad.astype(low)
            put_small(2, total(m.branch_low_small[...]))
            m.rows_small[1, pl.ds(3 * narrow, narrow), :] = grad.T[:narrow].astype(low)

        def contexts():
            weight_load(3 * turn + 2).wait()
            m.context[...] = dot_nn(m.branch_low[...], unit_rows(slot(2), 3)).astype(low)
            m.context_small[...] = dot_nn(m.branch_low_small[...], m.small_attn[3]).astype(low)
            m.mixed[...] = jnp.zeros_like(m.mixed)

        def pair_back(pair, carry):
            lanes = pl.ds(pl.multiple_of(pair * LANE, LANE), LANE)
            query, keyed, valued = (m.heads[n, :, lanes] for n in range(3))
            small_query, small_keyed, small_valued = (m.heads_small[n] for n in range(3))
            context, context_small = m.context[:, lanes], m.context_small[...]
            lane, small_lane = lane_of((1, LANE)), lane_of((1, PAD))
            results = []
            for side in range(2):
                head = 2 * pair + side
                chosen = (lane >= 64 * side) & (lane < 64 * side + 64)
                small_chosen = (small_lane >= 16 * head) & (small_lane < 16 * head + 16)
                mask = jnp.where(chosen, 1.0, 0.0).astype(low)
                small_mask = jnp.where(small_chosen, 1.0, 0.0).astype(low)
                probs = m.probs[head]
                grad_probs = dot_nt(context * mask, valued) + dot_nt(
                    context_small * small_mask, small_valued
                )
                inner = jnp.sum(grad_probs * probs, axis=1, keepdims=True)
                scores = probs * (grad_probs - inner)
                scores_low = scores.astype(low)
                scores_turned = scores.T.astype(low)
                probs_turned = probs.T.astype(low)
                results.append(
                    (
                        dot_nn(scores_low, keyed) * 0.125,
                        dot_nn(scores_turned, query) * 0.125,
                        dot_nn(probs_turned, context),
                    )
                )
                small = (
                    dot_nn(scores_low, small_keyed) * 0.25,
                    dot_nn(scores_turned, small_query) * 0.25,
                    dot_nn(probs_turned, context_small),
                )
                for n in range(3):
                    m.mixed[n] += jnp.where(small_chosen, small[n], 0.0)
            for n in range(3):
                m.joined[n, :, lanes] = jnp.where(lane < 64, results[0][n], results[1][n]).astype(
                    low
                )
            return carry


        def pairs(first, number):
            lax.fori_loop(first, first + number, pair_back, 0)

        def turn_rows():
            for part in range(3):
                for side in range(width // cut):
                    levels = depth * cut // width
                    tile = m.joined[part, :, side * cut : (side + 1) * cut].astype(jnp.float32)
                    m.rows_attn[part, pl.ds(side * levels, levels)] = (
                        tile.T.astype(low).reshape(levels, 2, -1, tokens)
                    )
                tile = m.mixed[part].astype(low).astype(jnp.float32)
                m.rows_small[1, pl.ds(part * narrow, narrow), :] = tile.T[:narrow].astype(low)
            cross(layer, 4).start()
            cross(layer, 9).start()
            put(0, total(m.joined[0]))
            put(1, total(m.joined[2]))
            put_small(0, total(m.mixed[0].astype(low)))
            put_small(1, total(m.mixed[2].astype(low)))

        def entering(part, carry):
            m.gx[...] += dot_nn(m.joined[part], unit_rows(slot(2), part))
            return carry


        def attn_sums():
            cross(layer, 4).wait_recv()
            own_sums(
                k + 2,
                m.rows_attn,
                m.rows_land.at[layer, 2],
                lambda owner: m.low[jnp.where(owner == PLANE - 1, 1, 0)],
                lambda owner: m.in_land[layer, jnp.where(owner == PLANE - 1, 1, 0)],
            )


        def enter():
            lax.fori_loop(0, 3, entering, 0)
            if 3 * turn + 4 < 3 * layers:
                weight_load(3 * turn + 4).start()
            grad = m.gy[...]
            for part in range(3):
                grad = grad + dot_nn(m.mixed[part].astype(low), m.small_attn[part])
            m.gy[...] = grad
            for group in range(LANGS):
                put(TABLE_ROW + group, total(onehot[:, group : group + 1] * m.gx[...]))
            if layer == 0:
                layout_turned[...] = m.gy[:, 0:narrow].T
                for one in early():
                    one.start()
                vector_out[...] = m.sums[...]
                vectors.send(0)

        def small_sums():
            for link in (5, 6, 7, 8, 9):
                cross(layer, link).wait_recv()
            arrange = rows_of_core(span, layers, layer, depth, core).astype(low)
            small_rows = (m.rows_small.at[1], m.rows_small.at[0], m.turned_small)
            small_land = (2, 1, 0)
            for member in range(3):
                for block in range(PLANE):
                    rows = pl.ds(block * narrow, narrow)
                    source = (1 if block == PLANE - 1 else 0, 2, 3)[member]
                    own_in = m.down_low_small[...] if member == 2 else m.low_small[source]
                    left = jnp.concatenate(
                        [
                            small_rows[member][rows, :],
                            m.rows_land_small[layer, small_land[member], rows, :],
                        ],
                        axis=1,
                    )
                    right = jnp.concatenate([own_in, m.in_land_small[layer, source]], axis=0)
                    placed = dot_nn(arrange, dot_nn(left, right).astype(low)).astype(low)
                    placed = placed.reshape(depth, layers * span, PAD)
                    lanes = pl.ds(member * PAD, PAD)
                    if turn > 0:
                        placed = mine_small[block, :, :, lanes] + placed
                    mine_small[block, :, :, lanes] = placed
            if layer > 0:
                for link in range(LINKS):
                    cross(layer, link).wait_send()
                for name in names:
                    saved_load(name, layer - 1).start()
            if layer == 0:
                for index in range(4):
                    plane(text_count, index).start()

        own = lambda n: ("o", k + n)
        crossed = lambda link: ("c", layer, link)
        free = lambda n: done(reuse[k + n]) if k + n in reuse else []
        then(("t", 0, turn), tail, 1.7, sends=[("c", 1.0, crossed(1)), ("c", 0.5, crossed(2))])
        then(("t", 1, turn), tail_small, 0.2, sends=[("c", 0.8, crossed(6))])
        then(own(0), own_down, 1.4, [crossed(1), crossed(2)], own_sends(k), free(0))
        add_scatter(k, k)
        then(
            ("h", 0, turn), functools.partial(hidden_blocks, 0, 2), 1.4, sends=[("c", 1.5, crossed(0))]
        )
        then(
            ("h", 1, turn), functools.partial(hidden_blocks, 2, 2), 1.3, sends=[("c", 1.0, crossed(3))]
        )
        then(("h", 2, turn), hide_small, 0.4, sends=[("c", 0.5, crossed(8))])
        then(own(1), own_up, 1.4, [crossed(0), crossed(3)], own_sends(k + 1), free(1))
        add_scatter(k + 1, k + 1)
        then(("n", 0, turn), lower_text, 1.7)
        then(("n", 1, turn), lower_small, 0.4)
        then(("n", 2, turn), contexts, 0.4)
        then(("p", 0, turn), functools.partial(pairs, 0, H // 4), 2.7)
        then(("p", 1, turn), functools.partial(pairs, H // 4, H // 4), 2.7)
        then(("r", turn), turn_rows, 0.4, sends=[("c", 1.0, crossed(4)), ("c", 0.5, crossed(9))])
        then(own(2), attn_sums, 1.4, [crossed(4)], own_sends(k + 2), free(2))
        add_scatter(k + 2, k + 2)
        then(("e", turn), enter, 1.4, sends=[("c", 0.3, ("v", 0))] if layer == 0 else [])
        if layer > 0:
            then(("w", turn), small_sums, 2.6, [crossed(9)])
        else:
            late = [("s", 2, k + 2)]
            then(("o", text_count), small_sums, 2.6, [crossed(9)], own_sends(text_count), late)
            add_scatter(text_count, text_count)

    for turn, layer in enumerate(reversed(range(layers))):
        add_layer(turn, layer)
    for n in range(AllSum.STEPS):
        sends = [((("z", 0), 2.2), (("z", 0), 4.4), ("x", 2.2), ("x", 2.2), ("c", 0.0))[n] + (("v", n + 1),)]
        after = [("v", n - 1)] if n else [("e", layers - 1)]
        if n == 3:
            after.append(("z", 1, text_count - 1, 0))
        plan.add(("v", n), functools.partial(vectors.advance, n), after, [("v", n)], sends, 0.2, -1)
    plan.run()
    vectors.close()
    for link in range(LINKS):
        cross(0, link).wait_send()
    drained = list(reuse.values())
    for k in range(count):
        put_out(k).wait()
    for one in early():
        one.wait()
    for k in range(count):
        if k not in drained:
            drain(k)


def run_backward(depth, layers, narrow, span, gathered, saved, vectors, text_cot, layout_cot, onehot):
    dma = pltpu.SemaphoreType.DMA
    tokens, width = text_cot.shape
    low, full = jnp.bfloat16, jnp.float32
    shapes = back_shapes(layers, depth, tokens, width, 4 * narrow)
    unit = gathered[0].shape[3:]
    small_unit = (layers * span, width)
    units = [unit] * (TEXT_MEMBERS * layers) + [small_unit]
    count = len(units)
    whole = (layers, PLANE, depth, 2, -1, tokens)
    kept = [
        array.reshape(whole) if array.ndim == 3 and array.shape[1] == 4 * width else array
        for array in saved
    ]
    scratch = [pltpu.VMEM(array.shape[1:], array.dtype) for array in kept]
    scratch += [pltpu.VMEM(*shapes[name]) for name in BACK_SCRATCH]
    scratch += [
        pltpu.VMEM((4, PLANE, depth) + unit, low),
        pltpu.VMEM((PLANE, depth) + small_unit, low),
    ]
    fill = 1
    landing = [((2, depth // 2) + one, (2, depth) + one, (depth + 1, 1) + one) for one in units]
    landing[fill] = (
        (2, unit[0] // 2, width),
        (2,) + unit,
        (depth + 1, PLANE) + unit,
    )
    for n in range(3):
        scratch += [pltpu.VMEM(shapes_of[n], low) for shapes_of in landing]
    scratch += [pltpu.VMEM(one, full) for one in units]
    scratch += [
        dma((len(gathered),)),
        dma((len(SAVED), layers)),
        dma((count,)),
        dma((layers, LINKS)),
        dma((layers, LINKS)),
        dma((count, 6)),
        dma((count, 6)),
        dma((count + 3, 2, depth)),
        dma((count + 3, 2, depth)),
    ]
    scratch += AllSum.scratch(vectors.shape)
    scratch += [pltpu.VMEM((narrow, tokens), full), dma((2,))]
    results = pl.pallas_call(
        functools.partial(backward_kernel, depth, layers, narrow, span),
        out_shape=[jax.ShapeDtypeStruct(one, full) for one in units]
        + [
            jax.ShapeDtypeStruct(vectors.shape, full),
            jax.ShapeDtypeStruct((tokens, width), full),
            jax.ShapeDtypeStruct((narrow, tokens), full),
        ],
        in_specs=[ANY] * (len(gathered) + len(kept)) + [IN_VMEM] * 4,
        out_specs=[ANY] * count + [IN_VMEM, ANY, ANY],
        scratch_shapes=scratch,
        compiler_params=pltpu.CompilerParams(
            collective_id=1, has_side_effects=True, vmem_limit_bytes=67000000
        ),
        name="backward_blocks",
    )(*gathered, *kept, vectors, text_cot, layout_cot, onehot)
    return results


def finish_kernel(depth, layers, narrow, span, small_span, *refs):
    count = TEXT_MEMBERS * layers + 1
    summed, totals, ins = refs[:count], refs[count], refs[count + 1 : count + 5]
    outs = refs[count + 5 :]
    width = ins[0].shape[1]
    at, unused = place(depth)
    for n in range(4):
        outs[n][...] = ins[n][...]
    attn, up, down = outs[4:7]
    pieces = outs[7:9] + outs[12:13]
    small_attn, small_up, small_down = outs[9:12]
    for layer in range(layers):
        parts = summed[TEXT_MEMBERS * (layers - 1 - layer) :]
        down[layer] = parts[0][...]
        up[layer] = parts[1][...]
        attn[layer] = parts[2][...]
        rows = summed[count - 1][layer * small_span : (layer + 1) * small_span, :]
        small_attn[layer] = rows[:, 0:narrow]
        small_up[layer] = rows[:, PAD : PAD + narrow]
        small_down[layer] = rows[:, 2 * PAD : 2 * PAD + narrow]
    lane = lane_of((layers, width))
    found = [jnp.zeros((layers, width), jnp.float32) for piece in pieces]
    for row, n, base, lanes in flat_rows(width, narrow):
        first = at.me * pieces[n].shape[1] - base
        rows = jnp.concatenate(
            [totals[pl.ds(layer * VECTOR_ROWS + row, 1), :] for layer in range(layers)], axis=0
        )
        rolled = pltpu.roll(rows, lax.rem(16 * width - first, width), 1)
        index = lane + first
        found[n] = found[n] + jnp.where((index >= 0) & (index < lanes), rolled, 0.0)
    for n, piece in enumerate(pieces):
        piece[...] = found[n][:, : piece.shape[1]]


def run_finish(depth, layers, narrow, span, small_span, lengths, results, text_out, layout_out):
    count = TEXT_MEMBERS * layers + 1
    summed, (totals, text_grad, layout_grad) = results[:count], results[count:]
    tokens, width = text_out.shape
    shapes = [
        (tokens, width),
        (narrow, tokens),
        (tokens, width),
        (narrow, tokens),
        (layers, span, width),
        (layers, span, width),
        (layers, span, width),
        (layers, lengths[0]),
        (layers, lengths[1]),
        (layers, small_span, narrow),
        (layers, small_span, narrow),
        (layers, small_span, narrow),
        (layers, lengths[2]),
    ]
    return pl.pallas_call(
        functools.partial(finish_kernel, depth, layers, narrow, span, small_span),
        out_shape=[jax.ShapeDtypeStruct(shape, jnp.float32) for shape in shapes],
        in_specs=[IN_VMEM] * (count + 5),
        out_specs=[IN_VMEM] * len(shapes),
        name="finish",
    )(*summed, totals, text_out, layout_out, text_grad, layout_grad)


def block_shards(
    depth,
    text_input,
    layout_input,
    text_cot,
    layout_cot,
    segment_ids,
    page_groups,
    lang_table,
    text_attn,
    text_up,
    text_down,
    text_vector,
    layout_attn,
    layout_up,
    layout_down,
    layout_vector,
):
    layers, unused, span = text_attn.shape
    narrow, small_span = layout_input.shape[1], layout_down.shape[1]

    def turned(array):
        return jnp.swapaxes(array, -1, -2)

    weights = (
        turned(text_attn),
        turned(text_up),
        text_down,
        turned(layout_attn),
        turned(layout_up),
        layout_down,
    )
    pieces = (text_vector, lang_table, layout_vector)
    gathered, (vectors, onehot, text_out, layout_out), saved = run_forward(
        depth,
        narrow,
        weights,
        pieces,
        text_input,
        turned(layout_input),
        segment_ids.reshape(1, -1),
        page_groups.reshape(1, -1),
    )
    text_gathered = [part for n, part in enumerate(gathered) if n != 1]
    results = run_backward(
        depth,
        layers,
        narrow,
        small_span,
        text_gathered,
        saved,
        vectors,
        text_cot,
        turned(layout_cot),
        onehot,
    )
    lengths = [piece.shape[1] for piece in pieces]
    outs = run_finish(
        depth, layers, narrow, span, small_span, lengths, results, text_out, layout_out
    )
    return tuple(turned(out) if n in (1, 3, 4, 5, 9, 10) else out for n, out in enumerate(outs))


def solution(mesh):
    in_specs = (
        P(AXES, None),
        P(AXES, None),
        P(AXES, None),
        P(AXES, None),
        P(AXES),
        P(AXES),
        P(None, AXES),
        P(None, None, AXES),
        P(None, None, AXES),
        P(None, AXES, None),
        P(None, AXES),
        P(None, None, AXES),
        P(None, None, AXES),
        P(None, AXES, None),
        P(None, AXES),
    )
    out_specs = (
        P(AXES, None),
        P(AXES, None),
        P(AXES, None),
        P(AXES, None),
        P(None, None, AXES),
        P(None, None, AXES),
        P(None, AXES, None),
        P(None, AXES),
        P(None, AXES),
        P(None, None, AXES),
        P(None, None, AXES),
        P(None, AXES, None),
        P(None, AXES),
    )
    plan = functools.partial(block_shards, mesh.shape[AXES[1]] // 2) if fits_blocks(mesh) else generic_shards
    return jax.shard_map(plan, mesh=mesh, in_specs=in_specs, out_specs=out_specs, check_vma=False)
```
